32 devices in a mesh: context: 4 (over x, core), fsdp: 8 (over z, y).
Axes of the slice: x: 2, y: 2, z: 4, core: 2. Of those that a mesh axis runs over, the one named last changes fastest.
Arguments:
- tokens: bfloat16 [8, 2048, 2048], P('fsdp', 'context'), may hold values from -6 to 6
- segment_ids: int32 [8, 2048], P('fsdp', 'context'), may hold values from 0 to 3, as said below
- norm1_gain: bfloat16 [2048], P('fsdp'), may hold values from 0.5 to 1.5
- w_query: bfloat16 [2048, 256], P('fsdp'), may hold values from -0.125 to 0.125
- w_key: bfloat16 [2048, 256], P('fsdp'), may hold values from -0.125 to 0.125
- w_value: bfloat16 [2048, 2048], P('fsdp'), may hold values from -0.125 to 0.125
- w_out: bfloat16 [2048, 2048], P('fsdp'), may hold values from -1 to 1
- norm2_gain: bfloat16 [2048], P('fsdp'), may hold values from 0.5 to 1.5
- w_gate: bfloat16 [2048, 5632], P('fsdp'), may hold values from -0.125 to 0.125
- w_up: bfloat16 [2048, 5632], P('fsdp'), may hold values from -0.125 to 0.125
- w_down: bfloat16 [5632, 2048], P('fsdp'), may hold values from -0.078125 to 0.078125
- cotangent: bfloat16 [8, 2048, 2048], P('fsdp', 'context'), may hold values from -6 to 6
Outputs:
- block_out: bfloat16 [8, 2048, 2048], P('fsdp', 'context')
- input_grad: float32 [8, 2048, 2048], P('fsdp', 'context')
- grad_norm1_gain: float32 [2048], P('fsdp')
- grad_w_query: float32 [2048, 256], P('fsdp')
- grad_w_key: float32 [2048, 256], P('fsdp')
- grad_w_value: float32 [2048, 2048], P('fsdp')
- grad_w_out: float32 [2048, 2048], P('fsdp')
- grad_norm2_gain: float32 [2048], P('fsdp')
- grad_w_gate: float32 [2048, 5632], P('fsdp')
- grad_w_up: float32 [2048, 5632], P('fsdp')
- grad_w_down: float32 [5632, 2048], P('fsdp')
The draws below stay inside these ranges and needn't reach their ends.
Inputs may be any that keep to these rules, and one draw needn't show every extreme that they name: `segment_ids`: within each sequence the ids start at 0, never fall and step by one; there are 4 documents of 200 to 1024 tokens, one of exactly 1024.
All inputs are finite; a program needn't handle non-finite values.
Results may differ from the reference program's by a relative error of at most 0.019.
Values may be sent and summed in bfloat16 or wider, within the bound.
No kernel may reach another device: no remote copies, remote signals or barrier semaphores. Data moves between devices by JAX's collectives and lax.ppermute only.
A program may use at most 448 MiB of HBM per device.

```python
import jax
import jax.numpy as jnp
from jax import lax

D = 2048
FF = 5632
HEADS = 16
QK = 16
VH = 128
BLOCK = 512
DOC_MIN = 200
SEQ_LEN = 2048
SEQS = 8
DOCS = 4
DOC_MOST = 1024


def draw_one_sequence(seq_key):
    weight_key, place_key = jax.random.split(seq_key)
    other_docs = DOCS - 1
    spare_tokens = SEQ_LEN - DOC_MOST - other_docs * DOC_MIN
    room_each = DOC_MOST - DOC_MIN
    weights = jax.random.randint(weight_key, (other_docs,), 1, 101, dtype=jnp.int32)
    extra_tokens = jnp.minimum(room_each, spare_tokens * weights // jnp.sum(weights))
    left_over = spare_tokens - jnp.sum(extra_tokens)
    space_left = room_each - extra_tokens
    room_before = jnp.cumsum(space_left) - space_left
    extra_tokens = extra_tokens + jnp.clip(left_over - room_before, 0, space_left)
    rest_lengths = DOC_MIN + extra_tokens
    most_place = jax.random.randint(place_key, (), 0, DOCS, dtype=jnp.int32)
    doc_index = jnp.arange(DOCS, dtype=jnp.int32)
    index_upto = jnp.clip(doc_index, 0, other_docs - 1)
    index_shifted = jnp.clip(doc_index - 1, 0, other_docs - 1)
    lengths = jnp.where(doc_index < most_place, rest_lengths[index_upto], jnp.where(doc_index == most_place, DOC_MOST, rest_lengths[index_shifted]))
    doc_ends = jnp.cumsum(lengths)[:-1]
    positions = jnp.arange(SEQ_LEN, dtype=jnp.int32)
    return jnp.sum((positions[:, None] >= doc_ends[None, :]).astype(jnp.int32), axis=1).astype(jnp.int32)


def draw_segment_ids(key, part):
    seq_keys = jax.random.split(jax.random.fold_in(key, 17), SEQS)
    return jax.vmap(draw_one_sequence)(seq_keys)


def shard_levels(rng, shape, shards, least, largest):
    loudness = 1.0
    for dim, shards_of in shards:
        steps = jax.random.uniform(jax.random.fold_in(jax.random.fold_in(rng, 6), dim), (shards_of,), jnp.float32, least / len(shards), largest / len(shards))
        loudness = loudness * jnp.repeat(jnp.exp(steps), shape[dim] // shards_of).reshape((-1,) + (1,) * (len(shape) - 1 - dim))
    return loudness


def noise(rng, dims, deviation, most, pieces=(), kind=jnp.bfloat16):
    factor_of = shard_levels(rng, dims, pieces, -0.22, 0.18) if pieces else 1.0
    array = jax.random.normal(rng, dims, jnp.float32) * deviation * factor_of
    return jnp.minimum(jnp.maximum(array, -most), most).astype(kind)


def setup_inputs(seed: int = 0) -> dict:
    arg_keys = jax.random.split(jax.random.key(seed), 13)
    tokens = noise(arg_keys[0], (SEQS, SEQ_LEN, D), 1.0, 6.0, ((0, 8), (1, 4)))
    segment_ids = draw_segment_ids(jax.random.fold_in(arg_keys[12], 71), 0)
    norm1_gain = jnp.clip(1.0 + 0.1 * jax.random.normal(arg_keys[2], (D,), jnp.float32), 0.5, 1.5).astype(jnp.bfloat16)
    w_query = noise(arg_keys[3], (D, HEADS * QK), D ** -0.5, 0.125, ((0, 8),))
    w_key = noise(arg_keys[4], (D, HEADS * QK), D ** -0.5, 0.125, ((0, 8),))
    w_value = noise(arg_keys[5], (D, HEADS * VH), D ** -0.5, 0.125, ((0, 8),))
    w_out = noise(arg_keys[6], (HEADS * VH, D), (HEADS * VH // 64) ** -0.5, 1.0, ((0, 8),))
    norm2_gain = jnp.clip(1.0 + 0.1 * jax.random.normal(arg_keys[7], (D,), jnp.float32), 0.5, 1.5).astype(jnp.bfloat16)
    w_gate = noise(arg_keys[8], (D, FF), D ** -0.5, 0.125, ((0, 8),))
    w_up = noise(arg_keys[9], (D, FF), D ** -0.5, 0.125, ((0, 8),))
    w_down = noise(arg_keys[10], (FF, D), FF ** -0.5, 0.078125, ((0, 8),))
    cotangent = noise(arg_keys[11], (SEQS, SEQ_LEN, D), 1.0, 6.0, ((0, 8), (1, 4)))
    return dict(tokens=tokens, segment_ids=segment_ids, norm1_gain=norm1_gain, w_query=w_query, w_key=w_key, w_value=w_value, w_out=w_out, norm2_gain=norm2_gain, w_gate=w_gate, w_up=w_up, w_down=w_down, cotangent=cotangent)


EPS = 1e-05
HIGHEST = lax.Precision.HIGHEST

@jax.custom_vjp
def low(v):
    return lax.optimization_barrier(v.astype(jnp.bfloat16)).astype(jnp.float32)

@jax.custom_vjp
def low_back(v):
    return v

def low_keep(v):
    return (low(v), None)

def low_pass(kept, grad):
    return (grad,)

def back_keep(v):
    return (v, None)

def back_low(kept, grad):
    return (low(grad),)
low.defvjp(low_keep, low_pass)
low_back.defvjp(back_keep, back_low)

def matmul(left, right):
    return jnp.dot(left, right, precision=HIGHEST)

def kernel_block(block_index, queries, key_heads, value_heads, segments):
    first_row = block_index * BLOCK
    query_rows = lax.dynamic_slice_in_dim(queries, first_row, BLOCK, 0)
    segment_rows = lax.dynamic_slice_in_dim(segments, first_row, BLOCK, 0)
    position_rows = first_row + jnp.arange(BLOCK, dtype=jnp.int32)
    positions = jnp.arange(key_heads.shape[0], dtype=jnp.int32)
    allowed = jnp.logical_and(positions[None, :] <= position_rows[:, None], segments[None, :] == segment_rows[:, None])
    scores = jnp.einsum('thd,uhd->htu', query_rows, key_heads, precision=HIGHEST) * QK ** (-0.5)
    weight = jnp.where(allowed[None], 1.0 + scores + 0.5 * scores * scores, 0.0)
    numerator = jnp.einsum('htu,uhv->thv', weight, value_heads, precision=HIGHEST)
    denominator = lax.optimization_barrier(jnp.sum(weight, axis=-1))
    return numerator / jnp.transpose(denominator)[:, :, None]

def attend(queries, key_heads, value_heads, segments):
    block_count = queries.shape[0] // BLOCK

    def one_block(block_index):
        return kernel_block(block_index, queries, key_heads, value_heads, segments)
    blocks = lax.map(jax.checkpoint(one_block), jnp.arange(block_count, dtype=jnp.int32))
    return blocks.reshape(queries.shape[0], HEADS * VH)

def layer(inputs, segments, gain_one, query_w, key_w, value_w, out_w, gain_two, gate_w, up_w, down_w):
    rows_here = inputs.shape[0]
    scale_one = lax.rsqrt(lax.optimization_barrier(jnp.mean(inputs * inputs, axis=-1, keepdims=True)) + EPS)
    normed_one = low(inputs * scale_one * gain_one)
    queries = low_back(low(matmul(normed_one, query_w))).reshape(rows_here, HEADS, QK)
    key_heads = low_back(low(matmul(normed_one, key_w))).reshape(rows_here, HEADS, QK)
    value_heads = low_back(low(matmul(normed_one, value_w))).reshape(rows_here, HEADS, VH)
    mixed_low = low(attend(queries, key_heads, value_heads, segments))
    residual = inputs + low_back(matmul(mixed_low, out_w))
    scale_two = lax.rsqrt(lax.optimization_barrier(jnp.mean(residual * residual, axis=-1, keepdims=True)) + EPS)
    normed_two = low(residual * scale_two * gain_two)
    gate_pre = low_back(matmul(normed_two, gate_w))
    up_pre = low_back(matmul(normed_two, up_w))
    hidden = low(jax.nn.silu(gate_pre) * up_pre)
    return residual + low_back(matmul(hidden, down_w))

def reference(tokens, segment_ids, norm1_gain, w_query, w_key, w_value, w_out, norm2_gain, w_gate, w_up, w_down, cotangent):

    def whole(inputs, gain_one, query_w, key_w, value_w, out_w, gain_two, gate_w, up_w, down_w):

        def one_sequence(paired):
            return layer(paired[0], paired[1], gain_one, query_w, key_w, value_w, out_w, gain_two, gate_w, up_w, down_w)
        return lax.map(one_sequence, (inputs, segment_ids))
    floats = [member.astype(jnp.float32) for member in (tokens, norm1_gain, w_query, w_key, w_value, w_out, norm2_gain, w_gate, w_up, w_down)]
    result, pullback = jax.vjp(whole, *floats)
    grads = pullback(cotangent.astype(jnp.float32))
    return (result.astype(jnp.bfloat16), grads[0], grads[1], grads[2], grads[3], grads[4], grads[5], grads[6], grads[7], grads[8], grads[9])
```

```python
import functools

import jax
import jax.numpy as jnp
from jax import lax
from jax.experimental import pallas as pl
from jax.experimental.pallas import tpu as pltpu
from jax.sharding import PartitionSpec as P

HEADS = 16
QK = 16
VH = 128
EPS = 1e-05

C = "context"
F = "fsdp"
BF = jnp.bfloat16
F32 = jnp.float32


def ring_order(n):
    if n % 2:
        return list(range(n))
    return list(range(0, n, 2)) + list(range(n - 1, 0, -2))


class Ring:
    def __init__(self):
        self.n = n = lax.axis_size(F)
        order = ring_order(n)
        where = [order.index(i) for i in range(n)]
        self.order = jnp.array(order + order, jnp.int32)
        self.pos = jnp.array(where, jnp.int32)[lax.axis_index(F)]
        self.up = [(order[i], order[(i + 1) % n]) for i in range(n)]
        self.down = [(b, a) for a, b in self.up]

    def member(self, distance):
        return self.order[lax.rem(self.pos + distance + self.n, self.n)]

    def paths(self, flip):
        long, short = self.n // 2, (self.n - 1) // 2
        if flip:
            long, short = short, long
        return ((self.up, 1, long), (self.down, -1, short))

    def gather(self, block, flip=False):
        out = jnp.zeros((self.n,) + block.shape, block.dtype)
        out = lax.dynamic_update_index_in_dim(out, block, lax.axis_index(F), 0)
        for perm, sign, steps in self.paths(flip):
            moving = block
            for d in range(1, steps + 1):
                moving = lax.ppermute(moving, F, perm)
                out = lax.dynamic_update_index_in_dim(out, moving, self.member(-sign * d), 0)
        return out

    def scatter_sum(self, stacked, flip=False):
        def part(index):
            return lax.dynamic_index_in_dim(stacked, index, 0, keepdims=False)

        total = part(lax.axis_index(F)).astype(F32)
        for perm, sign, steps in self.paths(flip):
            if not steps:
                continue
            moving = part(self.member(sign * steps))
            for d in range(steps - 1, -1, -1):
                arrived = lax.ppermute(moving, F, perm)
                if d:
                    moving = (
                        arrived.astype(F32) + part(self.member(sign * d)).astype(F32)
                    ).astype(stacked.dtype)
                else:
                    total = total + arrived.astype(F32)
        return total


def chips():
    return lax.axis_size(C) // 2


def core_swap(value):
    n = lax.axis_size(C)
    return lax.ppermute(value, C, [(i, i ^ 1) for i in range(n)])


def chip_shift(value, k):
    n = lax.axis_size(C)
    return lax.ppermute(value, C, [(i, (i + 2 * k) % n) for i in range(n)])


def spread(block):
    out = []
    for k in range(chips()):
        near = chip_shift(block, k) if k else block
        out += [near, core_swap(near)]
    return out


def spread_index():
    n, me = lax.axis_size(C), lax.axis_index(C)
    out = []
    for k in range(chips()):
        near = lax.rem(me - 2 * k + n, n)
        out += [near, near ^ 1]
    return out


def gather_back(parts):
    total = None
    for k in range(chips()):
        mine = parts[2 * k].astype(F32) + core_swap(parts[2 * k + 1].astype(BF)).astype(F32)
        if k:
            mine = chip_shift(mine.astype(BF), -k).astype(F32)
        total = mine if total is None else total + mine
    return total


def in_order(parts):
    out = jnp.zeros((len(parts),) + parts[0].shape, parts[0].dtype)
    for index, part in zip(spread_index(), parts):
        out = lax.dynamic_update_index_in_dim(out, part, index, 0)
    return out


def group_pairs(back):
    nc, nf = lax.axis_size(C), lax.axis_size(F)
    m = nf // nc
    out = []
    for q in range(nc):
        pairs = [
            (c * nf + m * c + s, c * nf + s * nc + q) for c in range(nc) for s in range(m)
        ]
        out.append([(b, a) for a, b in pairs] if back else pairs)
    return out


def group_pieces(shard):
    nc = lax.axis_size(C)
    rows = shard.shape[0] // nc
    out = None
    for q, pairs in enumerate(group_pairs(False)):
        got = lax.ppermute(shard[q * rows : (q + 1) * rows], (C, F), pairs)
        out = got if out is None else out + got
    return out


def ungroup_pieces(piece):
    nc, nf = lax.axis_size(C), lax.axis_size(F)
    m = nf // nc
    shard = jnp.concatenate(
        [lax.ppermute(piece, (C, F), pairs) for pairs in group_pairs(True)], axis=0
    )
    out = shard
    for k in range(1, nc // 2):
        out = out + lax.ppermute(
            shard, (C, F), [((j // m) * nf + j, ((j // m + 2 * k) % nc) * nf + j) for j in range(nf)]
        )
    holders = [((j // m) % 2, j) for j in range(nf)]
    swap = [
        ((2 * x + h) * nf + j, (2 * x + 1 - h) * nf + j) for h, j in holders for x in range(nc // 2)
    ]
    return out + lax.ppermute(out, (C, F), swap)


def dot_nt(a, b):
    return lax.dot_general(a, b, (((1,), (1,)), ((), ())), preferred_element_type=F32)


def dot_nn(a, b):
    return lax.dot_general(a, b, (((1,), (0,)), ((), ())), preferred_element_type=F32)


def with_one(values, width):
    rows = values.shape[0]
    padded = jnp.concatenate([values, jnp.zeros((rows, 128 - width), values.dtype)], axis=1)
    lane = lax.broadcasted_iota(jnp.int32, (rows, 128), 1)
    return jnp.where(lane == width, jnp.ones_like(padded), padded)


def one_head(values, head, width):
    lane = lax.broadcasted_iota(jnp.int32, values.shape, 1)
    keep = jnp.logical_or(lane // QK == head, lane == width)
    return jnp.where(keep, values, jnp.zeros_like(values))


def needed(meta, a, b, nb):
    before = meta[b] < meta[a]
    return jnp.logical_and(before, meta[nb + a] <= meta[2 * nb + b])


def forward_kernel(meta, qkv, seg_col, seg_row, mixed, den, num_sum, den_sum, *, heads, rows, nb):
    width = heads * QK
    a = pl.program_id(0)
    here = pl.ds(pl.multiple_of(a * rows, rows), rows)
    queries = with_one(qkv[here, :width] * 0.25, width)
    seg_q = seg_col[here, :]
    num_sum[...] = jnp.zeros_like(num_sum)
    den_sum[...] = jnp.zeros_like(den_sum)

    def pair(b, diagonal):
        there = pl.ds(pl.multiple_of(b * rows, rows), rows)
        keys = with_one(qkv[there, width : 2 * width], width)
        allowed = seg_q == seg_row[b]
        if diagonal:
            t = lax.broadcasted_iota(jnp.int32, (rows, rows), 0)
            u = lax.broadcasted_iota(jnp.int32, (rows, rows), 1)
            allowed = jnp.logical_and(allowed, u <= t)
        for h in range(heads):
            shifted = dot_nt(one_head(queries, h, width), keys)
            weight = jnp.where(allowed, shifted * shifted + 1.0, 0.0)
            lanes = slice(h * VH, (h + 1) * VH)
            values = qkv[there, 2 * width + h * VH : 2 * width + (h + 1) * VH]
            num_sum[:, lanes] += dot_nn(weight.astype(BF), values)
            den_sum[:, lanes] += jnp.broadcast_to(
                jnp.sum(weight, axis=1, keepdims=True), (rows, VH)
            )

    pair(a, True)

    @pl.loop(0, nb)
    def _(b):
        @pl.when(needed(meta, a, b, nb))
        def _():
            pair(b, False)

    mixed[...] = (num_sum[...] / den_sum[...]).astype(BF)
    for h in range(heads):
        den[:, h : h + 1] = den_sum[:, h * VH : h * VH + 1]


def backward_kernel(
    meta, qkv, seg_col, seg_row, gm, mixed, den, scale, out, key_sum, value_sum, query_sum, *, heads, rows, nb
):
    width = heads * QK
    a = pl.program_id(0)
    here = pl.ds(pl.multiple_of(a * rows, rows), rows)
    queries = with_one(qkv[here, :width] * 0.25, width)
    seg_q = seg_row[a]

    @pl.when(a == 0)
    def _():
        key_sum[...] = jnp.zeros_like(key_sum)
        value_sum[...] = jnp.zeros_like(value_sum)
        query_sum[...] = jnp.zeros_like(query_sum)

    grads, offsets, head_queries = [], [], []
    for h in range(heads):
        g = gm[:, h * VH : (h + 1) * VH].astype(F32)
        d = den[:, h : h + 1]
        grads.append((g / d).astype(BF))
        inner = -jnp.sum(g * mixed[:, h * VH : (h + 1) * VH].astype(F32), axis=1, keepdims=True) / d
        offsets.append(jnp.transpose(jnp.broadcast_to(inner, (rows, 128)))[0:1, :])
        head_queries.append(one_head(queries, h, width))

    def pair(b, diagonal):
        there = pl.ds(pl.multiple_of(b * rows, rows), rows)
        raw = qkv[there, width : 2 * width]
        keys = with_one(raw, width)
        turned = jnp.transpose(keys)
        allowed = seg_col[there, :] == seg_q
        if diagonal:
            u = lax.broadcasted_iota(jnp.int32, (rows, rows), 0)
            t = lax.broadcasted_iota(jnp.int32, (rows, rows), 1)
            allowed = jnp.logical_and(allowed, u <= t)
        for h in range(heads):
            lanes = slice(h * VH, (h + 1) * VH)
            shifted = dot_nt(keys, head_queries[h])
            weight = jnp.where(allowed, shifted * shifted + 1.0, 0.0).astype(BF)
            value_sum[there, lanes] += dot_nn(weight, grads[h])
            values = qkv[there, 2 * width + h * VH : 2 * width + (h + 1) * VH]
            grad = dot_nt(values, grads[h]) + offsets[h]
            score = jnp.where(allowed, grad * shifted, 0.0).astype(BF)
            key_sum[there, :] += dot_nn(score, head_queries[h])
            query_sum[a, h * QK : (h + 1) * QK, :] += dot_nn(turned[h * QK : (h + 1) * QK, :], score)

    pair(a, True)

    @pl.loop(0, nb)
    def _(b):
        @pl.when(needed(meta, a, b, nb))
        def _():
            pair(b, False)

    @pl.when(a == nb - 1)
    def _():
        for b in range(nb):
            span = slice(b * rows, (b + 1) * rows)
            s = scale[span, :]
            grad_q = jnp.transpose(query_sum[b]) * (0.5 * s)
            out[span, :width] = grad_q.astype(BF)
            out[span, width : 2 * width] = (key_sum[span, :width] * (2.0 * s)).astype(BF)
            out[span, 2 * width :] = (value_sum[span, :] * s).astype(BF)


def block_spec(shape, index):
    return pl.BlockSpec(shape, index)


def whole(shape):
    return pl.BlockSpec(shape, lambda a, *_: (0,) * len(shape))


def attention_forward(meta, qkv, seg_col, seg_row, heads, rows):
    tokens = qkv.shape[0]
    nb = tokens // rows
    values = heads * VH
    return pl.pallas_call(
        functools.partial(forward_kernel, heads=heads, rows=rows, nb=nb),
        out_shape=(
            jax.ShapeDtypeStruct((tokens, values), BF),
            jax.ShapeDtypeStruct((tokens, heads), F32),
        ),
        grid_spec=pltpu.PrefetchScalarGridSpec(
            num_scalar_prefetch=1,
            grid=(nb,),
            in_specs=[whole(qkv.shape), whole(seg_col.shape), whole(seg_row.shape)],
            out_specs=[
                pl.BlockSpec((rows, values), lambda a, *_: (a, 0)),
                pl.BlockSpec((rows, heads), lambda a, *_: (a, 0)),
            ],
            scratch_shapes=[pltpu.VMEM((rows, values), F32), pltpu.VMEM((rows, values), F32)],
        ),
        cost_estimate=pl.CostEstimate(
            flops=4 * tokens * tokens * values, transcendentals=0, bytes_accessed=8 * tokens * values
        ),
        name="attention_forward",
    )(meta, qkv, seg_col, seg_row)


def attention_backward(meta, qkv, seg_col, seg_row, gm, mixed, den, scale, heads, rows):
    tokens = qkv.shape[0]
    nb = tokens // rows
    values = heads * VH
    width = heads * QK
    return pl.pallas_call(
        functools.partial(backward_kernel, heads=heads, rows=rows, nb=nb),
        out_shape=jax.ShapeDtypeStruct((tokens, 2 * width + values), BF),
        grid_spec=pltpu.PrefetchScalarGridSpec(
            num_scalar_prefetch=1,
            grid=(nb,),
            in_specs=[
                whole(qkv.shape),
                whole(seg_col.shape),
                whole(seg_row.shape),
                pl.BlockSpec((rows, values), lambda a, *_: (a, 0)),
                pl.BlockSpec((rows, values), lambda a, *_: (a, 0)),
                pl.BlockSpec((rows, heads), lambda a, *_: (a, 0)),
                whole(scale.shape),
            ],
            out_specs=whole((tokens, 2 * width + values)),
            scratch_shapes=[
                pltpu.VMEM((tokens, 128), F32),
                pltpu.VMEM((tokens, values), F32),
                pltpu.VMEM((nb, width, rows), F32),
            ],
        ),
        cost_estimate=pl.CostEstimate(
            flops=10 * tokens * tokens * values, transcendentals=0, bytes_accessed=16 * tokens * values
        ),
        name="attention_backward",
    )(meta, qkv, seg_col, seg_row, gm, mixed, den, scale)


def mm(a, b):
    return jnp.dot(a, b, preferred_element_type=F32)


def mm_tn(a, b):
    return lax.dot_general(a, b, (((0,), (0,)), ((), ())), preferred_element_type=F32)


def mm_nt(a, b):
    return lax.dot_general(a, b, (((1,), (1,)), ((), ())), preferred_element_type=F32)


def inverse_rms(values):
    return lax.rsqrt(jnp.mean(values * values, axis=-1, keepdims=True) + EPS)


def local(
    tokens,
    segment_ids,
    norm1_gain,
    w_query,
    w_key,
    w_value,
    w_out,
    norm2_gain,
    w_gate,
    w_up,
    w_down,
    cotangent,
):
    nc, nf = lax.axis_size(C), lax.axis_size(F)
    c = lax.axis_index(C)
    ring = Ring()
    rows, width = tokens.shape[1], tokens.shape[2]
    heads = HEADS // nc
    qk = heads * QK
    hidden_all = w_gate.shape[1]
    seg_len = hidden_all // (nc * nf)
    hidden = seg_len * nf
    shard = w_gate.shape[0]

    own = tokens[0]
    grad_top = cotangent[0]
    gain_one = norm1_gain.astype(F32)[:, None]
    gain_two = norm2_gain.astype(F32)[:, None]

    def columns(weight, size):
        return lax.dynamic_slice_in_dim(weight, c * size, size, axis=1)

    part_qkv = (
        jnp.concatenate(
            [columns(w_query, qk), columns(w_key, qk), columns(w_value, heads * VH)], axis=1
        ).astype(F32)
        * gain_one
    ).astype(BF)

    def hidden_columns(weight):
        picked = lax.dynamic_index_in_dim(
            weight.reshape(shard, nf, nc, seg_len), c, axis=2, keepdims=False
        )
        return (picked.reshape(shard, hidden).astype(F32) * gain_two).astype(BF)

    part_out = group_pieces(w_out)
    part_gate = hidden_columns(w_gate)
    part_up = hidden_columns(w_up)
    part_down = lax.dynamic_slice_in_dim(w_down, c * seg_len, seg_len, axis=0)

    x_all = jnp.concatenate(spread(own), axis=0)
    seg_all = jnp.concatenate(spread(segment_ids[0]), axis=0)
    g_all = jnp.concatenate(spread(grad_top), axis=0)
    nb = nc
    seg_row = seg_all.reshape(nb, 1, rows)
    seg_col = seg_all.reshape(nb * rows, 1)
    meta = jnp.concatenate(
        [jnp.stack(spread_index()), seg_row[:, 0, 0], seg_row[:, 0, rows - 1]]
    ).astype(jnp.int32)

    full_qkv = ring.gather(part_qkv).reshape(width, -1)
    full_out = ring.gather(part_out, True).reshape(heads * VH, width)
    x_all32 = x_all.astype(F32)
    scale_one = inverse_rms(x_all32)
    qkv = (mm(x_all, full_qkv) * scale_one).astype(BF)
    mixed, den = attention_forward(meta, qkv, seg_col, seg_row, heads, rows)

    def blocks(value):
        return [value[i * rows : (i + 1) * rows] for i in range(nb)]

    residual = own.astype(F32) + gather_back(blocks(mm(mixed, full_out).astype(BF)))

    scale_two = inverse_rms(residual)
    unit_two = residual * scale_two
    n_all = jnp.concatenate(spread(unit_two.astype(BF)), axis=0)
    full_gate = ring.gather(part_gate).reshape(width, hidden)
    full_up = ring.gather(part_up, True).reshape(width, hidden)
    full_down = ring.gather(part_down).reshape(hidden, width)
    gate = mm(n_all, full_gate)
    up = mm(n_all, full_up)
    sigmoid = jax.nn.sigmoid(gate)
    silu = gate * sigmoid
    act = (silu * up).astype(BF)
    block_out = residual + gather_back(blocks(mm(act, full_down).astype(BF)))

    grad_hidden = mm_nt(g_all, full_down)
    grad_gate = (grad_hidden * up * sigmoid * (1.0 + gate * (1.0 - sigmoid))).astype(BF)
    grad_up = (grad_hidden * silu).astype(BF)
    grad_unit_two = gather_back(
        blocks((mm_nt(grad_gate, full_gate) + mm_nt(grad_up, full_up)).astype(BF))
    )
    sum_down = ring.scatter_sum(mm_tn(act, g_all).astype(BF).reshape(nf, seg_len, width))
    sum_gate = ring.scatter_sum(mm_tn(n_all, grad_gate).astype(BF).reshape(nf, shard, hidden))
    sum_up = ring.scatter_sum(mm_tn(n_all, grad_up).astype(BF).reshape(nf, shard, hidden), True)

    grad_residual = grad_top.astype(F32) + scale_two * (
        grad_unit_two - unit_two * jnp.mean(grad_unit_two * unit_two, axis=-1, keepdims=True)
    )
    b_all = jnp.concatenate(spread(grad_residual.astype(BF)), axis=0)

    grad_mixed = mm_nt(b_all, full_out)
    sum_out = ring.scatter_sum(
        mm_tn(mixed, b_all).astype(BF).reshape(nf, (heads * VH) // nf, width), True
    )
    grad_qkv = attention_backward(
        meta, qkv, seg_col, seg_row, grad_mixed, mixed, den, scale_one, heads, rows
    )
    grad_unit_one = gather_back(blocks(mm_nt(grad_qkv, full_qkv).astype(BF)))
    sum_qkv = ring.scatter_sum(mm_tn(x_all, grad_qkv).astype(BF).reshape(nf, shard, -1))

    unit_one = own.astype(F32) * inverse_rms(own.astype(F32))
    input_grad = grad_residual + grad_unit_one - unit_one * jnp.mean(
        grad_unit_one * unit_one, axis=-1, keepdims=True
    )

    def over_context(value):
        return in_order(spread(value.astype(BF)))

    def from_hidden(stacked):
        return (
            stacked.reshape(nc, shard, nf, seg_len)
            .transpose(1, 2, 0, 3)
            .reshape(shard, hidden_all)
            .astype(F32)
        )

    def side_by_side(stacked):
        return stacked.transpose(1, 0, 2).reshape(stacked.shape[1], -1).astype(F32)

    all_down = over_context(sum_down).reshape(nc * seg_len, width).astype(F32)
    all_gate = from_hidden(over_context(sum_gate))
    all_up = from_hidden(over_context(sum_up))
    all_qkv = over_context(sum_qkv)
    all_query = side_by_side(all_qkv[:, :, :qk])
    all_key = side_by_side(all_qkv[:, :, qk : 2 * qk])
    all_value = side_by_side(all_qkv[:, :, 2 * qk :])
    all_out = ungroup_pieces(sum_out.astype(BF)).astype(F32)

    def along(weight, grad):
        return jnp.sum(weight.astype(F32) * grad, axis=1)

    grad_gain_one = along(w_query, all_query) + along(w_key, all_key) + along(w_value, all_value)
    grad_gain_two = along(w_gate, all_gate) + along(w_up, all_up)
    return (
        block_out.astype(BF)[None],
        input_grad[None],
        grad_gain_one,
        all_query * gain_one,
        all_key * gain_one,
        all_value * gain_one,
        all_out,
        grad_gain_two,
        all_gate * gain_two,
        all_up * gain_two,
        all_down,
    )


def solution(mesh):
    rows = P(F, None)
    acts = P(F, C, None)
    return jax.shard_map(
        local,
        mesh=mesh,
        in_specs=(acts, P(F, C), P(F), rows, rows, rows, rows, P(F), rows, rows, rows, acts),
        out_specs=(acts, acts, P(F), rows, rows, rows, rows, P(F), rows, rows, rows),
        check_vma=False,
    )
```

```python
import functools

import jax
import jax.numpy as jnp
from jax import lax
from jax.experimental import pallas as pl
from jax.experimental.pallas import tpu as pltpu
from jax.sharding import PartitionSpec as P

HEADS = 16
QK = 16
VH = 128
EPS = 1e-05

C = "context"
F = "fsdp"
BF = jnp.bfloat16
F32 = jnp.float32


def after(value, *earlier):
    return lax.optimization_barrier((value,) + earlier)[0]


def lines():
    return lax.axis_size(F) // 2


def line_shift(value, k):
    n, m = lax.axis_size(F), lines()
    return lax.ppermute(value, F, [(j, (j // 2 + k) % m * 2 + j % 2) for j in range(n)])


def side_swap(value):
    return lax.ppermute(value, F, [(j, j ^ 1) for j in range(lax.axis_size(F))])


def line_and_side():
    me = lax.axis_index(F)
    return me // 2, lax.rem(me, 2)


def interleave(own, other):
    n, m = lax.axis_size(F), lines()
    line, side = line_and_side()
    both = jnp.concatenate([own, other], axis=0)
    size = both.shape[0] // n
    places = [
        lax.rem(j // 2 - line + m, m) + m * jnp.where(side == j % 2, 0, 1) for j in range(n)
    ]
    return jnp.concatenate(
        [lax.dynamic_slice_in_dim(both, p * size, size, axis=0) for p in places], axis=0
    )


def scatter_sides(total):
    m = lines()
    _, side = line_and_side()
    parts = total.reshape(m, 2, total.shape[0] // (2 * m), total.shape[1])
    mine = lax.dynamic_index_in_dim(parts, side, 1, keepdims=False)
    return mine, side_swap(lax.dynamic_index_in_dim(parts, 1 - side, 1, keepdims=False))


def scatter_lines(total):
    m = lines()
    line, _ = line_and_side()

    def part(k):
        return lax.dynamic_index_in_dim(total, lax.rem(line + k, m), 0, keepdims=False)

    return [part(0)] + [line_shift(part(k), k) for k in range(1, m)]


def gather_all(block):
    return lax.all_gather(block, F, axis=0, tiled=True)


def scatter_all(total):
    return lax.psum_scatter(total, F, scatter_dimension=0, tiled=True)


def add_all(parts):
    total = parts[0].astype(F32)
    for part in parts[1:]:
        total = total + part.astype(F32)
    return total


def chips():
    return lax.axis_size(C) // 2


def core_swap(value):
    n = lax.axis_size(C)
    return lax.ppermute(value, C, [(i, i ^ 1) for i in range(n)])


def chip_shift(value, k):
    n = lax.axis_size(C)
    return lax.ppermute(value, C, [(i, (i + 2 * k) % n) for i in range(n)])


def spread(block):
    out = []
    for k in range(chips()):
        near = chip_shift(block, k) if k else block
        out += [near, core_swap(near)]
    return out


def spread_index():
    n, me = lax.axis_size(C), lax.axis_index(C)
    out = []
    for k in range(chips()):
        near = lax.rem(me - 2 * k + n, n)
        out += [near, near ^ 1]
    return out


def add_cores(parts):
    sums = []
    for k in range(chips()):
        both = parts[2 * k].astype(F32) + core_swap(parts[2 * k + 1]).astype(F32)
        sums.append(both.astype(BF) if k else both)
    return sums


def add_chips(sums):
    total = sums[0]
    for k in range(1, chips()):
        total = total + chip_shift(sums[k], -k).astype(F32)
    return total


def gather_back(parts):
    return add_chips(add_cores(parts))


def in_order(parts):
    out = jnp.zeros((len(parts),) + parts[0].shape, parts[0].dtype)
    for index, part in zip(spread_index(), parts):
        out = lax.dynamic_update_index_in_dim(out, part, index, 0)
    return out


def group_pairs(back):
    nc, nf = lax.axis_size(C), lax.axis_size(F)
    m = nf // nc
    out = []
    for q in range(nc):
        pairs = [
            (c * nf + m * c + s, c * nf + s * nc + q) for c in range(nc) for s in range(m)
        ]
        out.append([(b, a) for a, b in pairs] if back else pairs)
    return out


def group_pieces(shard):
    nc = lax.axis_size(C)
    rows = shard.shape[0] // nc
    out = None
    for q, pairs in enumerate(group_pairs(False)):
        got = lax.ppermute(shard[q * rows : (q + 1) * rows], (C, F), pairs)
        out = got if out is None else out + got
    return out


def ungroup_pieces(piece):
    nc, nf = lax.axis_size(C), lax.axis_size(F)
    m = nf // nc
    shard = jnp.concatenate(
        [lax.ppermute(piece, (C, F), pairs) for pairs in group_pairs(True)], axis=0
    )
    out = shard
    for k in range(1, nc // 2):
        out = out + lax.ppermute(
            shard, (C, F), [((j // m) * nf + j, ((j // m + 2 * k) % nc) * nf + j) for j in range(nf)]
        )
    holders = [((j // m) % 2, j) for j in range(nf)]
    swap = [
        ((2 * x + h) * nf + j, (2 * x + 1 - h) * nf + j) for h, j in holders for x in range(nc // 2)
    ]
    return out + lax.ppermute(out, (C, F), swap)


def dot_nt(a, b):
    return lax.dot_general(a, b, (((1,), (1,)), ((), ())), preferred_element_type=F32)


def dot_nn(a, b):
    return lax.dot_general(a, b, (((1,), (0,)), ((), ())), preferred_element_type=F32)


def with_one(values, width):
    rows = values.shape[0]
    padded = jnp.concatenate([values, jnp.zeros((rows, 128 - width), values.dtype)], axis=1)
    lane = lax.broadcasted_iota(jnp.int32, (rows, 128), 1)
    return jnp.where(lane == width, jnp.ones_like(padded), padded)


def one_head(values, head, width):
    lane = lax.broadcasted_iota(jnp.int32, values.shape, 1)
    keep = jnp.logical_or(lane // QK == head, lane == width)
    return jnp.where(keep, values, jnp.zeros_like(values))


def needed(meta, a, b, nb):
    before = meta[b] < meta[a]
    return jnp.logical_and(before, meta[nb + a] <= meta[2 * nb + b])


def forward_kernel(meta, qkv, seg_col, seg_row, mixed, den, num_sum, den_sum, *, heads, rows, nb):
    width = heads * QK
    a = pl.program_id(0)
    here = pl.ds(pl.multiple_of(a * rows, rows), rows)
    queries = with_one(qkv[here, :width] * 0.25, width)
    seg_q = seg_col[here, :]
    num_sum[...] = jnp.zeros_like(num_sum)
    den_sum[...] = jnp.zeros_like(den_sum)

    def pair(b, diagonal):
        there = pl.ds(pl.multiple_of(b * rows, rows), rows)
        keys = with_one(qkv[there, width : 2 * width], width)
        allowed = seg_q == seg_row[b]
        if diagonal:
            t = lax.broadcasted_iota(jnp.int32, (rows, rows), 0)
            u = lax.broadcasted_iota(jnp.int32, (rows, rows), 1)
            allowed = jnp.logical_and(allowed, u <= t)
        for h in range(heads):
            shifted = dot_nt(one_head(queries, h, width), keys)
            weight = jnp.where(allowed, shifted * shifted + 1.0, 0.0)
            lanes = slice(h * VH, (h + 1) * VH)
            values = qkv[there, 2 * width + h * VH : 2 * width + (h + 1) * VH]
            num_sum[:, lanes] += dot_nn(weight.astype(BF), values)
            den_sum[:, lanes] += jnp.broadcast_to(
                jnp.sum(weight, axis=1, keepdims=True), (rows, VH)
            )

    pair(a, True)

    @pl.loop(0, nb)
    def _(b):
        @pl.when(needed(meta, a, b, nb))
        def _():
            pair(b, False)

    mixed[...] = (num_sum[...] / den_sum[...]).astype(BF)
    for h in range(heads):
        den[:, h : h + 1] = den_sum[:, h * VH : h * VH + 1]


def backward_kernel(
    meta, qkv, seg_col, seg_row, gm, mixed, den, scale, out, key_sum, value_sum, query_sum, *, heads, rows, nb
):
    width = heads * QK
    a = pl.program_id(0)
    here = pl.ds(pl.multiple_of(a * rows, rows), rows)
    queries = with_one(qkv[here, :width] * 0.25, width)
    seg_q = seg_row[a]

    @pl.when(a == 0)
    def _():
        key_sum[...] = jnp.zeros_like(key_sum)
        value_sum[...] = jnp.zeros_like(value_sum)
        query_sum[...] = jnp.zeros_like(query_sum)

    grads, offsets, head_queries = [], [], []
    for h in range(heads):
        g = gm[:, h * VH : (h + 1) * VH].astype(F32)
        d = den[:, h : h + 1]
        grads.append((g / d).astype(BF))
        inner = -jnp.sum(g * mixed[:, h * VH : (h + 1) * VH].astype(F32), axis=1, keepdims=True) / d
        offsets.append(jnp.transpose(jnp.broadcast_to(inner, (rows, 128)))[0:1, :])
        head_queries.append(one_head(queries, h, width))

    def pair(b, diagonal):
        there = pl.ds(pl.multiple_of(b * rows, rows), rows)
        raw = qkv[there, width : 2 * width]
        keys = with_one(raw, width)
        turned = jnp.transpose(keys)
        allowed = seg_col[there, :] == seg_q
        if diagonal:
            u = lax.broadcasted_iota(jnp.int32, (rows, rows), 0)
            t = lax.broadcasted_iota(jnp.int32, (rows, rows), 1)
            allowed = jnp.logical_and(allowed, u <= t)
        for h in range(heads):
            lanes = slice(h * VH, (h + 1) * VH)
            shifted = dot_nt(keys, head_queries[h])
            weight = jnp.where(allowed, shifted * shifted + 1.0, 0.0).astype(BF)
            value_sum[there, lanes] += dot_nn(weight, grads[h])
            values = qkv[there, 2 * width + h * VH : 2 * width + (h + 1) * VH]
            grad = dot_nt(values, grads[h]) + offsets[h]
            score = jnp.where(allowed, grad * shifted, 0.0).astype(BF)
            key_sum[there, :] += dot_nn(score, head_queries[h])
            query_sum[a, h * QK : (h + 1) * QK, :] += dot_nn(turned[h * QK : (h + 1) * QK, :], score)

    pair(a, True)

    @pl.loop(0, nb)
    def _(b):
        @pl.when(needed(meta, a, b, nb))
        def _():
            pair(b, False)

    @pl.when(a == nb - 1)
    def _():
        for b in range(nb):
            span = slice(b * rows, (b + 1) * rows)
            s = scale[span, :]
            grad_q = jnp.transpose(query_sum[b]) * (0.5 * s)
            out[span, :width] = grad_q.astype(BF)
            out[span, width : 2 * width] = (key_sum[span, :width] * (2.0 * s)).astype(BF)
            out[span, 2 * width :] = (value_sum[span, :] * s).astype(BF)


def block_spec(shape, index):
    return pl.BlockSpec(shape, index)


def whole(shape):
    return pl.BlockSpec(shape, lambda a, *_: (0,) * len(shape))


def attention_forward(meta, qkv, seg_col, seg_row, heads, rows):
    tokens = qkv.shape[0]
    nb = tokens // rows
    values = heads * VH
    return pl.pallas_call(
        functools.partial(forward_kernel, heads=heads, rows=rows, nb=nb),
        out_shape=(
            jax.ShapeDtypeStruct((tokens, values), BF),
            jax.ShapeDtypeStruct((tokens, heads), F32),
        ),
        grid_spec=pltpu.PrefetchScalarGridSpec(
            num_scalar_prefetch=1,
            grid=(nb,),
            in_specs=[whole(qkv.shape), whole(seg_col.shape), whole(seg_row.shape)],
            out_specs=[
                pl.BlockSpec((rows, values), lambda a, *_: (a, 0)),
                pl.BlockSpec((rows, heads), lambda a, *_: (a, 0)),
            ],
            scratch_shapes=[pltpu.VMEM((rows, values), F32), pltpu.VMEM((rows, values), F32)],
        ),
        cost_estimate=pl.CostEstimate(
            flops=4 * tokens * values, transcendentals=0, bytes_accessed=8 * tokens
        ),
        name="attention_forward",
    )(meta, qkv, seg_col, seg_row)


def attention_backward(meta, qkv, seg_col, seg_row, gm, mixed, den, scale, heads, rows):
    tokens = qkv.shape[0]
    nb = tokens // rows
    values = heads * VH
    width = heads * QK
    return pl.pallas_call(
        functools.partial(backward_kernel, heads=heads, rows=rows, nb=nb),
        out_shape=jax.ShapeDtypeStruct((tokens, 2 * width + values), BF),
        grid_spec=pltpu.PrefetchScalarGridSpec(
            num_scalar_prefetch=1,
            grid=(nb,),
            in_specs=[
                whole(qkv.shape),
                whole(seg_col.shape),
                whole(seg_row.shape),
                pl.BlockSpec((rows, values), lambda a, *_: (a, 0)),
                pl.BlockSpec((rows, values), lambda a, *_: (a, 0)),
                pl.BlockSpec((rows, heads), lambda a, *_: (a, 0)),
                whole(scale.shape),
            ],
            out_specs=whole((tokens, 2 * width + values)),
            scratch_shapes=[
                pltpu.VMEM((tokens, 128), F32),
                pltpu.VMEM((tokens, values), F32),
                pltpu.VMEM((nb, width, rows), F32),
            ],
        ),
        cost_estimate=pl.CostEstimate(
            flops=10 * tokens * values, transcendentals=0, bytes_accessed=16 * tokens
        ),
        name="attention_backward",
    )(meta, qkv, seg_col, seg_row, gm, mixed, den, scale)


def mm(a, b):
    return jnp.dot(a, b, preferred_element_type=F32)


def mm_tn(a, b):
    return lax.dot_general(a, b, (((0,), (0,)), ((), ())), preferred_element_type=F32)


def mm_nt(a, b):
    return lax.dot_general(a, b, (((1,), (1,)), ((), ())), preferred_element_type=F32)


def inverse_rms(values):
    return lax.rsqrt(jnp.mean(values * values, axis=-1, keepdims=True) + EPS)


def local(
    tokens,
    segment_ids,
    norm1_gain,
    w_query,
    w_key,
    w_value,
    w_out,
    norm2_gain,
    w_gate,
    w_up,
    w_down,
    cotangent,
):
    nc, nf = lax.axis_size(C), lax.axis_size(F)
    c = lax.axis_index(C)
    rows, width = tokens.shape[1], tokens.shape[2]
    heads = HEADS // nc
    qk = heads * QK
    hidden_all = w_gate.shape[1]
    seg_len = hidden_all // (nc * nf)
    hidden = seg_len * nf
    shard = w_gate.shape[0]

    own = tokens[0]
    grad_top = cotangent[0]
    gain_one = norm1_gain.astype(F32)[:, None]
    gain_two = norm2_gain.astype(F32)[:, None]

    def columns(weight, size):
        return lax.dynamic_slice_in_dim(weight, c * size, size, axis=1)

    part_qkv = (
        jnp.concatenate(
            [columns(w_query, qk), columns(w_key, qk), columns(w_value, heads * VH)], axis=1
        ).astype(F32)
        * gain_one
    ).astype(BF)

    def hidden_columns(weight):
        picked = lax.dynamic_index_in_dim(
            weight.reshape(shard, nf, nc, seg_len), c, axis=2, keepdims=False
        )
        return (picked.reshape(shard, hidden).astype(F32) * gain_two).astype(BF)

    part_out = group_pieces(w_out)
    part_gate = hidden_columns(w_gate)
    part_up = hidden_columns(w_up)
    part_down = lax.dynamic_slice_in_dim(w_down, c * seg_len, seg_len, axis=0)

    seg_all = jnp.concatenate(spread(segment_ids[0]), axis=0)
    nb = nc
    seg_row = seg_all.reshape(nb, 1, rows)
    seg_col = seg_all.reshape(nb * rows, 1)
    meta = jnp.concatenate(
        [jnp.stack(spread_index()), seg_row[:, 0, 0], seg_row[:, 0, rows - 1]]
    ).astype(jnp.int32)

    full_qkv = gather_all(part_qkv)
    full_out = gather_all(part_out)
    full_gate = gather_all(part_gate)
    full_up = gather_all(part_up)
    down_lines = [line_shift(part_down, -k) for k in range(1, lax.axis_size(F) // 2)]

    x_all = jnp.concatenate(spread(own), axis=0)
    scale_one = inverse_rms(x_all.astype(F32))
    qkv = (mm(after(x_all, *down_lines[:2]), full_qkv) * scale_one).astype(BF)
    g_parts = spread(grad_top)
    qkv = after(qkv, *down_lines)
    down_side = jnp.concatenate([part_down] + down_lines, axis=0)
    down_other = side_swap(down_side)
    mixed, den = attention_forward(meta, qkv, seg_col, seg_row, heads, rows)

    def blocks(value):
        return [value[i * rows : (i + 1) * rows] for i in range(nb)]

    projected = mm(after(mixed, *g_parts), full_out).astype(BF)
    residual = own.astype(F32) + gather_back(blocks(projected))

    scale_two = inverse_rms(residual)
    unit_two = residual * scale_two
    n_all = jnp.concatenate(spread(unit_two.astype(BF)), axis=0)
    full_down = interleave(down_side, down_other)
    g_all = jnp.concatenate(g_parts, axis=0)
    grad_hidden = mm_nt(g_all, full_down)
    gate = mm(after(n_all, grad_hidden), full_gate)
    up = mm(n_all, full_up)
    sigmoid = jax.nn.sigmoid(gate)
    silu = gate * sigmoid
    act = (silu * up).astype(BF)
    grad_gate = (grad_hidden * up * sigmoid * (1.0 + gate * (1.0 - sigmoid))).astype(BF)
    grad_up = (grad_hidden * silu).astype(BF)
    projected_two = mm(act, full_down).astype(BF)
    out_sums = add_cores(blocks(projected_two))
    grad_gate = after(grad_gate, projected_two)
    back_two = (mm_nt(grad_gate, full_gate) + mm_nt(grad_up, full_up)).astype(BF)
    block_out = residual + add_chips(out_sums)
    back_sums = add_cores(blocks(after(back_two, block_out)))

    total_down = mm_tn(after(act, back_two), g_all).astype(BF)
    sum_down = scatter_all(total_down)
    total_gate = mm_tn(n_all, after(grad_gate, total_down, *back_sums)).astype(BF)
    mine_gate, sent_gate = scatter_sides(total_gate)
    total_up = mm_tn(n_all, after(grad_up, total_gate)).astype(BF)
    mine_up, sent_up = scatter_sides(total_up)
    grad_unit_two = add_chips([after(back_sums[0], total_up)] + back_sums[1:])

    grad_residual = grad_top.astype(F32) + scale_two * (
        grad_unit_two - unit_two * jnp.mean(grad_unit_two * unit_two, axis=-1, keepdims=True)
    )
    branch = grad_residual.astype(BF)
    b_all = jnp.concatenate(spread(branch), axis=0)

    def both(mine, sent):
        return (mine.astype(F32) + sent.astype(F32)).astype(BF)

    both_gate = both(mine_gate, after(sent_gate, branch))
    lines_gate = scatter_lines(both_gate)

    b_all = after(b_all, both_gate)
    total_out = mm_tn(mixed, b_all).astype(BF)
    grad_mixed = mm_nt(after(b_all, total_out), full_out)
    grad_qkv = attention_backward(
        meta, qkv, seg_col, seg_row, grad_mixed, mixed, den, scale_one, heads, rows
    )
    both_up = both(mine_up, after(sent_up, grad_qkv))
    lines_up = scatter_lines(both_up)
    grad_qkv = after(grad_qkv, sum_down, both_up, *lines_gate)
    sum_out = scatter_all(after(total_out, grad_qkv))
    back_one = mm_nt(grad_qkv, full_qkv).astype(BF)
    one_sums = add_cores(blocks(back_one))
    total_qkv = mm_tn(x_all, after(grad_qkv, *one_sums)).astype(BF)
    grad_unit_one = add_chips(one_sums)
    sum_qkv = scatter_all(total_qkv)
    sum_down = after(sum_down, total_qkv)
    sum_gate = add_all([after(lines_gate[0], grad_unit_one)] + lines_gate[1:])
    sum_up = add_all([after(lines_up[0], grad_unit_one)] + lines_up[1:])

    unit_one = own.astype(F32) * inverse_rms(own.astype(F32))
    input_grad = grad_residual + grad_unit_one - unit_one * jnp.mean(
        grad_unit_one * unit_one, axis=-1, keepdims=True
    )

    def over_context(value):
        return in_order(spread(value.astype(BF)))

    def from_hidden(stacked):
        return (
            stacked.reshape(nc, shard, nf, seg_len)
            .transpose(1, 2, 0, 3)
            .reshape(shard, hidden_all)
            .astype(F32)
        )

    def side_by_side(stacked):
        return stacked.transpose(1, 0, 2).reshape(stacked.shape[1], -1).astype(F32)

    all_down = over_context(sum_down).reshape(nc * seg_len, width).astype(F32)
    all_gate = from_hidden(over_context(sum_gate))
    all_up = from_hidden(over_context(sum_up))
    all_qkv = over_context(sum_qkv)
    all_query = side_by_side(all_qkv[:, :, :qk])
    all_key = side_by_side(all_qkv[:, :, qk : 2 * qk])
    all_value = side_by_side(all_qkv[:, :, 2 * qk :])
    all_out = ungroup_pieces(sum_out.astype(BF)).astype(F32)

    def along(weight, grad):
        return jnp.sum(weight.astype(F32) * grad, axis=1)

    grad_gain_one = along(w_query, all_query) + along(w_key, all_key) + along(w_value, all_value)
    grad_gain_two = along(w_gate, all_gate) + along(w_up, all_up)
    return (
        block_out.astype(BF)[None],
        input_grad[None],
        grad_gain_one,
        all_query * gain_one,
        all_key * gain_one,
        all_value * gain_one,
        all_out,
        grad_gain_two,
        all_gate * gain_two,
        all_up * gain_two,
        all_down,
    )


def solution(mesh):
    rows = P(F, None)
    acts = P(F, C, None)
    return jax.shard_map(
        local,
        mesh=mesh,
        in_specs=(acts, P(F, C), P(F), rows, rows, rows, rows, P(F), rows, rows, rows, acts),
        out_specs=(acts, acts, P(F), rows, rows, rows, rows, P(F), rows, rows, rows),
        check_vma=False,
    )
```

```python
import functools

import jax
import jax.numpy as jnp
from jax import lax
from jax.experimental import pallas as pl
from jax.experimental.pallas import tpu as pltpu
from jax.sharding import PartitionSpec as P

HEADS = 16
QK = 16
VH = 128
EPS = 1e-05

C = "context"
F = "fsdp"
BF = jnp.bfloat16
F32 = jnp.float32


def after(value, *earlier):
    return lax.optimization_barrier((value,) + earlier)[0]


def lines():
    return lax.axis_size(F) // 2


def line_shift(value, k):
    n, m = lax.axis_size(F), lines()
    return lax.ppermute(value, F, [(j, (j // 2 + k) % m * 2 + j % 2) for j in range(n)])


def side_swap(value):
    return lax.ppermute(value, F, [(j, j ^ 1) for j in range(lax.axis_size(F))])


def line_and_side():
    me = lax.axis_index(F)
    return me // 2, lax.rem(me, 2)


class Arrivals:
    def __init__(self, block):
        self.own = [block] + [line_shift(block, -k) for k in range(1, lines())]
        self.other = [side_swap(part) for part in self.own]

    def first(self, own, other):
        m = lines()
        return self.own[1 : own * m // 4] + self.other[: other * m // 4]

    def whole(self):
        return assemble(self.own + self.other)


def assemble_kernel(*refs, n):
    m = n // 2
    me = lax.axis_index(F)
    line, side = me // 2, lax.rem(me, 2)
    out, sems = refs[n], refs[n + 1]
    copies = []
    for a in range(2):
        for k in range(m):
            place = lax.rem(line + k, m) * 2 + (side if a == 0 else 1 - side)
            i = a * m + k
            copies.append(pltpu.make_async_copy(refs[i], out.at[place], sems.at[i]))
    for copy in copies:
        copy.start()
    for copy in copies:
        copy.wait()


def assemble(parts):
    n = len(parts)
    shape = parts[0].shape
    out = pl.pallas_call(
        functools.partial(assemble_kernel, n=n),
        out_shape=jax.ShapeDtypeStruct((n,) + shape, parts[0].dtype),
        in_specs=[pl.BlockSpec(memory_space=pl.ANY)] * n,
        out_specs=pl.BlockSpec(memory_space=pl.ANY),
        scratch_shapes=[pltpu.SemaphoreType.DMA((n,))],
        cost_estimate=pl.CostEstimate(flops=0, transcendentals=0, bytes_accessed=1024),
        name="assemble",
    )(*parts)
    return out.reshape(n * shape[0], shape[1])


class Departures:
    def __init__(self, total):
        m = lines()
        line, side = line_and_side()
        parts = total.reshape(2 * m, total.shape[0] // (2 * m), total.shape[1])

        def part(k, s):
            place = lax.rem(line + k, m) * 2 + s
            return lax.dynamic_index_in_dim(parts, place, 0, keepdims=False)

        self.order = list(range(1, m)) + [0]
        self.mine = [part(k, side) for k in self.order]
        self.sent = [side_swap(part(k, 1 - side)) for k in self.order]

    def lines(self, marks):
        out = []
        for k, mine, sent, mark in zip(self.order, self.mine, self.sent, marks):
            both = (mine.astype(F32) + after(sent, mark).astype(F32)).astype(BF)
            out.append(line_shift(both, k) if k else both)
        return out


def gather_all(block):
    return lax.all_gather(block, F, axis=0, tiled=True)


def scatter_all(total):
    return lax.psum_scatter(total, F, scatter_dimension=0, tiled=True)


def add_all(parts):
    total = parts[0].astype(F32)
    for part in parts[1:]:
        total = total + part.astype(F32)
    return total


def chips():
    return lax.axis_size(C) // 2


def core_swap(value):
    n = lax.axis_size(C)
    return lax.ppermute(value, C, [(i, i ^ 1) for i in range(n)])


def chip_shift(value, k):
    n = lax.axis_size(C)
    return lax.ppermute(value, C, [(i, (i + 2 * k) % n) for i in range(n)])


def spread(block, marks=()):
    out = []
    for k in range(chips()):
        near = after(chip_shift(block, k), *marks) if k else block
        out += [near, core_swap(near)]
    return out


def spread_direct(block):
    n = lax.axis_size(C)
    return [
        lax.ppermute(block, C, [(i, (i + 2 * k) % n ^ h) for i in range(n)]) if k or h else block
        for k in range(chips())
        for h in range(2)
    ]


def spread_index():
    n, me = lax.axis_size(C), lax.axis_index(C)
    out = []
    for k in range(chips()):
        near = lax.rem(me - 2 * k + n, n)
        out += [near, near ^ 1]
    return out


def add_cores(parts):
    sums = []
    for k in range(chips()):
        both = parts[2 * k].astype(F32) + core_swap(parts[2 * k + 1]).astype(F32)
        sums.append(both.astype(BF) if k else both)
    return sums


def add_chips(sums):
    total = sums[0]
    for k in range(1, chips()):
        total = total + chip_shift(sums[k], -k).astype(F32)
    return total


def gather_back(parts):
    return add_chips(add_cores(parts))


def in_order(parts):
    out = jnp.zeros((len(parts),) + parts[0].shape, parts[0].dtype)
    for index, part in zip(spread_index(), parts):
        out = lax.dynamic_update_index_in_dim(out, part, index, 0)
    return out


def group_pairs(back):
    nc, nf = lax.axis_size(C), lax.axis_size(F)
    m = nf // nc
    out = []
    for q in range(nc):
        pairs = [
            (c * nf + m * c + s, c * nf + s * nc + q) for c in range(nc) for s in range(m)
        ]
        out.append([(b, a) for a, b in pairs] if back else pairs)
    return out


def group_pieces(shard):
    nc = lax.axis_size(C)
    rows = shard.shape[0] // nc
    out = None
    for q, pairs in enumerate(group_pairs(False)):
        got = lax.ppermute(shard[q * rows : (q + 1) * rows], (C, F), pairs)
        out = got if out is None else out + got
    return out


def ungroup_pieces(piece):
    nc, nf = lax.axis_size(C), lax.axis_size(F)
    m = nf // nc
    shard = jnp.concatenate(
        [lax.ppermute(piece, (C, F), pairs) for pairs in group_pairs(True)], axis=0
    )
    out = shard
    for k in range(1, nc // 2):
        out = out + lax.ppermute(
            shard, (C, F), [((j // m) * nf + j, ((j // m + 2 * k) % nc) * nf + j) for j in range(nf)]
        )
    holders = [((j // m) % 2, j) for j in range(nf)]
    swap = [
        ((2 * x + h) * nf + j, (2 * x + 1 - h) * nf + j) for h, j in holders for x in range(nc // 2)
    ]
    return out + lax.ppermute(out, (C, F), swap)


def dot_nt(a, b):
    return lax.dot_general(a, b, (((1,), (1,)), ((), ())), preferred_element_type=F32)


def dot_nn(a, b):
    return lax.dot_general(a, b, (((1,), (0,)), ((), ())), preferred_element_type=F32)


def with_one(values, width):
    rows = values.shape[0]
    padded = jnp.concatenate([values, jnp.zeros((rows, 128 - width), values.dtype)], axis=1)
    lane = lax.broadcasted_iota(jnp.int32, (rows, 128), 1)
    return jnp.where(lane == width, jnp.ones_like(padded), padded)


def one_head(values, head, width):
    lane = lax.broadcasted_iota(jnp.int32, values.shape, 1)
    keep = jnp.logical_or(lane // QK == head, lane == width)
    return jnp.where(keep, values, jnp.zeros_like(values))


def needed(meta, a, b, nb):
    before = meta[b] < meta[a]
    return jnp.logical_and(before, meta[nb + a] <= meta[2 * nb + b])


def forward_kernel(meta, qkv, seg_col, seg_row, mixed, den, num_sum, den_sum, *, heads, rows, nb):
    width = heads * QK
    a = pl.program_id(0)
    here = pl.ds(pl.multiple_of(a * rows, rows), rows)
    queries = with_one(qkv[here, :width] * 0.25, width)
    seg_q = seg_col[here, :]
    num_sum[...] = jnp.zeros_like(num_sum)
    den_sum[...] = jnp.zeros_like(den_sum)

    def pair(b, diagonal):
        there = pl.ds(pl.multiple_of(b * rows, rows), rows)
        keys = with_one(qkv[there, width : 2 * width], width)
        allowed = seg_q == seg_row[b]
        if diagonal:
            t = lax.broadcasted_iota(jnp.int32, (rows, rows), 0)
            u = lax.broadcasted_iota(jnp.int32, (rows, rows), 1)
            allowed = jnp.logical_and(allowed, u <= t)
        for h in range(heads):
            shifted = dot_nt(one_head(queries, h, width), keys)
            weight = jnp.where(allowed, shifted * shifted + 1.0, 0.0)
            lanes = slice(h * VH, (h + 1) * VH)
            values = qkv[there, 2 * width + h * VH : 2 * width + (h + 1) * VH]
            num_sum[:, lanes] += dot_nn(weight.astype(BF), values)
            den_sum[:, lanes] += jnp.broadcast_to(
                jnp.sum(weight, axis=1, keepdims=True), (rows, VH)
            )

    pair(a, True)

    @pl.loop(0, nb)
    def _(b):
        @pl.when(needed(meta, a, b, nb))
        def _():
            pair(b, False)

    mixed[...] = (num_sum[...] / den_sum[...]).astype(BF)
    for h in range(heads):
        den[:, h : h + 1] = den_sum[:, h * VH : h * VH + 1]


def backward_kernel(
    meta, qkv, seg_col, seg_row, gm, mixed, den, scale, out, key_sum, value_sum, query_sum, *, heads, rows, nb
):
    width = heads * QK
    a = pl.program_id(0)
    here = pl.ds(pl.multiple_of(a * rows, rows), rows)
    queries = with_one(qkv[here, :width] * 0.25, width)
    seg_q = seg_row[a]

    @pl.when(a == 0)
    def _():
        key_sum[...] = jnp.zeros_like(key_sum)
        value_sum[...] = jnp.zeros_like(value_sum)
        query_sum[...] = jnp.zeros_like(query_sum)

    grads, offsets, head_queries = [], [], []
    for h in range(heads):
        g = gm[:, h * VH : (h + 1) * VH].astype(F32)
        d = den[:, h : h + 1]
        grads.append((g / d).astype(BF))
        inner = -jnp.sum(g * mixed[:, h * VH : (h + 1) * VH].astype(F32), axis=1, keepdims=True) / d
        offsets.append(jnp.transpose(jnp.broadcast_to(inner, (rows, 128)))[0:1, :])
        head_queries.append(one_head(queries, h, width))

    def pair(b, diagonal):
        there = pl.ds(pl.multiple_of(b * rows, rows), rows)
        raw = qkv[there, width : 2 * width]
        keys = with_one(raw, width)
        turned = jnp.transpose(keys)
        allowed = seg_col[there, :] == seg_q
        if diagonal:
            u = lax.broadcasted_iota(jnp.int32, (rows, rows), 0)
            t = lax.broadcasted_iota(jnp.int32, (rows, rows), 1)
            allowed = jnp.logical_and(allowed, u <= t)
        for h in range(heads):
            lanes = slice(h * VH, (h + 1) * VH)
            shifted = dot_nt(keys, head_queries[h])
            weight = jnp.where(allowed, shifted * shifted + 1.0, 0.0).astype(BF)
            value_sum[there, lanes] += dot_nn(weight, grads[h])
            values = qkv[there, 2 * width + h * VH : 2 * width + (h + 1) * VH]
            grad = dot_nt(values, grads[h]) + offsets[h]
            score = jnp.where(allowed, grad * shifted, 0.0).astype(BF)
            key_sum[there, :] += dot_nn(score, head_queries[h])
            query_sum[a, h * QK : (h + 1) * QK, :] += dot_nn(turned[h * QK : (h + 1) * QK, :], score)

    pair(a, True)

    @pl.loop(0, nb)
    def _(b):
        @pl.when(needed(meta, a, b, nb))
        def _():
            pair(b, False)

    @pl.when(a == nb - 1)
    def _():
        for b in range(nb):
            span = slice(b * rows, (b + 1) * rows)
            s = scale[span, :]
            grad_q = jnp.transpose(query_sum[b]) * (0.5 * s)
            out[span, :width] = grad_q.astype(BF)
            out[span, width : 2 * width] = (key_sum[span, :width] * (2.0 * s)).astype(BF)
            out[span, 2 * width :] = (value_sum[span, :] * s).astype(BF)


def block_spec(shape, index):
    return pl.BlockSpec(shape, index)


def whole(shape):
    return pl.BlockSpec(shape, lambda a, *_: (0,) * len(shape))


def attention_forward(meta, qkv, seg_col, seg_row, heads, rows):
    tokens = qkv.shape[0]
    nb = tokens // rows
    values = heads * VH
    return pl.pallas_call(
        functools.partial(forward_kernel, heads=heads, rows=rows, nb=nb),
        out_shape=(
            jax.ShapeDtypeStruct((tokens, values), BF),
            jax.ShapeDtypeStruct((tokens, heads), F32),
        ),
        grid_spec=pltpu.PrefetchScalarGridSpec(
            num_scalar_prefetch=1,
            grid=(nb,),
            in_specs=[whole(qkv.shape), whole(seg_col.shape), whole(seg_row.shape)],
            out_specs=[
                pl.BlockSpec((rows, values), lambda a, *_: (a, 0)),
                pl.BlockSpec((rows, heads), lambda a, *_: (a, 0)),
            ],
            scratch_shapes=[pltpu.VMEM((rows, values), F32), pltpu.VMEM((rows, values), F32)],
        ),
        cost_estimate=pl.CostEstimate(
            flops=4 * tokens * values, transcendentals=0, bytes_accessed=8 * tokens
        ),
        name="attention_forward",
    )(meta, qkv, seg_col, seg_row)


def attention_backward(meta, qkv, seg_col, seg_row, gm, mixed, den, scale, heads, rows):
    tokens = qkv.shape[0]
    nb = tokens // rows
    values = heads * VH
    width = heads * QK
    return pl.pallas_call(
        functools.partial(backward_kernel, heads=heads, rows=rows, nb=nb),
        out_shape=jax.ShapeDtypeStruct((tokens, 2 * width + values), BF),
        grid_spec=pltpu.PrefetchScalarGridSpec(
            num_scalar_prefetch=1,
            grid=(nb,),
            in_specs=[
                whole(qkv.shape),
                whole(seg_col.shape),
                whole(seg_row.shape),
                pl.BlockSpec((rows, values), lambda a, *_: (a, 0)),
                pl.BlockSpec((rows, values), lambda a, *_: (a, 0)),
                pl.BlockSpec((rows, heads), lambda a, *_: (a, 0)),
                whole(scale.shape),
            ],
            out_specs=whole((tokens, 2 * width + values)),
            scratch_shapes=[
                pltpu.VMEM((tokens, 128), F32),
                pltpu.VMEM((tokens, values), F32),
                pltpu.VMEM((nb, width, rows), F32),
            ],
        ),
        cost_estimate=pl.CostEstimate(
            flops=10 * tokens * values, transcendentals=0, bytes_accessed=16 * tokens
        ),
        name="attention_backward",
    )(meta, qkv, seg_col, seg_row, gm, mixed, den, scale)


def mm(a, b):
    return jnp.dot(a, b, preferred_element_type=F32)


def mm_tn(a, b):
    return lax.dot_general(a, b, (((0,), (0,)), ((), ())), preferred_element_type=F32)


def mm_nt(a, b):
    return lax.dot_general(a, b, (((1,), (1,)), ((), ())), preferred_element_type=F32)


def inverse_rms(values):
    return lax.rsqrt(jnp.mean(values * values, axis=-1, keepdims=True) + EPS)


def local(
    tokens,
    segment_ids,
    norm1_gain,
    w_query,
    w_key,
    w_value,
    w_out,
    norm2_gain,
    w_gate,
    w_up,
    w_down,
    cotangent,
):
    nc, nf = lax.axis_size(C), lax.axis_size(F)
    c = lax.axis_index(C)
    rows, width = tokens.shape[1], tokens.shape[2]
    heads = HEADS // nc
    qk = heads * QK
    hidden_all = w_gate.shape[1]
    seg_len = hidden_all // (nc * nf)
    hidden = seg_len * nf
    shard = w_gate.shape[0]

    own = tokens[0]
    grad_top = cotangent[0]
    gain_one = norm1_gain.astype(F32)[:, None]
    gain_two = norm2_gain.astype(F32)[:, None]

    def columns(weight, size):
        return lax.dynamic_slice_in_dim(weight, c * size, size, axis=1)

    part_qkv = (
        jnp.concatenate(
            [columns(w_query, qk), columns(w_key, qk), columns(w_value, heads * VH)], axis=1
        ).astype(F32)
        * gain_one
    ).astype(BF)

    def hidden_columns(weight):
        picked = lax.dynamic_index_in_dim(
            weight.reshape(shard, nf, nc, seg_len), c, axis=2, keepdims=False
        )
        return (picked.reshape(shard, hidden).astype(F32) * gain_two).astype(BF)

    part_out = group_pieces(w_out)
    part_gate = hidden_columns(w_gate)
    part_up = hidden_columns(w_up)
    part_down = lax.dynamic_slice_in_dim(w_down, c * seg_len, seg_len, axis=0)

    seg_all = jnp.concatenate(spread_direct(segment_ids[0]), axis=0)
    nb = nc
    seg_row = seg_all.reshape(nb, 1, rows)
    seg_col = seg_all.reshape(nb * rows, 1)
    meta = jnp.concatenate(
        [jnp.stack(spread_index()), seg_row[:, 0, 0], seg_row[:, 0, rows - 1]]
    ).astype(jnp.int32)

    w_one, w_two = Arrivals(part_qkv), Arrivals(part_out)
    w_three, w_four, w_five = Arrivals(part_down), Arrivals(part_gate), Arrivals(part_up)

    x_all = jnp.concatenate(spread(own, w_one.first(4, 0)), axis=0)
    scale_one = inverse_rms(x_all.astype(F32))
    full_qkv = w_one.whole()
    x_all = after(x_all, *w_two.first(3, 1))
    qkv = (mm(x_all, full_qkv) * scale_one).astype(BF)
    g_parts = spread(grad_top)
    qkv = after(qkv, *w_two.first(4, 3), *w_three.first(2, 0))
    mixed, den = attention_forward(meta, qkv, seg_col, seg_row, heads, rows)

    def blocks(value):
        return [value[i * rows : (i + 1) * rows] for i in range(nb)]

    full_out = w_two.whole()
    projected = mm(after(mixed, *g_parts, *w_three.first(3, 2)), full_out).astype(BF)
    sums = add_cores(blocks(projected))
    residual = own.astype(F32) + add_chips(sums)
    residual = after(residual, *w_three.first(4, 4), *w_four.first(2, 2))

    scale_two = inverse_rms(residual)
    unit_two = residual * scale_two
    full_down = w_three.whole()
    g_all = jnp.concatenate(g_parts, axis=0)
    grad_hidden = mm_nt(after(g_all, unit_two), full_down)
    n_parts = spread(unit_two.astype(BF), [grad_hidden] + w_four.first(4, 3))
    n_all = jnp.concatenate(n_parts, axis=0)
    full_gate = w_four.whole()
    gate = mm(n_all, full_gate)
    full_up = w_five.whole()
    up = mm(n_all, full_up)
    sigmoid = jax.nn.sigmoid(gate)
    silu = gate * sigmoid
    act = (silu * up).astype(BF)
    grad_gate = (grad_hidden * up * sigmoid * (1.0 + gate * (1.0 - sigmoid))).astype(BF)
    grad_up = (grad_hidden * silu).astype(BF)
    back_two = (mm_nt(grad_gate, full_gate) + mm_nt(grad_up, full_up)).astype(BF)
    back_sums = add_cores(blocks(back_two))

    total_gate = mm_tn(n_all, after(grad_gate, back_two)).astype(BF)
    away_gate = Departures(total_gate)
    total_up = mm_tn(n_all, after(grad_up, total_gate, *back_sums)).astype(BF)
    away_up = Departures(total_up)
    total_down = mm_tn(after(act, total_up, away_gate.sent[0]), g_all).astype(BF)
    sum_down = scatter_all(total_down)
    grad_unit_two = after(add_chips(back_sums), total_down, away_gate.sent[1])

    grad_residual = grad_top.astype(F32) + scale_two * (
        grad_unit_two - unit_two * jnp.mean(grad_unit_two * unit_two, axis=-1, keepdims=True)
    )
    branch = grad_residual.astype(BF)
    projected_two = mm(after(act, branch), full_down).astype(BF)
    m = nf // 2
    lines_gate = away_gate.lines([branch] * m)
    b_parts = spread(branch, [projected_two, away_up.sent[0]] + away_gate.sent)
    b_all = jnp.concatenate(b_parts, axis=0)
    out_sums = add_cores(blocks(after(projected_two, b_all)))
    block_out = residual + add_chips(out_sums)

    total_out = mm_tn(mixed, b_all).astype(BF)
    grad_mixed = mm_nt(after(b_all, total_out, away_up.sent[1 % m]), full_out)
    sum_out = scatter_all(after(total_out, sum_down))
    grad_mixed = after(grad_mixed, sum_down, away_up.sent[2 % m], *out_sums)
    grad_qkv = attention_backward(
        meta, qkv, seg_col, seg_row, grad_mixed, mixed, den, scale_one, heads, rows
    )
    lines_up = away_up.lines([branch, b_all, grad_mixed] + [grad_qkv] * (m - 3))
    back_one = mm_nt(after(grad_qkv, block_out, *lines_gate), full_qkv).astype(BF)
    one_sums = add_cores(blocks(back_one))
    total_qkv = mm_tn(x_all, after(grad_qkv, *one_sums)).astype(BF)
    grad_unit_one = add_chips(one_sums)
    sum_qkv = scatter_all(total_qkv)
    sum_down = after(sum_down, total_qkv)
    sum_gate = add_all([after(lines_gate[0], total_qkv)] + lines_gate[1:])
    sum_up = add_all([after(lines_up[0], grad_unit_one)] + lines_up[1:])

    unit_one = own.astype(F32) * inverse_rms(own.astype(F32))
    input_grad = grad_residual + grad_unit_one - unit_one * jnp.mean(
        grad_unit_one * unit_one, axis=-1, keepdims=True
    )

    def over_context(value):
        return in_order(spread(value.astype(BF)))

    def from_hidden(stacked):
        return (
            stacked.reshape(nc, shard, nf, seg_len)
            .transpose(1, 2, 0, 3)
            .reshape(shard, hidden_all)
            .astype(F32)
        )

    def side_by_side(stacked):
        return stacked.transpose(1, 0, 2).reshape(stacked.shape[1], -1).astype(F32)

    all_down = over_context(sum_down).reshape(nc * seg_len, width).astype(F32)
    all_gate = from_hidden(over_context(sum_gate))
    all_up = from_hidden(over_context(sum_up))
    all_qkv = over_context(sum_qkv)
    all_query = side_by_side(all_qkv[:, :, :qk])
    all_key = side_by_side(all_qkv[:, :, qk : 2 * qk])
    all_value = side_by_side(all_qkv[:, :, 2 * qk :])
    all_out = ungroup_pieces(sum_out.astype(BF)).astype(F32)

    def along(weight, grad):
        return jnp.sum(weight.astype(F32) * grad, axis=1)

    grad_gain_one = along(w_query, all_query) + along(w_key, all_key) + along(w_value, all_value)
    grad_gain_two = along(w_gate, all_gate) + along(w_up, all_up)
    return (
        block_out.astype(BF)[None],
        input_grad[None],
        grad_gain_one,
        all_query * gain_one,
        all_key * gain_one,
        all_value * gain_one,
        all_out,
        grad_gain_two,
        all_gate * gain_two,
        all_up * gain_two,
        all_down,
    )


def solution(mesh):
    rows = P(F, None)
    acts = P(F, C, None)
    return jax.shard_map(
        local,
        mesh=mesh,
        in_specs=(acts, P(F, C), P(F), rows, rows, rows, rows, P(F), rows, rows, rows, acts),
        out_specs=(acts, acts, P(F), rows, rows, rows, rows, P(F), rows, rows, rows),
        check_vma=False,
    )
```

```python
import functools

import jax
import jax.numpy as jnp
from jax import lax
from jax.experimental import pallas as pl
from jax.experimental.pallas import tpu as pltpu
from jax.sharding import PartitionSpec as P

HEADS = 16
QK = 16
VH = 128
EPS = 1e-05

C = "context"
F = "fsdp"
BF = jnp.bfloat16
F32 = jnp.float32


def after(value, *earlier):
    return lax.optimization_barrier((value,) + earlier)[0]


def lines():
    return lax.axis_size(F) // 2


def line_shift(value, k):
    n, m = lax.axis_size(F), lines()
    return lax.ppermute(value, F, [(j, (j // 2 + k) % m * 2 + j % 2) for j in range(n)])


def side_swap(value):
    return lax.ppermute(value, F, [(j, j ^ 1) for j in range(lax.axis_size(F))])


def line_and_side():
    me = lax.axis_index(F)
    return me // 2, lax.rem(me, 2)


def scatter_sides(total):
    m = lines()
    _, side = line_and_side()
    parts = total.reshape(m, 2, total.shape[0] // (2 * m), total.shape[1])
    mine = lax.dynamic_index_in_dim(parts, side, 1, keepdims=False)
    return mine, side_swap(lax.dynamic_index_in_dim(parts, 1 - side, 1, keepdims=False))


def scatter_lines(mine, sent):
    m = lines()
    line, _ = line_and_side()
    total = (mine.astype(F32) + sent.astype(F32)).astype(BF)

    def part(k):
        return lax.dynamic_index_in_dim(total, lax.rem(line + k, m), 0, keepdims=False)

    return [part(0)] + [line_shift(part(k), k) for k in range(1, m)]


def gather_all(block):
    return lax.all_gather(block, F, axis=0, tiled=True)


def scatter_all(total):
    return lax.psum_scatter(total, F, scatter_dimension=0, tiled=True)


def add_all(parts):
    total = parts[0].astype(F32)
    for part in parts[1:]:
        total = total + part.astype(F32)
    return total


def chips():
    return lax.axis_size(C) // 2


def core_swap(value):
    n = lax.axis_size(C)
    return lax.ppermute(value, C, [(i, i ^ 1) for i in range(n)])


def chip_shift(value, k):
    n = lax.axis_size(C)
    return lax.ppermute(value, C, [(i, (i + 2 * k) % n) for i in range(n)])


def spread(block, marks=()):
    out = []
    for k in range(chips()):
        near = after(chip_shift(block, k), *marks) if k else block
        out += [near, core_swap(near)]
    return out


def spread_direct(block):
    n = lax.axis_size(C)
    return [
        lax.ppermute(block, C, [(i, (i + 2 * k) % n ^ h) for i in range(n)]) if k or h else block
        for k in range(chips())
        for h in range(2)
    ]


def spread_index():
    n, me = lax.axis_size(C), lax.axis_index(C)
    out = []
    for k in range(chips()):
        near = lax.rem(me - 2 * k + n, n)
        out += [near, near ^ 1]
    return out


def add_cores(parts):
    sums = []
    for k in range(chips()):
        both = parts[2 * k].astype(F32) + core_swap(parts[2 * k + 1]).astype(F32)
        sums.append(both.astype(BF) if k else both)
    return sums


def add_chips(sums):
    total = sums[0]
    for k in range(1, chips()):
        total = total + chip_shift(sums[k], -k).astype(F32)
    return total


def gather_back(parts):
    return add_chips(add_cores(parts))


def in_order(parts):
    out = jnp.zeros((len(parts),) + parts[0].shape, parts[0].dtype)
    for index, part in zip(spread_index(), parts):
        out = lax.dynamic_update_index_in_dim(out, part, index, 0)
    return out


def group_pairs(back):
    nc, nf = lax.axis_size(C), lax.axis_size(F)
    m = nf // nc
    out = []
    for q in range(nc):
        pairs = [
            (c * nf + m * c + s, c * nf + s * nc + q) for c in range(nc) for s in range(m)
        ]
        out.append([(b, a) for a, b in pairs] if back else pairs)
    return out


def group_pieces(shard):
    nc = lax.axis_size(C)
    rows = shard.shape[0] // nc
    out = None
    for q, pairs in enumerate(group_pairs(False)):
        got = lax.ppermute(shard[q * rows : (q + 1) * rows], (C, F), pairs)
        out = got if out is None else out + got
    return out


def ungroup_pieces(piece):
    nc, nf = lax.axis_size(C), lax.axis_size(F)
    m = nf // nc
    shard = jnp.concatenate(
        [lax.ppermute(piece, (C, F), pairs) for pairs in group_pairs(True)], axis=0
    )
    out = shard
    for k in range(1, nc // 2):
        out = out + lax.ppermute(
            shard, (C, F), [((j // m) * nf + j, ((j // m + 2 * k) % nc) * nf + j) for j in range(nf)]
        )
    holders = [((j // m) % 2, j) for j in range(nf)]
    swap = [
        ((2 * x + h) * nf + j, (2 * x + 1 - h) * nf + j) for h, j in holders for x in range(nc // 2)
    ]
    return out + lax.ppermute(out, (C, F), swap)


def dot_nt(a, b):
    return lax.dot_general(a, b, (((1,), (1,)), ((), ())), preferred_element_type=F32)


def dot_nn(a, b):
    return lax.dot_general(a, b, (((1,), (0,)), ((), ())), preferred_element_type=F32)


def with_one(values, width):
    rows = values.shape[0]
    padded = jnp.concatenate([values, jnp.zeros((rows, 128 - width), values.dtype)], axis=1)
    lane = lax.broadcasted_iota(jnp.int32, (rows, 128), 1)
    return jnp.where(lane == width, jnp.ones_like(padded), padded)


def one_head(values, head, width):
    lane = lax.broadcasted_iota(jnp.int32, values.shape, 1)
    keep = jnp.logical_or(lane // QK == head, lane == width)
    return jnp.where(keep, values, jnp.zeros_like(values))


def needed(meta, a, b, nb):
    before = meta[b] < meta[a]
    return jnp.logical_and(before, meta[nb + a] <= meta[2 * nb + b])


def forward_kernel(meta, qkv, seg_col, seg_row, mixed, den, num_sum, den_sum, *, heads, rows, nb):
    width = heads * QK
    a = pl.program_id(0)
    here = pl.ds(pl.multiple_of(a * rows, rows), rows)
    queries = with_one(qkv[here, :width] * 0.25, width)
    seg_q = seg_col[here, :]
    num_sum[...] = jnp.zeros_like(num_sum)
    den_sum[...] = jnp.zeros_like(den_sum)

    def pair(b, diagonal):
        there = pl.ds(pl.multiple_of(b * rows, rows), rows)
        keys = with_one(qkv[there, width : 2 * width], width)
        allowed = seg_q == seg_row[b]
        if diagonal:
            t = lax.broadcasted_iota(jnp.int32, (rows, rows), 0)
            u = lax.broadcasted_iota(jnp.int32, (rows, rows), 1)
            allowed = jnp.logical_and(allowed, u <= t)
        for h in range(heads):
            shifted = dot_nt(one_head(queries, h, width), keys)
            weight = jnp.where(allowed, shifted * shifted + 1.0, 0.0)
            lanes = slice(h * VH, (h + 1) * VH)
            values = qkv[there, 2 * width + h * VH : 2 * width + (h + 1) * VH]
            num_sum[:, lanes] += dot_nn(weight.astype(BF), values)
            den_sum[:, lanes] += jnp.broadcast_to(
                jnp.sum(weight, axis=1, keepdims=True), (rows, VH)
            )

    pair(a, True)

    @pl.loop(0, nb)
    def _(b):
        @pl.when(needed(meta, a, b, nb))
        def _():
            pair(b, False)

    mixed[...] = (num_sum[...] / den_sum[...]).astype(BF)
    for h in range(heads):
        den[:, h : h + 1] = den_sum[:, h * VH : h * VH + 1]


def backward_kernel(
    meta, qkv, seg_col, seg_row, gm, mixed, den, scale, out, key_sum, value_sum, query_sum, *, heads, rows, nb
):
    width = heads * QK
    a = pl.program_id(0)
    here = pl.ds(pl.multiple_of(a * rows, rows), rows)
    queries = with_one(qkv[here, :width] * 0.25, width)
    seg_q = seg_row[a]

    @pl.when(a == 0)
    def _():
        key_sum[...] = jnp.zeros_like(key_sum)
        value_sum[...] = jnp.zeros_like(value_sum)
        query_sum[...] = jnp.zeros_like(query_sum)

    grads, offsets, head_queries = [], [], []
    for h in range(heads):
        g = gm[:, h * VH : (h + 1) * VH].astype(F32)
        d = den[:, h : h + 1]
        grads.append((g / d).astype(BF))
        inner = -jnp.sum(g * mixed[:, h * VH : (h + 1) * VH].astype(F32), axis=1, keepdims=True) / d
        offsets.append(jnp.transpose(jnp.broadcast_to(inner, (rows, 128)))[0:1, :])
        head_queries.append(one_head(queries, h, width))

    def pair(b, diagonal):
        there = pl.ds(pl.multiple_of(b * rows, rows), rows)
        raw = qkv[there, width : 2 * width]
        keys = with_one(raw, width)
        turned = jnp.transpose(keys)
        allowed = seg_col[there, :] == seg_q
        if diagonal:
            u = lax.broadcasted_iota(jnp.int32, (rows, rows), 0)
            t = lax.broadcasted_iota(jnp.int32, (rows, rows), 1)
            allowed = jnp.logical_and(allowed, u <= t)
        for h in range(heads):
            lanes = slice(h * VH, (h + 1) * VH)
            shifted = dot_nt(keys, head_queries[h])
            weight = jnp.where(allowed, shifted * shifted + 1.0, 0.0).astype(BF)
            value_sum[there, lanes] += dot_nn(weight, grads[h])
            values = qkv[there, 2 * width + h * VH : 2 * width + (h + 1) * VH]
            grad = dot_nt(values, grads[h]) + offsets[h]
            score = jnp.where(allowed, grad * shifted, 0.0).astype(BF)
            key_sum[there, :] += dot_nn(score, head_queries[h])
            query_sum[a, h * QK : (h + 1) * QK, :] += dot_nn(turned[h * QK : (h + 1) * QK, :], score)

    pair(a, True)

    @pl.loop(0, nb)
    def _(b):
        @pl.when(needed(meta, a, b, nb))
        def _():
            pair(b, False)

    @pl.when(a == nb - 1)
    def _():
        for b in range(nb):
            span = slice(b * rows, (b + 1) * rows)
            s = scale[span, :]
            grad_q = jnp.transpose(query_sum[b]) * (0.5 * s)
            out[span, :width] = grad_q.astype(BF)
            out[span, width : 2 * width] = (key_sum[span, :width] * (2.0 * s)).astype(BF)
            out[span, 2 * width :] = (value_sum[span, :] * s).astype(BF)


def block_spec(shape, index):
    return pl.BlockSpec(shape, index)


def whole(shape):
    return pl.BlockSpec(shape, lambda a, *_: (0,) * len(shape))


def attention_forward(meta, qkv, seg_col, seg_row, heads, rows):
    tokens = qkv.shape[0]
    nb = tokens // rows
    values = heads * VH
    return pl.pallas_call(
        functools.partial(forward_kernel, heads=heads, rows=rows, nb=nb),
        out_shape=(
            jax.ShapeDtypeStruct((tokens, values), BF),
            jax.ShapeDtypeStruct((tokens, heads), F32),
        ),
        grid_spec=pltpu.PrefetchScalarGridSpec(
            num_scalar_prefetch=1,
            grid=(nb,),
            in_specs=[whole(qkv.shape), whole(seg_col.shape), whole(seg_row.shape)],
            out_specs=[
                pl.BlockSpec((rows, values), lambda a, *_: (a, 0)),
                pl.BlockSpec((rows, heads), lambda a, *_: (a, 0)),
            ],
            scratch_shapes=[pltpu.VMEM((rows, values), F32), pltpu.VMEM((rows, values), F32)],
        ),
        cost_estimate=pl.CostEstimate(
            flops=4 * tokens * values, transcendentals=0, bytes_accessed=8 * tokens
        ),
        name="attention_forward",
    )(meta, qkv, seg_col, seg_row)


def attention_backward(meta, qkv, seg_col, seg_row, gm, mixed, den, scale, heads, rows):
    tokens = qkv.shape[0]
    nb = tokens // rows
    values = heads * VH
    width = heads * QK
    return pl.pallas_call(
        functools.partial(backward_kernel, heads=heads, rows=rows, nb=nb),
        out_shape=jax.ShapeDtypeStruct((tokens, 2 * width + values), BF),
        grid_spec=pltpu.PrefetchScalarGridSpec(
            num_scalar_prefetch=1,
            grid=(nb,),
            in_specs=[
                whole(qkv.shape),
                whole(seg_col.shape),
                whole(seg_row.shape),
                pl.BlockSpec((rows, values), lambda a, *_: (a, 0)),
                pl.BlockSpec((rows, values), lambda a, *_: (a, 0)),
                pl.BlockSpec((rows, heads), lambda a, *_: (a, 0)),
                whole(scale.shape),
            ],
            out_specs=whole((tokens, 2 * width + values)),
            scratch_shapes=[
                pltpu.VMEM((tokens, 128), F32),
                pltpu.VMEM((tokens, values), F32),
                pltpu.VMEM((nb, width, rows), F32),
            ],
        ),
        cost_estimate=pl.CostEstimate(
            flops=10 * tokens * values, transcendentals=0, bytes_accessed=16 * tokens
        ),
        name="attention_backward",
    )(meta, qkv, seg_col, seg_row, gm, mixed, den, scale)


def mm(a, b):
    return jnp.dot(a, b, preferred_element_type=F32)


def mm_tn(a, b):
    return lax.dot_general(a, b, (((0,), (0,)), ((), ())), preferred_element_type=F32)


def mm_nt(a, b):
    return lax.dot_general(a, b, (((1,), (1,)), ((), ())), preferred_element_type=F32)


def inverse_rms(values):
    return lax.rsqrt(jnp.mean(values * values, axis=-1, keepdims=True) + EPS)


def local(
    tokens,
    segment_ids,
    norm1_gain,
    w_query,
    w_key,
    w_value,
    w_out,
    norm2_gain,
    w_gate,
    w_up,
    w_down,
    cotangent,
):
    nc, nf = lax.axis_size(C), lax.axis_size(F)
    c = lax.axis_index(C)
    rows, width = tokens.shape[1], tokens.shape[2]
    heads = HEADS // nc
    qk = heads * QK
    hidden_all = w_gate.shape[1]
    seg_len = hidden_all // (nc * nf)
    hidden = seg_len * nf
    shard = w_gate.shape[0]

    own = tokens[0]
    grad_top = cotangent[0]
    gain_one = norm1_gain.astype(F32)[:, None]
    gain_two = norm2_gain.astype(F32)[:, None]

    def columns(weight, size):
        return lax.dynamic_slice_in_dim(weight, c * size, size, axis=1)

    part_qkv = (
        jnp.concatenate(
            [columns(w_query, qk), columns(w_key, qk), columns(w_value, heads * VH)], axis=1
        ).astype(F32)
        * gain_one
    ).astype(BF)

    def hidden_columns(weight):
        picked = lax.dynamic_index_in_dim(
            weight.reshape(shard, nf, nc, seg_len), c, axis=2, keepdims=False
        )
        return (picked.reshape(shard, hidden).astype(F32) * gain_two).astype(BF)

    part_out = group_pieces(w_out)
    part_gate = hidden_columns(w_gate)
    part_up = hidden_columns(w_up)
    part_down = lax.dynamic_slice_in_dim(w_down, c * seg_len, seg_len, axis=0)

    seg_all = jnp.concatenate(spread_direct(segment_ids[0]), axis=0)
    nb = nc
    seg_row = seg_all.reshape(nb, 1, rows)
    seg_col = seg_all.reshape(nb * rows, 1)
    meta = jnp.concatenate(
        [jnp.stack(spread_index()), seg_row[:, 0, 0], seg_row[:, 0, rows - 1]]
    ).astype(jnp.int32)

    x_parts = spread(own)
    full_qkv = gather_all(part_qkv)
    full_out = gather_all(after(part_out, x_parts[-2]))
    full_gate = gather_all(part_gate)
    full_up = gather_all(part_up)
    full_down = gather_all(part_down)

    x_all = jnp.concatenate(x_parts, axis=0)
    scale_one = inverse_rms(x_all.astype(F32))
    qkv = (mm(x_all, full_qkv) * scale_one).astype(BF)
    g_parts = spread(grad_top)
    mixed, den = attention_forward(meta, qkv, seg_col, seg_row, heads, rows)

    def blocks(value):
        return [value[i * rows : (i + 1) * rows] for i in range(nb)]

    projected = mm(after(mixed, *g_parts), full_out).astype(BF)
    residual = own.astype(F32) + add_chips(add_cores(blocks(projected)))

    scale_two = inverse_rms(residual)
    unit_two = residual * scale_two
    n_all = jnp.concatenate(spread(unit_two.astype(BF)), axis=0)
    g_all = jnp.concatenate(g_parts, axis=0)
    gate = mm(n_all, full_gate)
    up = mm(after(n_all, gate), full_up)
    grad_hidden = mm_nt(after(g_all, up), full_down)
    sigmoid = jax.nn.sigmoid(gate)
    silu = gate * sigmoid
    act = (silu * up).astype(BF)
    grad_gate = (grad_hidden * up * sigmoid * (1.0 + gate * (1.0 - sigmoid))).astype(BF)
    grad_up = (grad_hidden * silu).astype(BF)
    back_two = (mm_nt(grad_gate, full_gate) + mm_nt(grad_up, full_up)).astype(BF)
    back_sums = add_cores(blocks(back_two))

    total_gate = mm_tn(n_all, after(grad_gate, *back_sums)).astype(BF)
    sum_gate = scatter_all(total_gate)
    total_up = mm_tn(n_all, after(grad_up, total_gate)).astype(BF)
    mine_up, sent_up = scatter_sides(total_up)
    grad_unit_two = add_chips([after(back_sums[0], total_up)] + back_sums[1:])

    grad_residual = grad_top.astype(F32) + scale_two * (
        grad_unit_two - unit_two * jnp.mean(grad_unit_two * unit_two, axis=-1, keepdims=True)
    )
    branch = grad_residual.astype(BF)
    total_down = mm_tn(after(act, branch), g_all).astype(BF)
    sum_down = scatter_all(total_down)
    projected_two = mm(after(act, total_down), full_down).astype(BF)
    b_all = jnp.concatenate(spread(branch, [projected_two]), axis=0)
    out_sums = add_cores(blocks(after(projected_two, b_all)))

    grad_mixed = mm_nt(b_all, full_out)
    lines_up = scatter_lines(mine_up, after(sent_up, grad_mixed))
    total_out = mm_tn(mixed, after(b_all, lines_up[0])).astype(BF)
    grad_qkv = attention_backward(
        meta, qkv, seg_col, seg_row, after(grad_mixed, total_out, *out_sums), mixed, den, scale_one, heads, rows
    )
    sum_out = scatter_all(total_out)
    block_out = residual + after(add_chips([jnp.zeros_like(out_sums[0])] + out_sums[1:]), grad_qkv) + out_sums[0]
    back_one = mm_nt(after(grad_qkv, block_out), full_qkv).astype(BF)
    one_sums = add_cores(blocks(back_one))
    total_qkv = mm_tn(x_all, after(grad_qkv, *one_sums, *lines_up)).astype(BF)
    mine_qkv, sent_qkv = scatter_sides(total_qkv)
    grad_unit_one = add_chips(one_sums)
    lines_qkv = scatter_lines(mine_qkv, sent_qkv)
    sum_gate = after(sum_gate, lines_qkv[0])
    sum_up = add_all([after(lines_up[0], grad_unit_one)] + lines_up[1:])
    sum_down = after(sum_down, grad_unit_one)
    sum_out = after(sum_out, grad_unit_one)
    sum_qkv = add_all(lines_qkv)

    unit_one = own.astype(F32) * inverse_rms(own.astype(F32))
    input_grad = grad_residual + grad_unit_one - unit_one * jnp.mean(
        grad_unit_one * unit_one, axis=-1, keepdims=True
    )

    def over_context(value):
        return in_order(spread(value.astype(BF)))

    def from_hidden(stacked):
        return (
            stacked.reshape(nc, shard, nf, seg_len)
            .transpose(1, 2, 0, 3)
            .reshape(shard, hidden_all)
            .astype(F32)
        )

    def side_by_side(stacked):
        return stacked.transpose(1, 0, 2).reshape(stacked.shape[1], -1).astype(F32)

    all_down = over_context(sum_down).reshape(nc * seg_len, width).astype(F32)
    all_gate = from_hidden(over_context(sum_gate))
    all_up = from_hidden(over_context(sum_up))
    all_qkv = over_context(sum_qkv)
    all_query = side_by_side(all_qkv[:, :, :qk])
    all_key = side_by_side(all_qkv[:, :, qk : 2 * qk])
    all_value = side_by_side(all_qkv[:, :, 2 * qk :])
    all_out = ungroup_pieces(sum_out.astype(BF)).astype(F32)

    def along(weight, grad):
        return jnp.sum(weight.astype(F32) * grad, axis=1)

    grad_gain_one = along(w_query, all_query) + along(w_key, all_key) + along(w_value, all_value)
    grad_gain_two = along(w_gate, all_gate) + along(w_up, all_up)
    return (
        block_out.astype(BF)[None],
        input_grad[None],
        grad_gain_one,
        all_query * gain_one,
        all_key * gain_one,
        all_value * gain_one,
        all_out,
        grad_gain_two,
        all_gate * gain_two,
        all_up * gain_two,
        all_down,
    )


def solution(mesh):
    rows = P(F, None)
    acts = P(F, C, None)
    return jax.shard_map(
        local,
        mesh=mesh,
        in_specs=(acts, P(F, C), P(F), rows, rows, rows, rows, P(F), rows, rows, rows, acts),
        out_specs=(acts, acts, P(F), rows, rows, rows, rows, P(F), rows, rows, rows),
        check_vma=False,
    )
```

```python
import functools

import jax
import jax.numpy as jnp
from jax import lax
from jax.experimental import pallas as pl
from jax.experimental.pallas import tpu as pltpu
from jax.sharding import PartitionSpec as P

HEADS = 16
QK = 16
VH = 128
EPS = 1e-05

C = "context"
F = "fsdp"
BF = jnp.bfloat16
F32 = jnp.float32


def after(value, *earlier):
    return lax.optimization_barrier((value,) + earlier)[0]


def lines():
    return lax.axis_size(F) // 2


def line_groups():
    m = lines()
    return [[2 * line + side for line in range(m)] for side in range(2)]


def side_swap(value):
    return lax.ppermute(value, F, [(j, j ^ 1) for j in range(lax.axis_size(F))])


def line_and_side():
    me = lax.axis_index(F)
    return me // 2, lax.rem(me, 2)


def scatter_sides(total):
    m = lines()
    _, side = line_and_side()
    parts = total.reshape(m, 2, total.shape[0] // (2 * m), total.shape[1])
    mine = lax.dynamic_index_in_dim(parts, side, 1, keepdims=False)
    return mine, side_swap(lax.dynamic_index_in_dim(parts, 1 - side, 1, keepdims=False))


def add_sides(mine, sent):
    both = (mine.astype(F32) + sent.astype(F32)).astype(BF)
    return both.reshape(-1, both.shape[-1])


def scatter_lines(total):
    return lax.psum_scatter(total, F, scatter_dimension=0, axis_index_groups=line_groups(), tiled=True)


def gather_lines(block):
    return lax.all_gather(block, F, axis=0, axis_index_groups=line_groups())


def assemble_kernel(own, other, out, sems, *, m):
    side = lax.rem(lax.axis_index(F), 2)
    copies = []
    for k in range(m):
        copies.append(pltpu.make_async_copy(own.at[k], out.at[2 * k + side], sems.at[k]))
        copies.append(pltpu.make_async_copy(other.at[k], out.at[2 * k + 1 - side], sems.at[m + k]))
    for copy in copies:
        copy.start()
    for copy in copies:
        copy.wait()


def assemble(own, other):
    m, rows, width = own.shape
    out = pl.pallas_call(
        functools.partial(assemble_kernel, m=m),
        out_shape=jax.ShapeDtypeStruct((2 * m, rows, width), own.dtype),
        in_specs=[pl.BlockSpec(memory_space=pl.ANY)] * 2,
        out_specs=pl.BlockSpec(memory_space=pltpu.VMEM),
        scratch_shapes=[pltpu.SemaphoreType.DMA((2 * m,))],
        cost_estimate=pl.CostEstimate(flops=0, transcendentals=0, bytes_accessed=1024),
        name="assemble",
    )(own, other)
    return out.reshape(2 * m * rows, width)


def chips():
    return lax.axis_size(C) // 2


def core_swap(value):
    n = lax.axis_size(C)
    return lax.ppermute(value, C, [(i, i ^ 1) for i in range(n)])


def chip_shift(value, k):
    n = lax.axis_size(C)
    return lax.ppermute(value, C, [(i, (i + 2 * k) % n) for i in range(n)])


def spread(block, marks=()):
    out = []
    for k in range(chips()):
        near = after(chip_shift(block, k), *marks) if k else block
        out += [near, core_swap(near)]
    return out


def spread_direct(block):
    n = lax.axis_size(C)
    return [
        lax.ppermute(block, C, [(i, (i + 2 * k) % n ^ h) for i in range(n)]) if k or h else block
        for k in range(chips())
        for h in range(2)
    ]


def spread_index():
    n, me = lax.axis_size(C), lax.axis_index(C)
    out = []
    for k in range(chips()):
        near = lax.rem(me - 2 * k + n, n)
        out += [near, near ^ 1]
    return out


def add_cores(parts):
    sums = []
    for k in range(chips()):
        both = parts[2 * k].astype(F32) + core_swap(parts[2 * k + 1]).astype(F32)
        sums.append(both.astype(BF) if k else both)
    return sums


def add_chips(sums):
    total = sums[0]
    for k in range(1, chips()):
        total = total + chip_shift(sums[k], -k).astype(F32)
    return total


def gather_back(parts):
    return add_chips(add_cores(parts))


def in_order(parts):
    out = jnp.zeros((len(parts),) + parts[0].shape, parts[0].dtype)
    for index, part in zip(spread_index(), parts):
        out = lax.dynamic_update_index_in_dim(out, part, index, 0)
    return out


def group_pairs(back):
    nc, nf = lax.axis_size(C), lax.axis_size(F)
    m = nf // nc
    out = []
    for q in range(nc):
        pairs = [
            (c * nf + m * c + s, c * nf + s * nc + q) for c in range(nc) for s in range(m)
        ]
        out.append([(b, a) for a, b in pairs] if back else pairs)
    return out


def group_pieces(shard):
    nc = lax.axis_size(C)
    rows = shard.shape[0] // nc
    out = None
    for q, pairs in enumerate(group_pairs(False)):
        got = lax.ppermute(shard[q * rows : (q + 1) * rows], (C, F), pairs)
        out = got if out is None else out + got
    return out


def ungroup_pieces(piece):
    nc, nf = lax.axis_size(C), lax.axis_size(F)
    m = nf // nc
    shard = jnp.concatenate(
        [lax.ppermute(piece, (C, F), pairs) for pairs in group_pairs(True)], axis=0
    )
    out = shard
    for k in range(1, nc // 2):
        out = out + lax.ppermute(
            shard, (C, F), [((j // m) * nf + j, ((j // m + 2 * k) % nc) * nf + j) for j in range(nf)]
        )
    holders = [((j // m) % 2, j) for j in range(nf)]
    swap = [
        ((2 * x + h) * nf + j, (2 * x + 1 - h) * nf + j) for h, j in holders for x in range(nc // 2)
    ]
    return out + lax.ppermute(out, (C, F), swap)


def dot_nt(a, b):
    return lax.dot_general(a, b, (((1,), (1,)), ((), ())), preferred_element_type=F32)


def dot_nn(a, b):
    return lax.dot_general(a, b, (((1,), (0,)), ((), ())), preferred_element_type=F32)


def with_one(values, width):
    rows = values.shape[0]
    padded = jnp.concatenate([values, jnp.zeros((rows, 128 - width), values.dtype)], axis=1)
    lane = lax.broadcasted_iota(jnp.int32, (rows, 128), 1)
    return jnp.where(lane == width, jnp.ones_like(padded), padded)


def one_head(values, head, width):
    lane = lax.broadcasted_iota(jnp.int32, values.shape, 1)
    keep = jnp.logical_or(lane // QK == head, lane == width)
    return jnp.where(keep, values, jnp.zeros_like(values))


def needed(meta, a, b, nb):
    before = meta[b] < meta[a]
    return jnp.logical_and(before, meta[nb + a] <= meta[2 * nb + b])


def forward_kernel(meta, qkv, seg_col, seg_row, mixed, den, num_sum, den_sum, *, heads, rows, nb):
    width = heads * QK
    a = pl.program_id(0)
    here = pl.ds(pl.multiple_of(a * rows, rows), rows)
    queries = with_one(qkv[here, :width] * 0.25, width)
    seg_q = seg_col[here, :]
    num_sum[...] = jnp.zeros_like(num_sum)
    den_sum[...] = jnp.zeros_like(den_sum)

    def pair(b, diagonal):
        there = pl.ds(pl.multiple_of(b * rows, rows), rows)
        keys = with_one(qkv[there, width : 2 * width], width)
        allowed = seg_q == seg_row[b]
        if diagonal:
            t = lax.broadcasted_iota(jnp.int32, (rows, rows), 0)
            u = lax.broadcasted_iota(jnp.int32, (rows, rows), 1)
            allowed = jnp.logical_and(allowed, u <= t)
        for h in range(heads):
            shifted = dot_nt(one_head(queries, h, width), keys)
            weight = jnp.where(allowed, shifted * shifted + 1.0, 0.0)
            lanes = slice(h * VH, (h + 1) * VH)
            values = qkv[there, 2 * width + h * VH : 2 * width + (h + 1) * VH]
            num_sum[:, lanes] += dot_nn(weight.astype(BF), values)
            den_sum[:, lanes] += jnp.broadcast_to(
                jnp.sum(weight, axis=1, keepdims=True), (rows, VH)
            )

    pair(a, True)

    @pl.loop(0, nb)
    def _(b):
        @pl.when(needed(meta, a, b, nb))
        def _():
            pair(b, False)

    mixed[...] = (num_sum[...] / den_sum[...]).astype(BF)
    for h in range(heads):
        den[:, h : h + 1] = den_sum[:, h * VH : h * VH + 1]


def backward_kernel(
    meta, qkv, seg_col, seg_row, gm, mixed, den, scale, out, key_sum, value_sum, query_sum, *, heads, rows, nb
):
    width = heads * QK
    a = pl.program_id(0)
    here = pl.ds(pl.multiple_of(a * rows, rows), rows)
    queries = with_one(qkv[here, :width] * 0.25, width)
    seg_q = seg_row[a]

    @pl.when(a == 0)
    def _():
        key_sum[...] = jnp.zeros_like(key_sum)
        value_sum[...] = jnp.zeros_like(value_sum)
        query_sum[...] = jnp.zeros_like(query_sum)

    grads, offsets, head_queries = [], [], []
    for h in range(heads):
        g = gm[:, h * VH : (h + 1) * VH].astype(F32)
        d = den[:, h : h + 1]
        grads.append((g / d).astype(BF))
        inner = -jnp.sum(g * mixed[:, h * VH : (h + 1) * VH].astype(F32), axis=1, keepdims=True) / d
        offsets.append(jnp.transpose(jnp.broadcast_to(inner, (rows, 128)))[0:1, :])
        head_queries.append(one_head(queries, h, width))

    def pair(b, diagonal):
        there = pl.ds(pl.multiple_of(b * rows, rows), rows)
        raw = qkv[there, width : 2 * width]
        keys = with_one(raw, width)
        turned = jnp.transpose(keys)
        allowed = seg_col[there, :] == seg_q
        if diagonal:
            u = lax.broadcasted_iota(jnp.int32, (rows, rows), 0)
            t = lax.broadcasted_iota(jnp.int32, (rows, rows), 1)
            allowed = jnp.logical_and(allowed, u <= t)
        for h in range(heads):
            lanes = slice(h * VH, (h + 1) * VH)
            shifted = dot_nt(keys, head_queries[h])
            weight = jnp.where(allowed, shifted * shifted + 1.0, 0.0).astype(BF)
            value_sum[there, lanes] += dot_nn(weight, grads[h])
            values = qkv[there, 2 * width + h * VH : 2 * width + (h + 1) * VH]
            grad = dot_nt(values, grads[h]) + offsets[h]
            score = jnp.where(allowed, grad * shifted, 0.0).astype(BF)
            key_sum[there, :] += dot_nn(score, head_queries[h])
            query_sum[a, h * QK : (h + 1) * QK, :] += dot_nn(turned[h * QK : (h + 1) * QK, :], score)

    pair(a, True)

    @pl.loop(0, nb)
    def _(b):
        @pl.when(needed(meta, a, b, nb))
        def _():
            pair(b, False)

    @pl.when(a == nb - 1)
    def _():
        for b in range(nb):
            span = slice(b * rows, (b + 1) * rows)
            s = scale[span, :]
            grad_q = jnp.transpose(query_sum[b]) * (0.5 * s)
            out[span, :width] = grad_q.astype(BF)
            out[span, width : 2 * width] = (key_sum[span, :width] * (2.0 * s)).astype(BF)
            out[span, 2 * width :] = (value_sum[span, :] * s).astype(BF)


def block_spec(shape, index):
    return pl.BlockSpec(shape, index)


def whole(shape):
    return pl.BlockSpec(shape, lambda a, *_: (0,) * len(shape))


def attention_forward(meta, qkv, seg_col, seg_row, heads, rows):
    tokens = qkv.shape[0]
    nb = tokens // rows
    values = heads * VH
    return pl.pallas_call(
        functools.partial(forward_kernel, heads=heads, rows=rows, nb=nb),
        out_shape=(
            jax.ShapeDtypeStruct((tokens, values), BF),
            jax.ShapeDtypeStruct((tokens, heads), F32),
        ),
        grid_spec=pltpu.PrefetchScalarGridSpec(
            num_scalar_prefetch=1,
            grid=(nb,),
            in_specs=[whole(qkv.shape), whole(seg_col.shape), whole(seg_row.shape)],
            out_specs=[
                pl.BlockSpec((rows, values), lambda a, *_: (a, 0)),
                pl.BlockSpec((rows, heads), lambda a, *_: (a, 0)),
            ],
            scratch_shapes=[pltpu.VMEM((rows, values), F32), pltpu.VMEM((rows, values), F32)],
        ),
        cost_estimate=pl.CostEstimate(
            flops=4 * tokens * values, transcendentals=0, bytes_accessed=8 * tokens
        ),
        name="attention_forward",
    )(meta, qkv, seg_col, seg_row)


def attention_backward(meta, qkv, seg_col, seg_row, gm, mixed, den, scale, heads, rows):
    tokens = qkv.shape[0]
    nb = tokens // rows
    values = heads * VH
    width = heads * QK
    return pl.pallas_call(
        functools.partial(backward_kernel, heads=heads, rows=rows, nb=nb),
        out_shape=jax.ShapeDtypeStruct((tokens, 2 * width + values), BF),
        grid_spec=pltpu.PrefetchScalarGridSpec(
            num_scalar_prefetch=1,
            grid=(nb,),
            in_specs=[
                whole(qkv.shape),
                whole(seg_col.shape),
                whole(seg_row.shape),
                pl.BlockSpec((rows, values), lambda a, *_: (a, 0)),
                pl.BlockSpec((rows, values), lambda a, *_: (a, 0)),
                pl.BlockSpec((rows, heads), lambda a, *_: (a, 0)),
                whole(scale.shape),
            ],
            out_specs=whole((tokens, 2 * width + values)),
            scratch_shapes=[
                pltpu.VMEM((tokens, 128), F32),
                pltpu.VMEM((tokens, values), F32),
                pltpu.VMEM((nb, width, rows), F32),
            ],
        ),
        cost_estimate=pl.CostEstimate(
            flops=10 * tokens * values, transcendentals=0, bytes_accessed=16 * tokens
        ),
        name="attention_backward",
    )(meta, qkv, seg_col, seg_row, gm, mixed, den, scale)


def of_context(parts, c, nc):
    me = lax.axis_index(C)
    out = parts[0][...]
    for i in range(1, nc):
        near = lax.rem(me - 2 * (i // 2) + nc, nc)
        index = near if i % 2 == 0 else near + 1 - 2 * lax.rem(near, 2)
        out = jnp.where(index == c, parts[i][...], out)
    return out


def columns_kernel(*refs, nc, seg, groups):
    parts, weight, gain, out, along = refs[:nc], refs[nc], refs[nc + 1], refs[nc + 2], refs[nc + 3]
    total = jnp.zeros(along.shape, F32)
    for c in range(nc):
        part = of_context(parts, c, nc)
        for j in range(groups):
            place = slice((j * nc + c) * seg, (j * nc + c + 1) * seg)
            value = part[:, j * seg : (j + 1) * seg].astype(F32)
            total += jnp.sum(value * weight[:, place].astype(F32), axis=1, keepdims=True)
            out[:, place] = value * gain[...]
    along[...] = total


def finish_columns(parts, weight, gain, seg, groups):
    nc = len(parts)
    rows, width = weight.shape
    tile = next(t for t in (64, 32, 16, 8) if rows % t == 0)

    def spec(size):
        return pl.BlockSpec((tile, size), lambda i: (i, 0))

    return pl.pallas_call(
        functools.partial(columns_kernel, nc=nc, seg=seg, groups=groups),
        out_shape=(
            jax.ShapeDtypeStruct((rows, width), F32),
            jax.ShapeDtypeStruct((rows, 1), F32),
        ),
        grid=(rows // tile,),
        in_specs=[spec(parts[0].shape[1])] * nc + [spec(width), spec(1)],
        out_specs=[spec(width), spec(1)],
        cost_estimate=pl.CostEstimate(flops=0, transcendentals=0, bytes_accessed=1024),
        name="finish_columns",
    )(*parts, weight, gain)


def rows_kernel(*refs, nc):
    out = refs[nc]
    size = refs[0].shape[0]
    for c in range(nc):
        out[c * size : (c + 1) * size, :] = of_context(refs[:nc], c, nc).astype(F32)


def finish_rows(parts):
    nc = len(parts)
    rows, width = parts[0].shape
    tile = next(t for t in (512, 256, 128) if width % t == 0)
    return pl.pallas_call(
        functools.partial(rows_kernel, nc=nc),
        out_shape=jax.ShapeDtypeStruct((nc * rows, width), F32),
        grid=(width // tile,),
        in_specs=[pl.BlockSpec((rows, tile), lambda i: (0, i))] * nc,
        out_specs=pl.BlockSpec((nc * rows, tile), lambda i: (0, i)),
        cost_estimate=pl.CostEstimate(flops=0, transcendentals=0, bytes_accessed=1024),
        name="finish_rows",
    )(*parts)


def mm(a, b):
    return jnp.dot(a, b, preferred_element_type=F32)


def mm_tn(a, b):
    return lax.dot_general(a, b, (((0,), (0,)), ((), ())), preferred_element_type=F32)


def mm_nt(a, b):
    return lax.dot_general(a, b, (((1,), (1,)), ((), ())), preferred_element_type=F32)


def inverse_rms(values):
    return lax.rsqrt(jnp.mean(values * values, axis=-1, keepdims=True) + EPS)


def local(
    tokens,
    segment_ids,
    norm1_gain,
    w_query,
    w_key,
    w_value,
    w_out,
    norm2_gain,
    w_gate,
    w_up,
    w_down,
    cotangent,
):
    nc, nf = lax.axis_size(C), lax.axis_size(F)
    c = lax.axis_index(C)
    rows, width = tokens.shape[1], tokens.shape[2]
    heads = HEADS // nc
    qk = heads * QK
    hidden_all = w_gate.shape[1]
    seg_len = hidden_all // (nc * nf)
    hidden = seg_len * nf
    shard = w_gate.shape[0]

    own = tokens[0]
    grad_top = cotangent[0]
    gain_one = norm1_gain.astype(F32)[:, None]
    gain_two = norm2_gain.astype(F32)[:, None]

    def columns(weight, size):
        return lax.dynamic_slice_in_dim(weight, c * size, size, axis=1)

    part_qkv = (
        jnp.concatenate(
            [columns(w_query, qk), columns(w_key, qk), columns(w_value, heads * VH)], axis=1
        ).astype(F32)
        * gain_one
    ).astype(BF)

    def hidden_columns(weight):
        picked = lax.dynamic_index_in_dim(
            weight.reshape(shard, nf, nc, seg_len), c, axis=2, keepdims=False
        )
        return (picked.reshape(shard, hidden).astype(F32) * gain_two).astype(BF)

    part_out = group_pieces(w_out)
    part_gate = hidden_columns(w_gate)
    part_up = hidden_columns(w_up)
    part_down = lax.dynamic_slice_in_dim(w_down, c * seg_len, seg_len, axis=0)

    seg_all = jnp.concatenate(spread_direct(segment_ids[0]), axis=0)
    nb = nc
    seg_row = seg_all.reshape(nb, 1, rows)
    seg_col = seg_all.reshape(nb * rows, 1)
    meta = jnp.concatenate(
        [jnp.stack(spread_index()), seg_row[:, 0, 0], seg_row[:, 0, rows - 1]]
    ).astype(jnp.int32)

    line_qkv = gather_lines(part_qkv)
    x_parts = spread(own, [line_qkv])
    line_out = gather_lines(after(part_out, x_parts[-2]))
    line_gate = gather_lines(part_gate)
    line_up = gather_lines(part_up)
    line_down = gather_lines(part_down)
    x_all = jnp.concatenate(x_parts, axis=0)
    scale_one = inverse_rms(x_all.astype(F32))
    full_qkv = assemble(line_qkv, side_swap(line_qkv))
    g_parts = spread(after(grad_top, seg_all, x_all))
    qkv = (mm(x_all, full_qkv) * scale_one).astype(BF)
    mixed, den = attention_forward(meta, qkv, seg_col, seg_row, heads, rows)

    def blocks(value):
        return [value[i * rows : (i + 1) * rows] for i in range(nb)]

    full_out = assemble(line_out, side_swap(line_out))
    projected = mm(after(mixed, *g_parts), full_out).astype(BF)
    sums = add_cores(blocks(projected))
    residual = own.astype(F32) + add_chips(sums)

    scale_two = inverse_rms(residual)
    unit_two = residual * scale_two
    full_gate = assemble(line_gate, side_swap(after(line_gate, *sums)))
    n_all = jnp.concatenate(spread(unit_two.astype(BF)), axis=0)
    g_all = jnp.concatenate(g_parts, axis=0)
    full_up = assemble(line_up, side_swap(after(line_up, unit_two)))
    gate = mm(n_all, full_gate)
    full_down = assemble(line_down, side_swap(after(line_down, n_all)))
    up = mm(after(n_all, gate), full_up)
    grad_hidden = mm_nt(after(g_all, up), full_down)
    sigmoid = jax.nn.sigmoid(gate)
    silu = gate * sigmoid
    act = (silu * up).astype(BF)
    grad_gate = (grad_hidden * up * sigmoid * (1.0 + gate * (1.0 - sigmoid))).astype(BF)
    grad_up = (grad_hidden * silu).astype(BF)
    back_two = (mm_nt(grad_gate, full_gate) + mm_nt(grad_up, full_up)).astype(BF)
    back_sums = add_cores(blocks(back_two))

    total_gate = mm_tn(n_all, after(grad_gate, *back_sums)).astype(BF)
    mine_gate, sent_gate = scatter_sides(total_gate)
    total_up = mm_tn(n_all, after(grad_up, total_gate)).astype(BF)
    mine_up, sent_up = scatter_sides(total_up)
    grad_unit_two = add_chips([after(back_sums[0], total_up)] + back_sums[1:])

    grad_residual = grad_top.astype(F32) + scale_two * (
        grad_unit_two - unit_two * jnp.mean(grad_unit_two * unit_two, axis=-1, keepdims=True)
    )
    branch = grad_residual.astype(BF)
    total_down = mm_tn(after(act, branch), g_all).astype(BF)
    mine_down, sent_down = scatter_sides(total_down)
    projected_two = mm(after(act, total_down), full_down).astype(BF)
    both_gate = add_sides(mine_gate, after(sent_gate, total_down))
    sum_gate = scatter_lines(both_gate)
    b_all = jnp.concatenate(spread(branch, [projected_two, both_gate]), axis=0)
    out_sums = add_cores(blocks(after(projected_two, b_all)))

    grad_mixed = mm_nt(b_all, full_out)
    total_out = mm_tn(mixed, after(b_all, grad_mixed)).astype(BF)
    mine_out, sent_out = scatter_sides(total_out)
    both_up = add_sides(mine_up, after(sent_up, total_out))
    sum_up = scatter_lines(both_up)
    grad_qkv = attention_backward(
        meta, qkv, seg_col, seg_row, after(grad_mixed, both_up, *out_sums), mixed, den, scale_one, heads, rows
    )
    block_out = residual + after(add_chips([jnp.zeros_like(out_sums[0])] + out_sums[1:]), grad_qkv) + out_sums[0]
    back_one = mm_nt(after(grad_qkv, block_out), full_qkv).astype(BF)
    one_sums = add_cores(blocks(back_one))
    both_down = add_sides(mine_down, after(sent_down, *one_sums))
    total_qkv = mm_tn(x_all, after(grad_qkv, both_down)).astype(BF)
    mine_qkv, sent_qkv = scatter_sides(total_qkv)
    grad_unit_one = add_chips(one_sums)
    sum_down = scatter_lines(both_down)
    both_out = add_sides(mine_out, after(sent_out, both_down))
    sum_out = scatter_lines(both_out)
    both_qkv = add_sides(mine_qkv, after(sent_qkv, both_out, grad_unit_one))
    sum_qkv = scatter_lines(both_qkv)
    sum_gate = after(sum_gate, both_qkv)
    sum_up = after(sum_up, both_qkv, grad_unit_one)

    unit_one = own.astype(F32) * inverse_rms(own.astype(F32))
    input_grad = grad_residual + grad_unit_one - unit_one * jnp.mean(
        grad_unit_one * unit_one, axis=-1, keepdims=True
    )

    def over_context(value):
        return spread(value.astype(BF))

    def from_hidden(value, weight):
        stacked = in_order(over_context(value)).reshape(nc, shard, nf, seg_len)
        grad = stacked.transpose(1, 2, 0, 3).reshape(shard, hidden_all).astype(F32)
        return grad * gain_two, jnp.sum(weight.astype(F32) * grad, axis=1, keepdims=True)

    grad_w_gate, along_gate = from_hidden(sum_gate, w_gate)
    grad_w_up, along_up = from_hidden(sum_up, w_up)
    qkv_parts = over_context(sum_qkv)

    def columns_of(first, size):
        return [part[:, first : first + size] for part in qkv_parts]

    grad_w_query, along_query = finish_columns(columns_of(0, qk), w_query, gain_one, qk, 1)
    grad_w_key, along_key = finish_columns(columns_of(qk, qk), w_key, gain_one, qk, 1)
    grad_w_value, along_value = finish_columns(
        columns_of(2 * qk, heads * VH), w_value, gain_one, heads * VH, 1
    )
    grad_w_down = finish_rows(over_context(sum_down))
    grad_w_out = ungroup_pieces(sum_out.astype(BF)).astype(F32)
    return (
        block_out.astype(BF)[None],
        input_grad[None],
        (along_query + along_key + along_value)[:, 0],
        grad_w_query,
        grad_w_key,
        grad_w_value,
        grad_w_out,
        (along_gate + along_up)[:, 0],
        grad_w_gate,
        grad_w_up,
        grad_w_down,
    )


def solution(mesh):
    rows = P(F, None)
    acts = P(F, C, None)
    return jax.shard_map(
        local,
        mesh=mesh,
        in_specs=(acts, P(F, C), P(F), rows, rows, rows, rows, P(F), rows, rows, rows, acts),
        out_specs=(acts, acts, P(F), rows, rows, rows, rows, P(F), rows, rows, rows),
        check_vma=False,
    )
```

```python
import functools

import jax
import jax.numpy as jnp
from jax import lax
from jax.experimental import pallas as pl
from jax.experimental.pallas import tpu as pltpu
from jax.sharding import PartitionSpec as P

HEADS = 16
QK = 16
VH = 128
EPS = 1e-05

C = "context"
F = "fsdp"
BF = jnp.bfloat16
F32 = jnp.float32


def after(value, *earlier):
    return lax.optimization_barrier((value,) + earlier)[0]


def lines():
    return lax.axis_size(F) // 2


def line_groups():
    m = lines()
    return [[2 * line + side for line in range(m)] for side in range(2)]


def side_swap(value):
    return lax.ppermute(value, F, [(j, j ^ 1) for j in range(lax.axis_size(F))])


def swap_pieces(value, pieces):
    size = value.shape[0] // pieces
    return [side_swap(value[i * size : (i + 1) * size]) for i in range(pieces)]


def line_and_side():
    me = lax.axis_index(F)
    return me // 2, lax.rem(me, 2)


def scatter_sides(total, pieces=1):
    m = lines()
    _, side = line_and_side()
    parts = total.reshape(m, 2, total.shape[0] // (2 * m), total.shape[1])
    mine = lax.dynamic_index_in_dim(parts, side, 1, keepdims=False)
    return mine, swap_pieces(lax.dynamic_index_in_dim(parts, 1 - side, 1, keepdims=False), pieces)


def add_sides(mine, sent, *marks):
    sent = jnp.concatenate([after(sent[0], *marks)] + sent[1:], axis=0)
    both = (mine.astype(F32) + sent.astype(F32)).astype(BF)
    return both.reshape(-1, both.shape[-1])


def scatter_lines(total):
    return lax.psum_scatter(total, F, scatter_dimension=0, axis_index_groups=line_groups(), tiled=True)


def gather_lines(block):
    return lax.all_gather(block, F, axis=0, axis_index_groups=line_groups())


def assemble_kernel(own, *refs, m, pieces):
    side = lax.rem(lax.axis_index(F), 2)
    out, sems = refs[pieces], refs[pieces + 1]
    size = m // pieces
    copies = []
    for k in range(m):
        other = refs[k // size].at[k % size]
        copies.append(pltpu.make_async_copy(own.at[k], out.at[2 * k + side], sems.at[k]))
        copies.append(pltpu.make_async_copy(other, out.at[2 * k + 1 - side], sems.at[m + k]))
    for copy in copies:
        copy.start()
    for copy in copies:
        copy.wait()


def assemble(own, other):
    m, rows, width = own.shape
    out = pl.pallas_call(
        functools.partial(assemble_kernel, m=m, pieces=len(other)),
        out_shape=jax.ShapeDtypeStruct((2 * m, rows, width), own.dtype),
        in_specs=[pl.BlockSpec(memory_space=pl.ANY)] * (1 + len(other)),
        out_specs=pl.BlockSpec(memory_space=pltpu.VMEM),
        scratch_shapes=[pltpu.SemaphoreType.DMA((2 * m,))],
        cost_estimate=pl.CostEstimate(flops=0, transcendentals=0, bytes_accessed=1024),
        name="assemble",
    )(own, *other)
    return out.reshape(2 * m * rows, width)


def chips():
    return lax.axis_size(C) // 2


def core_swap(value):
    n = lax.axis_size(C)
    return lax.ppermute(value, C, [(i, i ^ 1) for i in range(n)])


def chip_shift(value, k):
    n = lax.axis_size(C)
    return lax.ppermute(value, C, [(i, (i + 2 * k) % n) for i in range(n)])


def spread(block, marks=()):
    out = []
    for k in range(chips()):
        near = after(chip_shift(block, k), *marks) if k else block
        out += [near, core_swap(near)]
    return out


def spread_direct(block):
    n = lax.axis_size(C)
    return [
        lax.ppermute(block, C, [(i, (i + 2 * k) % n ^ h) for i in range(n)]) if k or h else block
        for k in range(chips())
        for h in range(2)
    ]


def spread_index():
    n, me = lax.axis_size(C), lax.axis_index(C)
    out = []
    for k in range(chips()):
        near = lax.rem(me - 2 * k + n, n)
        out += [near, near ^ 1]
    return out


def add_cores(parts):
    sums = []
    for k in range(chips()):
        both = parts[2 * k].astype(F32) + core_swap(parts[2 * k + 1]).astype(F32)
        sums.append(both.astype(BF) if k else both)
    return sums


def add_chips(sums):
    total = sums[0]
    for k in range(1, chips()):
        total = total + chip_shift(sums[k], -k).astype(F32)
    return total


def gather_back(parts):
    return add_chips(add_cores(parts))


def in_order(parts):
    out = jnp.zeros((len(parts),) + parts[0].shape, parts[0].dtype)
    for index, part in zip(spread_index(), parts):
        out = lax.dynamic_update_index_in_dim(out, part, index, 0)
    return out


def group_pairs(back):
    nc, nf = lax.axis_size(C), lax.axis_size(F)
    m = nf // nc
    out = []
    for q in range(nc):
        pairs = [
            (c * nf + m * c + s, c * nf + s * nc + q) for c in range(nc) for s in range(m)
        ]
        out.append([(b, a) for a, b in pairs] if back else pairs)
    return out


def group_pieces(shard):
    nc = lax.axis_size(C)
    rows = shard.shape[0] // nc
    out = None
    for q, pairs in enumerate(group_pairs(False)):
        got = lax.ppermute(shard[q * rows : (q + 1) * rows], (C, F), pairs)
        out = got if out is None else out + got
    return out


def ungroup_pieces(piece):
    nc, nf = lax.axis_size(C), lax.axis_size(F)
    m = nf // nc
    shard = jnp.concatenate(
        [lax.ppermute(piece, (C, F), pairs) for pairs in group_pairs(True)], axis=0
    )
    out = shard
    for k in range(1, nc // 2):
        out = out + lax.ppermute(
            shard, (C, F), [((j // m) * nf + j, ((j // m + 2 * k) % nc) * nf + j) for j in range(nf)]
        )
    holders = [((j // m) % 2, j) for j in range(nf)]
    swap = [
        ((2 * x + h) * nf + j, (2 * x + 1 - h) * nf + j) for h, j in holders for x in range(nc // 2)
    ]
    return out + lax.ppermute(out, (C, F), swap)


def dot_nt(a, b):
    return lax.dot_general(a, b, (((1,), (1,)), ((), ())), preferred_element_type=F32)


def dot_nn(a, b):
    return lax.dot_general(a, b, (((1,), (0,)), ((), ())), preferred_element_type=F32)


def with_one(values, width):
    rows = values.shape[0]
    padded = jnp.concatenate([values, jnp.zeros((rows, 128 - width), values.dtype)], axis=1)
    lane = lax.broadcasted_iota(jnp.int32, (rows, 128), 1)
    return jnp.where(lane == width, jnp.ones_like(padded), padded)


def one_head(values, head, width):
    lane = lax.broadcasted_iota(jnp.int32, values.shape, 1)
    keep = jnp.logical_or(lane // QK == head, lane == width)
    return jnp.where(keep, values, jnp.zeros_like(values))


def needed(meta, a, b, nb):
    before = meta[b] < meta[a]
    return jnp.logical_and(before, meta[nb + a] <= meta[2 * nb + b])


def forward_kernel(meta, qkv, seg_col, seg_row, mixed, den, num_sum, den_sum, *, heads, rows, nb):
    width = heads * QK
    a = pl.program_id(0)
    here = pl.ds(pl.multiple_of(a * rows, rows), rows)
    queries = with_one(qkv[here, :width] * 0.25, width)
    seg_q = seg_col[here, :]
    num_sum[...] = jnp.zeros_like(num_sum)
    den_sum[...] = jnp.zeros_like(den_sum)

    def pair(b, diagonal):
        there = pl.ds(pl.multiple_of(b * rows, rows), rows)
        keys = with_one(qkv[there, width : 2 * width], width)
        allowed = seg_q == seg_row[b]
        if diagonal:
            t = lax.broadcasted_iota(jnp.int32, (rows, rows), 0)
            u = lax.broadcasted_iota(jnp.int32, (rows, rows), 1)
            allowed = jnp.logical_and(allowed, u <= t)
        for h in range(heads):
            shifted = dot_nt(one_head(queries, h, width), keys)
            weight = jnp.where(allowed, shifted * shifted + 1.0, 0.0)
            lanes = slice(h * VH, (h + 1) * VH)
            values = qkv[there, 2 * width + h * VH : 2 * width + (h + 1) * VH]
            num_sum[:, lanes] += dot_nn(weight.astype(BF), values)
            den_sum[:, lanes] += jnp.broadcast_to(
                jnp.sum(weight, axis=1, keepdims=True), (rows, VH)
            )

    pair(a, True)

    @pl.loop(0, nb)
    def _(b):
        @pl.when(needed(meta, a, b, nb))
        def _():
            pair(b, False)

    mixed[...] = (num_sum[...] / den_sum[...]).astype(BF)
    for h in range(heads):
        den[:, h : h + 1] = den_sum[:, h * VH : h * VH + 1]


def backward_kernel(
    meta, qkv, seg_col, seg_row, gm, mixed, den, scale, out, key_sum, value_sum, query_sum, *, heads, rows, nb
):
    width = heads * QK
    a = pl.program_id(0)
    here = pl.ds(pl.multiple_of(a * rows, rows), rows)
    queries = with_one(qkv[here, :width] * 0.25, width)
    seg_q = seg_row[a]

    @pl.when(a == 0)
    def _():
        key_sum[...] = jnp.zeros_like(key_sum)
        value_sum[...] = jnp.zeros_like(value_sum)
        query_sum[...] = jnp.zeros_like(query_sum)

    grads, offsets, head_queries = [], [], []
    for h in range(heads):
        g = gm[:, h * VH : (h + 1) * VH].astype(F32)
        d = den[:, h : h + 1]
        grads.append((g / d).astype(BF))
        inner = -jnp.sum(g * mixed[:, h * VH : (h + 1) * VH].astype(F32), axis=1, keepdims=True) / d
        offsets.append(jnp.transpose(jnp.broadcast_to(inner, (rows, 128)))[0:1, :])
        head_queries.append(one_head(queries, h, width))

    def pair(b, diagonal):
        there = pl.ds(pl.multiple_of(b * rows, rows), rows)
        raw = qkv[there, width : 2 * width]
        keys = with_one(raw, width)
        turned = jnp.transpose(keys)
        allowed = seg_col[there, :] == seg_q
        if diagonal:
            u = lax.broadcasted_iota(jnp.int32, (rows, rows), 0)
            t = lax.broadcasted_iota(jnp.int32, (rows, rows), 1)
            allowed = jnp.logical_and(allowed, u <= t)
        for h in range(heads):
            lanes = slice(h * VH, (h + 1) * VH)
            shifted = dot_nt(keys, head_queries[h])
            weight = jnp.where(allowed, shifted * shifted + 1.0, 0.0).astype(BF)
            value_sum[there, lanes] += dot_nn(weight, grads[h])
            values = qkv[there, 2 * width + h * VH : 2 * width + (h + 1) * VH]
            grad = dot_nt(values, grads[h]) + offsets[h]
            score = jnp.where(allowed, grad * shifted, 0.0).astype(BF)
            key_sum[there, :] += dot_nn(score, head_queries[h])
            query_sum[a, h * QK : (h + 1) * QK, :] += dot_nn(turned[h * QK : (h + 1) * QK, :], score)

    pair(a, True)

    @pl.loop(0, nb)
    def _(b):
        @pl.when(needed(meta, a, b, nb))
        def _():
            pair(b, False)

    @pl.when(a == nb - 1)
    def _():
        for b in range(nb):
            span = slice(b * rows, (b + 1) * rows)
            s = scale[span, :]
            grad_q = jnp.transpose(query_sum[b]) * (0.5 * s)
            out[span, :width] = grad_q.astype(BF)
            out[span, width : 2 * width] = (key_sum[span, :width] * (2.0 * s)).astype(BF)
            out[span, 2 * width :] = (value_sum[span, :] * s).astype(BF)


def block_spec(shape, index):
    return pl.BlockSpec(shape, index)


def whole(shape):
    return pl.BlockSpec(shape, lambda a, *_: (0,) * len(shape))


def attention_forward(meta, qkv, seg_col, seg_row, heads, rows):
    tokens = qkv.shape[0]
    nb = tokens // rows
    values = heads * VH
    return pl.pallas_call(
        functools.partial(forward_kernel, heads=heads, rows=rows, nb=nb),
        out_shape=(
            jax.ShapeDtypeStruct((tokens, values), BF),
            jax.ShapeDtypeStruct((tokens, heads), F32),
        ),
        grid_spec=pltpu.PrefetchScalarGridSpec(
            num_scalar_prefetch=1,
            grid=(nb,),
            in_specs=[whole(qkv.shape), whole(seg_col.shape), whole(seg_row.shape)],
            out_specs=[
                pl.BlockSpec((rows, values), lambda a, *_: (a, 0)),
                pl.BlockSpec((rows, heads), lambda a, *_: (a, 0)),
            ],
            scratch_shapes=[pltpu.VMEM((rows, values), F32), pltpu.VMEM((rows, values), F32)],
        ),
        cost_estimate=pl.CostEstimate(
            flops=4 * tokens * values, transcendentals=0, bytes_accessed=8 * tokens
        ),
        name="attention_forward",
    )(meta, qkv, seg_col, seg_row)


def attention_backward(meta, qkv, seg_col, seg_row, gm, mixed, den, scale, heads, rows):
    tokens = qkv.shape[0]
    nb = tokens // rows
    values = heads * VH
    width = heads * QK
    return pl.pallas_call(
        functools.partial(backward_kernel, heads=heads, rows=rows, nb=nb),
        out_shape=jax.ShapeDtypeStruct((tokens, 2 * width + values), BF),
        grid_spec=pltpu.PrefetchScalarGridSpec(
            num_scalar_prefetch=1,
            grid=(nb,),
            in_specs=[
                whole(qkv.shape),
                whole(seg_col.shape),
                whole(seg_row.shape),
                pl.BlockSpec((rows, values), lambda a, *_: (a, 0)),
                pl.BlockSpec((rows, values), lambda a, *_: (a, 0)),
                pl.BlockSpec((rows, heads), lambda a, *_: (a, 0)),
                whole(scale.shape),
            ],
            out_specs=whole((tokens, 2 * width + values)),
            scratch_shapes=[
                pltpu.VMEM((tokens, 128), F32),
                pltpu.VMEM((tokens, values), F32),
                pltpu.VMEM((nb, width, rows), F32),
            ],
        ),
        cost_estimate=pl.CostEstimate(
            flops=10 * tokens * values, transcendentals=0, bytes_accessed=16 * tokens
        ),
        name="attention_backward",
    )(meta, qkv, seg_col, seg_row, gm, mixed, den, scale)


def of_context(parts, c, nc):
    me = lax.axis_index(C)
    out = parts[0][...]
    for i in range(1, nc):
        near = lax.rem(me - 2 * (i // 2) + nc, nc)
        index = near if i % 2 == 0 else near + 1 - 2 * lax.rem(near, 2)
        out = jnp.where(index == c, parts[i][...], out)
    return out


def columns_kernel(*refs, nc, seg, groups):
    parts, weight, gain, out, along = refs[:nc], refs[nc], refs[nc + 1], refs[nc + 2], refs[nc + 3]
    total = jnp.zeros(along.shape, F32)
    for c in range(nc):
        part = of_context(parts, c, nc)
        for j in range(groups):
            place = slice((j * nc + c) * seg, (j * nc + c + 1) * seg)
            value = part[:, j * seg : (j + 1) * seg].astype(F32)
            total += jnp.sum(value * weight[:, place].astype(F32), axis=1, keepdims=True)
            out[:, place] = value * gain[...]
    along[...] = total


def finish_columns(parts, weight, gain, seg, groups):
    nc = len(parts)
    rows, width = weight.shape
    tile = next(t for t in (64, 32, 16, 8) if rows % t == 0)

    def spec(size):
        return pl.BlockSpec((tile, size), lambda i: (i, 0))

    return pl.pallas_call(
        functools.partial(columns_kernel, nc=nc, seg=seg, groups=groups),
        out_shape=(
            jax.ShapeDtypeStruct((rows, width), F32),
            jax.ShapeDtypeStruct((rows, 1), F32),
        ),
        grid=(rows // tile,),
        in_specs=[spec(parts[0].shape[1])] * nc + [spec(width), spec(1)],
        out_specs=[spec(width), spec(1)],
        cost_estimate=pl.CostEstimate(flops=0, transcendentals=0, bytes_accessed=1024),
        name="finish_columns",
    )(*parts, weight, gain)


def rows_kernel(*refs, nc):
    out = refs[nc]
    size = refs[0].shape[0]
    for c in range(nc):
        out[c * size : (c + 1) * size, :] = of_context(refs[:nc], c, nc).astype(F32)


def finish_rows(parts):
    nc = len(parts)
    rows, width = parts[0].shape
    tile = next(t for t in (512, 256, 128) if width % t == 0)
    return pl.pallas_call(
        functools.partial(rows_kernel, nc=nc),
        out_shape=jax.ShapeDtypeStruct((nc * rows, width), F32),
        grid=(width // tile,),
        in_specs=[pl.BlockSpec((rows, tile), lambda i: (0, i))] * nc,
        out_specs=pl.BlockSpec((nc * rows, tile), lambda i: (0, i)),
        cost_estimate=pl.CostEstimate(flops=0, transcendentals=0, bytes_accessed=1024),
        name="finish_rows",
    )(*parts)


def mm(a, b):
    return jnp.dot(a, b, preferred_element_type=F32)


def mm_tn(a, b):
    return lax.dot_general(a, b, (((0,), (0,)), ((), ())), preferred_element_type=F32)


def mm_nt(a, b):
    return lax.dot_general(a, b, (((1,), (1,)), ((), ())), preferred_element_type=F32)


def inverse_rms(values):
    return lax.rsqrt(jnp.mean(values * values, axis=-1, keepdims=True) + EPS)


def local(
    tokens,
    segment_ids,
    norm1_gain,
    w_query,
    w_key,
    w_value,
    w_out,
    norm2_gain,
    w_gate,
    w_up,
    w_down,
    cotangent,
):
    nc, nf = lax.axis_size(C), lax.axis_size(F)
    c = lax.axis_index(C)
    rows, width = tokens.shape[1], tokens.shape[2]
    heads = HEADS // nc
    qk = heads * QK
    hidden_all = w_gate.shape[1]
    seg_len = hidden_all // (nc * nf)
    hidden = seg_len * nf
    shard = w_gate.shape[0]

    own = tokens[0]
    grad_top = cotangent[0]
    gain_one = norm1_gain.astype(F32)[:, None]
    gain_two = norm2_gain.astype(F32)[:, None]

    def columns(weight, size):
        return lax.dynamic_slice_in_dim(weight, c * size, size, axis=1)

    part_qkv = (
        jnp.concatenate(
            [columns(w_query, qk), columns(w_key, qk), columns(w_value, heads * VH)], axis=1
        ).astype(F32)
        * gain_one
    ).astype(BF)

    def hidden_columns(weight):
        picked = lax.dynamic_index_in_dim(
            weight.reshape(shard, nf, nc, seg_len), c, axis=2, keepdims=False
        )
        return (picked.reshape(shard, hidden).astype(F32) * gain_two).astype(BF)

    part_out = group_pieces(w_out)
    part_gate = hidden_columns(w_gate)
    part_up = hidden_columns(w_up)
    part_down = lax.dynamic_slice_in_dim(w_down, c * seg_len, seg_len, axis=0)

    seg_all = jnp.concatenate(spread_direct(segment_ids[0]), axis=0)
    nb = nc
    seg_row = seg_all.reshape(nb, 1, rows)
    seg_col = seg_all.reshape(nb * rows, 1)
    meta = jnp.concatenate(
        [jnp.stack(spread_index()), seg_row[:, 0, 0], seg_row[:, 0, rows - 1]]
    ).astype(jnp.int32)

    line_qkv = gather_lines(part_qkv)
    other_qkv = swap_pieces(line_qkv, 1)
    x_parts = spread(own, [line_qkv, part_out])
    line_out = gather_lines(part_out)
    line_gate = gather_lines(part_gate)
    line_up = gather_lines(part_up)
    line_down = gather_lines(part_down)
    x_all = jnp.concatenate(x_parts, axis=0)
    scale_one = inverse_rms(x_all.astype(F32))
    full_qkv = assemble(line_qkv, other_qkv)
    g_parts = spread(after(grad_top, seg_all, x_all, *other_qkv))
    qkv = (mm(x_all, full_qkv) * scale_one).astype(BF)
    mixed, den = attention_forward(meta, qkv, seg_col, seg_row, heads, rows)

    def blocks(value):
        return [value[i * rows : (i + 1) * rows] for i in range(nb)]

    full_out = assemble(line_out, swap_pieces(line_out, 1))
    projected = mm(after(mixed, *g_parts), full_out).astype(BF)
    sums = add_cores(blocks(projected))
    other_gate = swap_pieces(after(line_gate, *sums), 2)
    residual = after(own.astype(F32) + add_chips(sums), other_gate[0])

    scale_two = inverse_rms(residual)
    unit_two = residual * scale_two
    full_gate = assemble(line_gate, other_gate)
    n_all = jnp.concatenate(spread(unit_two.astype(BF), other_gate), axis=0)
    g_all = jnp.concatenate(g_parts, axis=0)
    other_up = swap_pieces(after(line_up, unit_two), 1)
    other_down = swap_pieces(line_down, 2)
    gate = mm(after(n_all, line_down), full_gate)
    full_up = assemble(line_up, [after(part, gate) for part in other_up])
    up = mm(after(n_all, gate, other_down[0]), full_up)
    full_down = assemble(line_down, [after(part, up) for part in other_down])
    grad_hidden = mm_nt(after(g_all, up), full_down)
    sigmoid = jax.nn.sigmoid(gate)
    silu = gate * sigmoid
    act = (silu * up).astype(BF)
    grad_gate = (grad_hidden * up * sigmoid * (1.0 + gate * (1.0 - sigmoid))).astype(BF)
    grad_up = (grad_hidden * silu).astype(BF)
    back_two = (mm_nt(grad_gate, full_gate) + mm_nt(grad_up, full_up)).astype(BF)
    back_sums = add_cores(blocks(back_two))

    total_gate = mm_tn(n_all, after(grad_gate, *back_sums)).astype(BF)
    mine_gate, sent_gate = scatter_sides(total_gate, 2)
    total_up = mm_tn(n_all, after(grad_up, total_gate)).astype(BF)
    mine_up, sent_up = scatter_sides(total_up, 2)
    grad_unit_two = add_chips([after(back_sums[0], total_up, sent_gate[0])] + back_sums[1:])

    grad_residual = grad_top.astype(F32) + scale_two * (
        grad_unit_two - unit_two * jnp.mean(grad_unit_two * unit_two, axis=-1, keepdims=True)
    )
    branch = grad_residual.astype(BF)
    total_down = mm_tn(after(act, branch), g_all).astype(BF)
    mine_down, sent_down = scatter_sides(total_down, 2)
    projected_two = mm(after(act, total_down), full_down).astype(BF)
    both_gate = add_sides(mine_gate, sent_gate, total_down)
    sum_gate = scatter_lines(both_gate)
    b_all = jnp.concatenate(spread(branch, [projected_two, both_gate]), axis=0)
    out_sums = add_cores(blocks(after(projected_two, b_all)))

    grad_mixed = mm_nt(b_all, full_out)
    total_out = mm_tn(mixed, after(b_all, grad_mixed, sent_up[0])).astype(BF)
    mine_out, sent_out = scatter_sides(total_out)
    grad_qkv = attention_backward(
        meta, qkv, seg_col, seg_row, after(grad_mixed, total_out, *out_sums), mixed, den, scale_one, heads, rows
    )
    block_out = residual + after(add_chips([jnp.zeros_like(out_sums[0])] + out_sums[1:]), grad_qkv) + out_sums[0]
    back_one = mm_nt(after(grad_qkv, block_out, *sent_up), full_qkv).astype(BF)
    one_sums = add_cores(blocks(back_one))
    both_up = add_sides(mine_up, sent_up, *one_sums)
    sum_up = scatter_lines(both_up)
    total_qkv = mm_tn(x_all, after(grad_qkv, both_up, sum_gate, sent_down[0])).astype(BF)
    both_down = add_sides(mine_down, sent_down, total_qkv)
    mine_qkv, sent_qkv = scatter_sides(total_qkv)
    grad_unit_one = after(add_chips(one_sums), sum_up)
    sum_down = scatter_lines(both_down)
    both_out = add_sides(mine_out, sent_out, both_down, grad_unit_one)
    sum_out = scatter_lines(both_out)
    both_qkv = add_sides(mine_qkv, sent_qkv, both_out, grad_unit_one)
    sum_qkv = scatter_lines(both_qkv)
    sum_gate = after(sum_gate, both_qkv)
    sum_up = after(sum_up, both_qkv)
    sum_out = after(sum_out, both_qkv)

    unit_one = own.astype(F32) * inverse_rms(own.astype(F32))
    input_grad = grad_residual + grad_unit_one - unit_one * jnp.mean(
        grad_unit_one * unit_one, axis=-1, keepdims=True
    )

    def over_context(value):
        return spread(value.astype(BF))

    def from_hidden(value, weight):
        stacked = in_order(over_context(value)).reshape(nc, shard, nf, seg_len)
        grad = stacked.transpose(1, 2, 0, 3).reshape(shard, hidden_all).astype(F32)
        return grad * gain_two, jnp.sum(weight.astype(F32) * grad, axis=1, keepdims=True)

    grad_w_gate, along_gate = from_hidden(sum_gate, w_gate)
    grad_w_up, along_up = from_hidden(sum_up, w_up)
    qkv_parts = over_context(sum_qkv)

    def columns_of(first, size):
        return [part[:, first : first + size] for part in qkv_parts]

    grad_w_query, along_query = finish_columns(columns_of(0, qk), w_query, gain_one, qk, 1)
    grad_w_key, along_key = finish_columns(columns_of(qk, qk), w_key, gain_one, qk, 1)
    grad_w_value, along_value = finish_columns(
        columns_of(2 * qk, heads * VH), w_value, gain_one, heads * VH, 1
    )
    grad_w_down = finish_rows(over_context(sum_down))
    grad_w_out = ungroup_pieces(sum_out.astype(BF)).astype(F32)
    return (
        block_out.astype(BF)[None],
        input_grad[None],
        (along_query + along_key + along_value)[:, 0],
        grad_w_query,
        grad_w_key,
        grad_w_value,
        grad_w_out,
        (along_gate + along_up)[:, 0],
        grad_w_gate,
        grad_w_up,
        grad_w_down,
    )


def solution(mesh):
    rows = P(F, None)
    acts = P(F, C, None)
    return jax.shard_map(
        local,
        mesh=mesh,
        in_specs=(acts, P(F, C), P(F), rows, rows, rows, rows, P(F), rows, rows, rows, acts),
        out_specs=(acts, acts, P(F), rows, rows, rows, rows, P(F), rows, rows, rows),
        check_vma=False,
    )
```

```python
import functools

import jax
import jax.numpy as jnp
from jax import lax
from jax.experimental import pallas as pl
from jax.experimental.pallas import tpu as pltpu
from jax.sharding import PartitionSpec as P

HEADS = 16
QK = 16
VH = 128
EPS = 1e-05

C = "context"
F = "fsdp"
BF = jnp.bfloat16
F32 = jnp.float32


def after(value, *earlier):
    return lax.optimization_barrier((value,) + earlier)[0]


def lines():
    return lax.axis_size(F) // 2


def line_groups():
    m = lines()
    return [[2 * line + side for line in range(m)] for side in range(2)]


def side_swap(value):
    return lax.ppermute(value, F, [(j, j ^ 1) for j in range(lax.axis_size(F))])


def line_and_side():
    me = lax.axis_index(F)
    return me // 2, lax.rem(me, 2)


def scatter_sides(total):
    m = lines()
    _, side = line_and_side()
    parts = total.reshape(m, 2, total.shape[0] // (2 * m), total.shape[1])
    mine = lax.dynamic_index_in_dim(parts, side, 1, keepdims=False)
    return mine, side_swap(lax.dynamic_index_in_dim(parts, 1 - side, 1, keepdims=False))


def add_sides(mine, sent):
    both = (mine.astype(F32) + sent.astype(F32)).astype(BF)
    return both.reshape(-1, both.shape[-1])


def scatter_lines(total):
    return lax.psum_scatter(total, F, scatter_dimension=0, axis_index_groups=line_groups(), tiled=True)


def gather_lines(block):
    return lax.all_gather(block, F, axis=0, axis_index_groups=line_groups())


def assemble_kernel(own, *refs, m, pieces):
    side = lax.rem(lax.axis_index(F), 2)
    out, sems = refs[pieces], refs[pieces + 1]
    size = m // pieces
    copies = []
    for k in range(m):
        other = refs[k // size].at[k % size]
        copies.append(pltpu.make_async_copy(own.at[k], out.at[2 * k + side], sems.at[k]))
        copies.append(pltpu.make_async_copy(other, out.at[2 * k + 1 - side], sems.at[m + k]))
    for copy in copies:
        copy.start()
    for copy in copies:
        copy.wait()


def assemble(own, *other):
    m, rows, width = own.shape
    out = pl.pallas_call(
        functools.partial(assemble_kernel, m=m, pieces=len(other)),
        out_shape=jax.ShapeDtypeStruct((2 * m, rows, width), own.dtype),
        in_specs=[pl.BlockSpec(memory_space=pl.ANY)] * (1 + len(other)),
        out_specs=pl.BlockSpec(memory_space=pltpu.VMEM),
        scratch_shapes=[pltpu.SemaphoreType.DMA((2 * m,))],
        cost_estimate=pl.CostEstimate(flops=0, transcendentals=0, bytes_accessed=1024),
        name="assemble",
    )(own, *other)
    return out.reshape(2 * m * rows, width)


def chips():
    return lax.axis_size(C) // 2


def core_swap(value):
    n = lax.axis_size(C)
    return lax.ppermute(value, C, [(i, i ^ 1) for i in range(n)])


def chip_shift(value, k):
    n = lax.axis_size(C)
    return lax.ppermute(value, C, [(i, (i + 2 * k) % n) for i in range(n)])


def spread(block, marks=()):
    out = []
    for k in range(chips()):
        near = after(chip_shift(block, k), *marks) if k else block
        out += [near, core_swap(near)]
    return out


def spread_direct(block):
    n = lax.axis_size(C)
    return [
        lax.ppermute(block, C, [(i, (i + 2 * k) % n ^ h) for i in range(n)]) if k or h else block
        for k in range(chips())
        for h in range(2)
    ]


def spread_index():
    n, me = lax.axis_size(C), lax.axis_index(C)
    out = []
    for k in range(chips()):
        near = lax.rem(me - 2 * k + n, n)
        out += [near, near ^ 1]
    return out


def add_cores(parts):
    sums = []
    for k in range(chips()):
        both = parts[2 * k].astype(F32) + core_swap(parts[2 * k + 1]).astype(F32)
        sums.append(both.astype(BF) if k else both)
    return sums


def add_chips(sums):
    total = sums[0]
    for k in range(1, chips()):
        total = total + chip_shift(sums[k], -k).astype(F32)
    return total


def gather_back(parts):
    return add_chips(add_cores(parts))


def in_order(parts):
    out = jnp.zeros((len(parts),) + parts[0].shape, parts[0].dtype)
    for index, part in zip(spread_index(), parts):
        out = lax.dynamic_update_index_in_dim(out, part, index, 0)
    return out


def group_pairs(back):
    nc, nf = lax.axis_size(C), lax.axis_size(F)
    m = nf // nc
    out = []
    for q in range(nc):
        pairs = [
            (c * nf + m * c + s, c * nf + s * nc + q) for c in range(nc) for s in range(m)
        ]
        out.append([(b, a) for a, b in pairs] if back else pairs)
    return out


def group_pieces(shard):
    nc = lax.axis_size(C)
    rows = shard.shape[0] // nc
    out = None
    for q, pairs in enumerate(group_pairs(False)):
        got = lax.ppermute(shard[q * rows : (q + 1) * rows], (C, F), pairs)
        out = got if out is None else out + got
    return out


def ungroup_pieces(piece):
    nc, nf = lax.axis_size(C), lax.axis_size(F)
    m = nf // nc
    shard = jnp.concatenate(
        [lax.ppermute(piece, (C, F), pairs) for pairs in group_pairs(True)], axis=0
    )
    out = shard
    for k in range(1, nc // 2):
        out = out + lax.ppermute(
            shard, (C, F), [((j // m) * nf + j, ((j // m + 2 * k) % nc) * nf + j) for j in range(nf)]
        )
    holders = [((j // m) % 2, j) for j in range(nf)]
    swap = [
        ((2 * x + h) * nf + j, (2 * x + 1 - h) * nf + j) for h, j in holders for x in range(nc // 2)
    ]
    return out + lax.ppermute(out, (C, F), swap)


def dot_nt(a, b):
    return lax.dot_general(a, b, (((1,), (1,)), ((), ())), preferred_element_type=F32)


def dot_nn(a, b):
    return lax.dot_general(a, b, (((1,), (0,)), ((), ())), preferred_element_type=F32)


def with_one(values, width):
    rows = values.shape[0]
    padded = jnp.concatenate([values, jnp.zeros((rows, 128 - width), values.dtype)], axis=1)
    lane = lax.broadcasted_iota(jnp.int32, (rows, 128), 1)
    return jnp.where(lane == width, jnp.ones_like(padded), padded)


def one_head(values, head, width):
    lane = lax.broadcasted_iota(jnp.int32, values.shape, 1)
    keep = jnp.logical_or(lane // QK == head, lane == width)
    return jnp.where(keep, values, jnp.zeros_like(values))


def needed(meta, a, b, nb):
    before = meta[b] < meta[a]
    return jnp.logical_and(before, meta[nb + a] <= meta[2 * nb + b])


def forward_kernel(meta, qkv, seg_col, seg_row, mixed, den, num_sum, den_sum, *, heads, rows, nb):
    width = heads * QK
    a = pl.program_id(0)
    here = pl.ds(pl.multiple_of(a * rows, rows), rows)
    queries = with_one(qkv[here, :width] * 0.25, width)
    seg_q = seg_col[here, :]
    num_sum[...] = jnp.zeros_like(num_sum)
    den_sum[...] = jnp.zeros_like(den_sum)

    def pair(b, diagonal):
        there = pl.ds(pl.multiple_of(b * rows, rows), rows)
        keys = with_one(qkv[there, width : 2 * width], width)
        allowed = seg_q == seg_row[b]
        if diagonal:
            t = lax.broadcasted_iota(jnp.int32, (rows, rows), 0)
            u = lax.broadcasted_iota(jnp.int32, (rows, rows), 1)
            allowed = jnp.logical_and(allowed, u <= t)
        for h in range(heads):
            shifted = dot_nt(one_head(queries, h, width), keys)
            weight = jnp.where(allowed, shifted * shifted + 1.0, 0.0)
            lanes = slice(h * VH, (h + 1) * VH)
            values = qkv[there, 2 * width + h * VH : 2 * width + (h + 1) * VH]
            num_sum[:, lanes] += dot_nn(weight.astype(BF), values)
            den_sum[:, lanes] += jnp.broadcast_to(
                jnp.sum(weight, axis=1, keepdims=True), (rows, VH)
            )

    pair(a, True)

    @pl.loop(0, nb)
    def _(b):
        @pl.when(needed(meta, a, b, nb))
        def _():
            pair(b, False)

    mixed[...] = (num_sum[...] / den_sum[...]).astype(BF)
    for h in range(heads):
        den[:, h : h + 1] = den_sum[:, h * VH : h * VH + 1]


def backward_kernel(
    meta, qkv, seg_col, seg_row, gm, mixed, den, scale, out, key_sum, value_sum, query_sum, *, heads, rows, nb
):
    width = heads * QK
    a = pl.program_id(0)
    here = pl.ds(pl.multiple_of(a * rows, rows), rows)
    queries = with_one(qkv[here, :width] * 0.25, width)
    seg_q = seg_row[a]

    @pl.when(a == 0)
    def _():
        key_sum[...] = jnp.zeros_like(key_sum)
        value_sum[...] = jnp.zeros_like(value_sum)
        query_sum[...] = jnp.zeros_like(query_sum)

    grads, offsets, head_queries = [], [], []
    for h in range(heads):
        g = gm[:, h * VH : (h + 1) * VH].astype(F32)
        d = den[:, h : h + 1]
        grads.append((g / d).astype(BF))
        inner = -jnp.sum(g * mixed[:, h * VH : (h + 1) * VH].astype(F32), axis=1, keepdims=True) / d
        offsets.append(jnp.transpose(jnp.broadcast_to(inner, (rows, 128)))[0:1, :])
        head_queries.append(one_head(queries, h, width))

    def pair(b, diagonal):
        there = pl.ds(pl.multiple_of(b * rows, rows), rows)
        raw = qkv[there, width : 2 * width]
        keys = with_one(raw, width)
        turned = jnp.transpose(keys)
        allowed = seg_col[there, :] == seg_q
        if diagonal:
            u = lax.broadcasted_iota(jnp.int32, (rows, rows), 0)
            t = lax.broadcasted_iota(jnp.int32, (rows, rows), 1)
            allowed = jnp.logical_and(allowed, u <= t)
        for h in range(heads):
            lanes = slice(h * VH, (h + 1) * VH)
            shifted = dot_nt(keys, head_queries[h])
            weight = jnp.where(allowed, shifted * shifted + 1.0, 0.0).astype(BF)
            value_sum[there, lanes] += dot_nn(weight, grads[h])
            values = qkv[there, 2 * width + h * VH : 2 * width + (h + 1) * VH]
            grad = dot_nt(values, grads[h]) + offsets[h]
            score = jnp.where(allowed, grad * shifted, 0.0).astype(BF)
            key_sum[there, :] += dot_nn(score, head_queries[h])
            query_sum[a, h * QK : (h + 1) * QK, :] += dot_nn(turned[h * QK : (h + 1) * QK, :], score)

    pair(a, True)

    @pl.loop(0, nb)
    def _(b):
        @pl.when(needed(meta, a, b, nb))
        def _():
            pair(b, False)

    @pl.when(a == nb - 1)
    def _():
        for b in range(nb):
            span = slice(b * rows, (b + 1) * rows)
            s = scale[span, :]
            grad_q = jnp.transpose(query_sum[b]) * (0.5 * s)
            out[span, :width] = grad_q.astype(BF)
            out[span, width : 2 * width] = (key_sum[span, :width] * (2.0 * s)).astype(BF)
            out[span, 2 * width :] = (value_sum[span, :] * s).astype(BF)


def block_spec(shape, index):
    return pl.BlockSpec(shape, index)


def whole(shape):
    return pl.BlockSpec(shape, lambda a, *_: (0,) * len(shape))


def attention_forward(meta, qkv, seg_col, seg_row, heads, rows):
    tokens = qkv.shape[0]
    nb = tokens // rows
    values = heads * VH
    return pl.pallas_call(
        functools.partial(forward_kernel, heads=heads, rows=rows, nb=nb),
        out_shape=(
            jax.ShapeDtypeStruct((tokens, values), BF),
            jax.ShapeDtypeStruct((tokens, heads), F32),
        ),
        grid_spec=pltpu.PrefetchScalarGridSpec(
            num_scalar_prefetch=1,
            grid=(nb,),
            in_specs=[whole(qkv.shape), whole(seg_col.shape), whole(seg_row.shape)],
            out_specs=[
                pl.BlockSpec((rows, values), lambda a, *_: (a, 0)),
                pl.BlockSpec((rows, heads), lambda a, *_: (a, 0)),
            ],
            scratch_shapes=[pltpu.VMEM((rows, values), F32), pltpu.VMEM((rows, values), F32)],
        ),
        cost_estimate=pl.CostEstimate(
            flops=4 * tokens * values, transcendentals=0, bytes_accessed=8 * tokens
        ),
        name="attention_forward",
    )(meta, qkv, seg_col, seg_row)


def attention_backward(meta, qkv, seg_col, seg_row, gm, mixed, den, scale, heads, rows):
    tokens = qkv.shape[0]
    nb = tokens // rows
    values = heads * VH
    width = heads * QK
    return pl.pallas_call(
        functools.partial(backward_kernel, heads=heads, rows=rows, nb=nb),
        out_shape=jax.ShapeDtypeStruct((tokens, 2 * width + values), BF),
        grid_spec=pltpu.PrefetchScalarGridSpec(
            num_scalar_prefetch=1,
            grid=(nb,),
            in_specs=[
                whole(qkv.shape),
                whole(seg_col.shape),
                whole(seg_row.shape),
                pl.BlockSpec((rows, values), lambda a, *_: (a, 0)),
                pl.BlockSpec((rows, values), lambda a, *_: (a, 0)),
                pl.BlockSpec((rows, heads), lambda a, *_: (a, 0)),
                whole(scale.shape),
            ],
            out_specs=whole((tokens, 2 * width + values)),
            scratch_shapes=[
                pltpu.VMEM((tokens, 128), F32),
                pltpu.VMEM((tokens, values), F32),
                pltpu.VMEM((nb, width, rows), F32),
            ],
        ),
        cost_estimate=pl.CostEstimate(
            flops=10 * tokens * values, transcendentals=0, bytes_accessed=16 * tokens
        ),
        name="attention_backward",
    )(meta, qkv, seg_col, seg_row, gm, mixed, den, scale)


def of_context(parts, c, nc):
    me = lax.axis_index(C)
    out = parts[0][...]
    for i in range(1, nc):
        near = lax.rem(me - 2 * (i // 2) + nc, nc)
        index = near if i % 2 == 0 else near + 1 - 2 * lax.rem(near, 2)
        out = jnp.where(index == c, parts[i][...], out)
    return out


def columns_kernel(*refs, nc, seg, groups):
    parts, weight, gain, out, along = refs[:nc], refs[nc], refs[nc + 1], refs[nc + 2], refs[nc + 3]
    total = jnp.zeros(along.shape, F32)
    for c in range(nc):
        part = of_context(parts, c, nc)
        for j in range(groups):
            place = slice((j * nc + c) * seg, (j * nc + c + 1) * seg)
            value = part[:, j * seg : (j + 1) * seg].astype(F32)
            total += jnp.sum(value * weight[:, place].astype(F32), axis=1, keepdims=True)
            out[:, place] = value * gain[...]
    along[...] = total


def finish_columns(parts, weight, gain, seg, groups):
    nc = len(parts)
    rows, width = weight.shape
    tile = next(t for t in (64, 32, 16, 8) if rows % t == 0)

    def spec(size):
        return pl.BlockSpec((tile, size), lambda i: (i, 0))

    return pl.pallas_call(
        functools.partial(columns_kernel, nc=nc, seg=seg, groups=groups),
        out_shape=(
            jax.ShapeDtypeStruct((rows, width), F32),
            jax.ShapeDtypeStruct((rows, 1), F32),
        ),
        grid=(rows // tile,),
        in_specs=[spec(parts[0].shape[1])] * nc + [spec(width), spec(1)],
        out_specs=[spec(width), spec(1)],
        cost_estimate=pl.CostEstimate(flops=0, transcendentals=0, bytes_accessed=1024),
        name="finish_columns",
    )(*parts, weight, gain)


def rows_kernel(*refs, nc):
    out = refs[nc]
    size = refs[0].shape[0]
    for c in range(nc):
        out[c * size : (c + 1) * size, :] = of_context(refs[:nc], c, nc).astype(F32)


def finish_rows(parts):
    nc = len(parts)
    rows, width = parts[0].shape
    tile = next(t for t in (512, 256, 128) if width % t == 0)
    return pl.pallas_call(
        functools.partial(rows_kernel, nc=nc),
        out_shape=jax.ShapeDtypeStruct((nc * rows, width), F32),
        grid=(width // tile,),
        in_specs=[pl.BlockSpec((rows, tile), lambda i: (0, i))] * nc,
        out_specs=pl.BlockSpec((nc * rows, tile), lambda i: (0, i)),
        cost_estimate=pl.CostEstimate(flops=0, transcendentals=0, bytes_accessed=1024),
        name="finish_rows",
    )(*parts)


def mm(a, b):
    return jnp.dot(a, b, preferred_element_type=F32)


def mm_tn(a, b):
    return lax.dot_general(a, b, (((0,), (0,)), ((), ())), preferred_element_type=F32)


def mm_nt(a, b):
    return lax.dot_general(a, b, (((1,), (1,)), ((), ())), preferred_element_type=F32)


def inverse_rms(values):
    return lax.rsqrt(jnp.mean(values * values, axis=-1, keepdims=True) + EPS)


def local(
    tokens,
    segment_ids,
    norm1_gain,
    w_query,
    w_key,
    w_value,
    w_out,
    norm2_gain,
    w_gate,
    w_up,
    w_down,
    cotangent,
):
    nc, nf = lax.axis_size(C), lax.axis_size(F)
    c = lax.axis_index(C)
    rows, width = tokens.shape[1], tokens.shape[2]
    heads = HEADS // nc
    qk = heads * QK
    hidden_all = w_gate.shape[1]
    seg_len = hidden_all // (nc * nf)
    hidden = seg_len * nf
    shard = w_gate.shape[0]

    own = tokens[0]
    grad_top = cotangent[0]
    gain_one = norm1_gain.astype(F32)[:, None]
    gain_two = norm2_gain.astype(F32)[:, None]

    def columns(weight, size):
        return lax.dynamic_slice_in_dim(weight, c * size, size, axis=1)

    part_qkv = (
        jnp.concatenate(
            [columns(w_query, qk), columns(w_key, qk), columns(w_value, heads * VH)], axis=1
        ).astype(F32)
        * gain_one
    ).astype(BF)

    def hidden_columns(weight):
        picked = lax.dynamic_index_in_dim(
            weight.reshape(shard, nf, nc, seg_len), c, axis=2, keepdims=False
        )
        return (picked.reshape(shard, hidden).astype(F32) * gain_two).astype(BF)

    part_out = group_pieces(w_out)
    part_gate = hidden_columns(w_gate)
    part_up = hidden_columns(w_up)
    part_down = lax.dynamic_slice_in_dim(w_down, c * seg_len, seg_len, axis=0)

    seg_all = jnp.concatenate(spread_direct(segment_ids[0]), axis=0)
    nb = nc
    seg_row = seg_all.reshape(nb, 1, rows)
    seg_col = seg_all.reshape(nb * rows, 1)
    meta = jnp.concatenate(
        [jnp.stack(spread_index()), seg_row[:, 0, 0], seg_row[:, 0, rows - 1]]
    ).astype(jnp.int32)

    line_qkv = gather_lines(part_qkv)
    x_parts = spread(own, [line_qkv])
    line_out = gather_lines(after(part_out, x_parts[-2]))
    line_gate = gather_lines(part_gate)
    line_up = gather_lines(part_up)
    line_down = gather_lines(part_down)
    x_all = jnp.concatenate(x_parts, axis=0)
    scale_one = inverse_rms(x_all.astype(F32))
    full_qkv = assemble(line_qkv, side_swap(line_qkv))
    g_parts = spread(after(grad_top, seg_all, x_all))
    qkv = (mm(x_all, full_qkv) * scale_one).astype(BF)
    mixed, den = attention_forward(meta, qkv, seg_col, seg_row, heads, rows)

    def blocks(value):
        return [value[i * rows : (i + 1) * rows] for i in range(nb)]

    full_out = assemble(line_out, side_swap(line_out))
    projected = mm(after(mixed, *g_parts), full_out).astype(BF)
    sums = add_cores(blocks(projected))
    low, high = jnp.split(after(line_gate, *sums), 2)
    other_gate = [side_swap(low), side_swap(high)]
    residual = after(own.astype(F32) + add_chips(sums), other_gate[0])

    scale_two = inverse_rms(residual)
    unit_two = residual * scale_two
    full_gate = assemble(line_gate, *other_gate)
    n_all = jnp.concatenate(spread(unit_two.astype(BF)), axis=0)
    g_all = jnp.concatenate(g_parts, axis=0)
    other_up = side_swap(after(line_up, unit_two))
    gate = mm(n_all, full_gate)
    full_up = assemble(line_up, after(other_up, gate))
    full_down = assemble(line_down, side_swap(after(line_down, n_all)))
    up = mm(after(n_all, gate), full_up)
    grad_hidden = mm_nt(after(g_all, up), full_down)
    sigmoid = jax.nn.sigmoid(gate)
    silu = gate * sigmoid
    act = (silu * up).astype(BF)
    grad_gate = (grad_hidden * up * sigmoid * (1.0 + gate * (1.0 - sigmoid))).astype(BF)
    grad_up = (grad_hidden * silu).astype(BF)
    back_two = (mm_nt(grad_gate, full_gate) + mm_nt(grad_up, full_up)).astype(BF)
    back_sums = add_cores(blocks(back_two))

    total_gate = mm_tn(n_all, after(grad_gate, *back_sums)).astype(BF)
    mine_gate, sent_gate = scatter_sides(total_gate)
    total_up = mm_tn(n_all, after(grad_up, total_gate)).astype(BF)
    mine_up, sent_up = scatter_sides(total_up)
    grad_unit_two = add_chips([after(back_sums[0], total_up)] + back_sums[1:])

    grad_residual = grad_top.astype(F32) + scale_two * (
        grad_unit_two - unit_two * jnp.mean(grad_unit_two * unit_two, axis=-1, keepdims=True)
    )
    branch = grad_residual.astype(BF)
    total_down = mm_tn(after(act, branch), g_all).astype(BF)
    mine_down, sent_down = scatter_sides(total_down)
    projected_two = mm(after(act, total_down), full_down).astype(BF)
    both_gate = add_sides(mine_gate, after(sent_gate, total_down))
    sum_gate = scatter_lines(both_gate)
    b_all = jnp.concatenate(spread(branch, [projected_two, both_gate]), axis=0)
    out_sums = add_cores(blocks(after(projected_two, b_all)))

    grad_mixed = mm_nt(b_all, full_out)
    total_out = mm_tn(mixed, after(b_all, grad_mixed)).astype(BF)
    mine_out, sent_out = scatter_sides(total_out)
    grad_qkv = attention_backward(
        meta, qkv, seg_col, seg_row, after(grad_mixed, total_out, *out_sums), mixed, den, scale_one, heads, rows
    )
    block_out = residual + after(add_chips([jnp.zeros_like(out_sums[0])] + out_sums[1:]), grad_qkv) + out_sums[0]
    both_up = add_sides(mine_up, after(sent_up, grad_qkv))
    sum_up = scatter_lines(both_up)
    back_one = mm_nt(after(grad_qkv, block_out, both_up), full_qkv).astype(BF)
    one_sums = add_cores(blocks(back_one))
    total_qkv = mm_tn(x_all, after(grad_qkv, sum_gate, *one_sums)).astype(BF)
    mine_qkv, sent_qkv = scatter_sides(total_qkv)
    grad_unit_one = add_chips(one_sums)
    both_down = add_sides(mine_down, after(sent_down, total_qkv, grad_unit_one))
    sum_down = scatter_lines(both_down)
    both_out = add_sides(mine_out, after(sent_out, both_down, sum_up))
    sum_out = scatter_lines(both_out)
    both_qkv = add_sides(mine_qkv, after(sent_qkv, both_out, sum_down))
    sum_qkv = scatter_lines(both_qkv)
    sum_gate = after(sum_gate, both_out)
    sum_up = after(sum_up, both_out)
    sum_out = after(sum_out, both_qkv)

    unit_one = own.astype(F32) * inverse_rms(own.astype(F32))
    input_grad = grad_residual + grad_unit_one - unit_one * jnp.mean(
        grad_unit_one * unit_one, axis=-1, keepdims=True
    )

    def over_context(value):
        return spread(value.astype(BF))

    def from_hidden(value, weight):
        stacked = in_order(over_context(value)).reshape(nc, shard, nf, seg_len)
        grad = stacked.transpose(1, 2, 0, 3).reshape(shard, hidden_all).astype(F32)
        return grad * gain_two, jnp.sum(weight.astype(F32) * grad, axis=1, keepdims=True)

    grad_w_gate, along_gate = from_hidden(sum_gate, w_gate)
    grad_w_up, along_up = from_hidden(sum_up, w_up)
    qkv_parts = over_context(sum_qkv)

    def columns_of(first, size):
        return [part[:, first : first + size] for part in qkv_parts]

    grad_w_query, along_query = finish_columns(columns_of(0, qk), w_query, gain_one, qk, 1)
    grad_w_key, along_key = finish_columns(columns_of(qk, qk), w_key, gain_one, qk, 1)
    grad_w_value, along_value = finish_columns(
        columns_of(2 * qk, heads * VH), w_value, gain_one, heads * VH, 1
    )
    grad_w_down = finish_rows(over_context(sum_down))
    grad_w_out = ungroup_pieces(sum_out.astype(BF)).astype(F32)
    return (
        block_out.astype(BF)[None],
        input_grad[None],
        (along_query + along_key + along_value)[:, 0],
        grad_w_query,
        grad_w_key,
        grad_w_value,
        grad_w_out,
        (along_gate + along_up)[:, 0],
        grad_w_gate,
        grad_w_up,
        grad_w_down,
    )


def solution(mesh):
    rows = P(F, None)
    acts = P(F, C, None)
    return jax.shard_map(
        local,
        mesh=mesh,
        in_specs=(acts, P(F, C), P(F), rows, rows, rows, rows, P(F), rows, rows, rows, acts),
        out_specs=(acts, acts, P(F), rows, rows, rows, rows, P(F), rows, rows, rows),
        check_vma=False,
    )
```

```python
import functools

import jax
import jax.numpy as jnp
from jax import lax
from jax.experimental import pallas as pl
from jax.experimental.pallas import tpu as pltpu
from jax.sharding import PartitionSpec as P

HEADS = 16
QK = 16
VH = 128
EPS = 1e-05

C = "context"
F = "fsdp"
BF = jnp.bfloat16
F32 = jnp.float32


def after(value, *earlier):
    return lax.optimization_barrier((value,) + earlier)[0]


def lines():
    return lax.axis_size(F) // 2


def line_groups():
    m = lines()
    return [[2 * line + side for line in range(m)] for side in range(2)]


def side_swap(value):
    return lax.ppermute(value, F, [(j, j ^ 1) for j in range(lax.axis_size(F))])


def line_and_side():
    me = lax.axis_index(F)
    return me // 2, lax.rem(me, 2)


def scatter_sides(total, pieces=1):
    m = lines()
    _, side = line_and_side()
    parts = total.reshape(m, 2, total.shape[0] // (2 * m), total.shape[1])
    mine = lax.dynamic_index_in_dim(parts, side, 1, keepdims=False)
    theirs = lax.dynamic_index_in_dim(parts, 1 - side, 1, keepdims=False)
    return mine, [side_swap(part) for part in jnp.split(theirs, pieces)]


def add_sides(mine, sent, *marks):
    sent = jnp.concatenate([after(sent[0], *marks)] + sent[1:], axis=0)
    both = (mine.astype(F32) + sent.astype(F32)).astype(BF)
    return both.reshape(-1, both.shape[-1])


def scatter_lines(total):
    return lax.psum_scatter(total, F, scatter_dimension=0, axis_index_groups=line_groups(), tiled=True)


def gather_lines(block):
    return lax.all_gather(block, F, axis=0, axis_index_groups=line_groups())


def assemble_kernel(own, *refs, m, pieces):
    side = lax.rem(lax.axis_index(F), 2)
    out, sems = refs[pieces], refs[pieces + 1]
    size = m // pieces
    copies = []
    for k in range(m):
        other = refs[k // size].at[k % size]
        copies.append(pltpu.make_async_copy(own.at[k], out.at[2 * k + side], sems.at[k]))
        copies.append(pltpu.make_async_copy(other, out.at[2 * k + 1 - side], sems.at[m + k]))
    for copy in copies:
        copy.start()
    for copy in copies:
        copy.wait()


def assemble(own, *other):
    m, rows, width = own.shape
    out = pl.pallas_call(
        functools.partial(assemble_kernel, m=m, pieces=len(other)),
        out_shape=jax.ShapeDtypeStruct((2 * m, rows, width), own.dtype),
        in_specs=[pl.BlockSpec(memory_space=pl.ANY)] * (1 + len(other)),
        out_specs=pl.BlockSpec(memory_space=pltpu.VMEM),
        scratch_shapes=[pltpu.SemaphoreType.DMA((2 * m,))],
        cost_estimate=pl.CostEstimate(flops=0, transcendentals=0, bytes_accessed=1024),
        name="assemble",
    )(own, *other)
    return out.reshape(2 * m * rows, width)


def chips():
    return lax.axis_size(C) // 2


def core_swap(value):
    n = lax.axis_size(C)
    return lax.ppermute(value, C, [(i, i ^ 1) for i in range(n)])


def chip_shift(value, k):
    n = lax.axis_size(C)
    return lax.ppermute(value, C, [(i, (i + 2 * k) % n) for i in range(n)])


def spread(block, marks=()):
    out = []
    for k in range(chips()):
        near = after(chip_shift(block, k), *marks) if k else block
        out += [near, core_swap(near)]
    return out


def spread_direct(block):
    n = lax.axis_size(C)
    return [
        lax.ppermute(block, C, [(i, (i + 2 * k) % n ^ h) for i in range(n)]) if k or h else block
        for k in range(chips())
        for h in range(2)
    ]


def spread_index():
    n, me = lax.axis_size(C), lax.axis_index(C)
    out = []
    for k in range(chips()):
        near = lax.rem(me - 2 * k + n, n)
        out += [near, near ^ 1]
    return out


def add_cores(parts):
    sums = []
    for k in range(chips()):
        both = parts[2 * k].astype(F32) + core_swap(parts[2 * k + 1]).astype(F32)
        sums.append(both.astype(BF) if k else both)
    return sums


def add_chips(sums):
    total = sums[0]
    for k in range(1, chips()):
        total = total + chip_shift(sums[k], -k).astype(F32)
    return total


def gather_back(parts):
    return add_chips(add_cores(parts))


def in_order(parts):
    out = jnp.zeros((len(parts),) + parts[0].shape, parts[0].dtype)
    for index, part in zip(spread_index(), parts):
        out = lax.dynamic_update_index_in_dim(out, part, index, 0)
    return out


def group_pairs(back):
    nc, nf = lax.axis_size(C), lax.axis_size(F)
    m = nf // nc
    out = []
    for q in range(nc):
        pairs = [
            (c * nf + m * c + s, c * nf + s * nc + q) for c in range(nc) for s in range(m)
        ]
        out.append([(b, a) for a, b in pairs] if back else pairs)
    return out


def group_pieces(shard):
    nc = lax.axis_size(C)
    rows = shard.shape[0] // nc
    out = None
    for q, pairs in enumerate(group_pairs(False)):
        got = lax.ppermute(shard[q * rows : (q + 1) * rows], (C, F), pairs)
        out = got if out is None else out + got
    return out


def ungroup_pieces(piece):
    nc, nf = lax.axis_size(C), lax.axis_size(F)
    m = nf // nc
    shard = jnp.concatenate(
        [lax.ppermute(piece, (C, F), pairs) for pairs in group_pairs(True)], axis=0
    )
    out = shard
    for k in range(1, nc // 2):
        out = out + lax.ppermute(
            shard, (C, F), [((j // m) * nf + j, ((j // m + 2 * k) % nc) * nf + j) for j in range(nf)]
        )
    holders = [((j // m) % 2, j) for j in range(nf)]
    swap = [
        ((2 * x + h) * nf + j, (2 * x + 1 - h) * nf + j) for h, j in holders for x in range(nc // 2)
    ]
    return out + lax.ppermute(out, (C, F), swap)


def dot_nt(a, b):
    return lax.dot_general(a, b, (((1,), (1,)), ((), ())), preferred_element_type=F32)


def dot_nn(a, b):
    return lax.dot_general(a, b, (((1,), (0,)), ((), ())), preferred_element_type=F32)


def with_one(values, width):
    rows = values.shape[0]
    padded = jnp.concatenate([values, jnp.zeros((rows, 128 - width), values.dtype)], axis=1)
    lane = lax.broadcasted_iota(jnp.int32, (rows, 128), 1)
    return jnp.where(lane == width, jnp.ones_like(padded), padded)


def one_head(values, head, width):
    lane = lax.broadcasted_iota(jnp.int32, values.shape, 1)
    keep = jnp.logical_or(lane // QK == head, lane == width)
    return jnp.where(keep, values, jnp.zeros_like(values))


def needed(meta, a, b, nb):
    before = meta[b] < meta[a]
    return jnp.logical_and(before, meta[nb + a] <= meta[2 * nb + b])


def forward_kernel(meta, qkv, seg_col, seg_row, mixed, den, num_sum, den_sum, *, heads, rows, nb):
    width = heads * QK
    a = pl.program_id(0)
    here = pl.ds(pl.multiple_of(a * rows, rows), rows)
    queries = with_one(qkv[here, :width] * 0.25, width)
    seg_q = seg_col[here, :]
    num_sum[...] = jnp.zeros_like(num_sum)
    den_sum[...] = jnp.zeros_like(den_sum)

    def pair(b, diagonal):
        there = pl.ds(pl.multiple_of(b * rows, rows), rows)
        keys = with_one(qkv[there, width : 2 * width], width)
        allowed = seg_q == seg_row[b]
        if diagonal:
            t = lax.broadcasted_iota(jnp.int32, (rows, rows), 0)
            u = lax.broadcasted_iota(jnp.int32, (rows, rows), 1)
            allowed = jnp.logical_and(allowed, u <= t)
        for h in range(heads):
            shifted = dot_nt(one_head(queries, h, width), keys)
            weight = jnp.where(allowed, shifted * shifted + 1.0, 0.0)
            lanes = slice(h * VH, (h + 1) * VH)
            values = qkv[there, 2 * width + h * VH : 2 * width + (h + 1) * VH]
            num_sum[:, lanes] += dot_nn(weight.astype(BF), values)
            den_sum[:, lanes] += jnp.broadcast_to(
                jnp.sum(weight, axis=1, keepdims=True), (rows, VH)
            )

    pair(a, True)

    @pl.loop(0, nb)
    def _(b):
        @pl.when(needed(meta, a, b, nb))
        def _():
            pair(b, False)

    mixed[...] = (num_sum[...] / den_sum[...]).astype(BF)
    for h in range(heads):
        den[:, h : h + 1] = den_sum[:, h * VH : h * VH + 1]


def backward_kernel(
    meta, qkv, seg_col, seg_row, gm, mixed, den, scale, out, key_sum, value_sum, query_sum, *, heads, rows, nb
):
    width = heads * QK
    a = pl.program_id(0)
    here = pl.ds(pl.multiple_of(a * rows, rows), rows)
    queries = with_one(qkv[here, :width] * 0.25, width)
    seg_q = seg_row[a]

    @pl.when(a == 0)
    def _():
        key_sum[...] = jnp.zeros_like(key_sum)
        value_sum[...] = jnp.zeros_like(value_sum)
        query_sum[...] = jnp.zeros_like(query_sum)

    grads, offsets, head_queries = [], [], []
    for h in range(heads):
        g = gm[:, h * VH : (h + 1) * VH].astype(F32)
        d = den[:, h : h + 1]
        grads.append((g / d).astype(BF))
        inner = -jnp.sum(g * mixed[:, h * VH : (h + 1) * VH].astype(F32), axis=1, keepdims=True) / d
        offsets.append(jnp.transpose(jnp.broadcast_to(inner, (rows, 128)))[0:1, :])
        head_queries.append(one_head(queries, h, width))

    def pair(b, diagonal):
        there = pl.ds(pl.multiple_of(b * rows, rows), rows)
        raw = qkv[there, width : 2 * width]
        keys = with_one(raw, width)
        turned = jnp.transpose(keys)
        allowed = seg_col[there, :] == seg_q
        if diagonal:
            u = lax.broadcasted_iota(jnp.int32, (rows, rows), 0)
            t = lax.broadcasted_iota(jnp.int32, (rows, rows), 1)
            allowed = jnp.logical_and(allowed, u <= t)
        for h in range(heads):
            lanes = slice(h * VH, (h + 1) * VH)
            shifted = dot_nt(keys, head_queries[h])
            weight = jnp.where(allowed, shifted * shifted + 1.0, 0.0).astype(BF)
            value_sum[there, lanes] += dot_nn(weight, grads[h])
            values = qkv[there, 2 * width + h * VH : 2 * width + (h + 1) * VH]
            grad = dot_nt(values, grads[h]) + offsets[h]
            score = jnp.where(allowed, grad * shifted, 0.0).astype(BF)
            key_sum[there, :] += dot_nn(score, head_queries[h])
            query_sum[a, h * QK : (h + 1) * QK, :] += dot_nn(turned[h * QK : (h + 1) * QK, :], score)

    pair(a, True)

    @pl.loop(0, nb)
    def _(b):
        @pl.when(needed(meta, a, b, nb))
        def _():
            pair(b, False)

    @pl.when(a == nb - 1)
    def _():
        for b in range(nb):
            span = slice(b * rows, (b + 1) * rows)
            s = scale[span, :]
            grad_q = jnp.transpose(query_sum[b]) * (0.5 * s)
            out[span, :width] = grad_q.astype(BF)
            out[span, width : 2 * width] = (key_sum[span, :width] * (2.0 * s)).astype(BF)
            out[span, 2 * width :] = (value_sum[span, :] * s).astype(BF)


def block_spec(shape, index):
    return pl.BlockSpec(shape, index)


def whole(shape):
    return pl.BlockSpec(shape, lambda a, *_: (0,) * len(shape))


def attention_forward(meta, qkv, seg_col, seg_row, heads, rows):
    tokens = qkv.shape[0]
    nb = tokens // rows
    values = heads * VH
    return pl.pallas_call(
        functools.partial(forward_kernel, heads=heads, rows=rows, nb=nb),
        out_shape=(
            jax.ShapeDtypeStruct((tokens, values), BF),
            jax.ShapeDtypeStruct((tokens, heads), F32),
        ),
        grid_spec=pltpu.PrefetchScalarGridSpec(
            num_scalar_prefetch=1,
            grid=(nb,),
            in_specs=[whole(qkv.shape), whole(seg_col.shape), whole(seg_row.shape)],
            out_specs=[
                pl.BlockSpec((rows, values), lambda a, *_: (a, 0)),
                pl.BlockSpec((rows, heads), lambda a, *_: (a, 0)),
            ],
            scratch_shapes=[pltpu.VMEM((rows, values), F32), pltpu.VMEM((rows, values), F32)],
        ),
        cost_estimate=pl.CostEstimate(
            flops=4 * tokens * values, transcendentals=0, bytes_accessed=8 * tokens
        ),
        name="attention_forward",
    )(meta, qkv, seg_col, seg_row)


def attention_backward(meta, qkv, seg_col, seg_row, gm, mixed, den, scale, heads, rows):
    tokens = qkv.shape[0]
    nb = tokens // rows
    values = heads * VH
    width = heads * QK
    return pl.pallas_call(
        functools.partial(backward_kernel, heads=heads, rows=rows, nb=nb),
        out_shape=jax.ShapeDtypeStruct((tokens, 2 * width + values), BF),
        grid_spec=pltpu.PrefetchScalarGridSpec(
            num_scalar_prefetch=1,
            grid=(nb,),
            in_specs=[
                whole(qkv.shape),
                whole(seg_col.shape),
                whole(seg_row.shape),
                pl.BlockSpec((rows, values), lambda a, *_: (a, 0)),
                pl.BlockSpec((rows, values), lambda a, *_: (a, 0)),
                pl.BlockSpec((rows, heads), lambda a, *_: (a, 0)),
                whole(scale.shape),
            ],
            out_specs=whole((tokens, 2 * width + values)),
            scratch_shapes=[
                pltpu.VMEM((tokens, 128), F32),
                pltpu.VMEM((tokens, values), F32),
                pltpu.VMEM((nb, width, rows), F32),
            ],
        ),
        cost_estimate=pl.CostEstimate(
            flops=10 * tokens * values, transcendentals=0, bytes_accessed=16 * tokens
        ),
        name="attention_backward",
    )(meta, qkv, seg_col, seg_row, gm, mixed, den, scale)


def of_context(parts, c, nc):
    me = lax.axis_index(C)
    out = parts[0][...]
    for i in range(1, nc):
        near = lax.rem(me - 2 * (i // 2) + nc, nc)
        index = near if i % 2 == 0 else near + 1 - 2 * lax.rem(near, 2)
        out = jnp.where(index == c, parts[i][...], out)
    return out


def columns_kernel(*refs, nc, seg, groups):
    parts, weight, gain, out, along = refs[:nc], refs[nc], refs[nc + 1], refs[nc + 2], refs[nc + 3]
    total = jnp.zeros(along.shape, F32)
    for c in range(nc):
        part = of_context(parts, c, nc)
        for j in range(groups):
            place = slice((j * nc + c) * seg, (j * nc + c + 1) * seg)
            value = part[:, j * seg : (j + 1) * seg].astype(F32)
            total += jnp.sum(value * weight[:, place].astype(F32), axis=1, keepdims=True)
            out[:, place] = value * gain[...]
    along[...] = total


def finish_columns(parts, weight, gain, seg, groups):
    nc = len(parts)
    rows, width = weight.shape
    tile = next(t for t in (64, 32, 16, 8) if rows % t == 0)

    def spec(size):
        return pl.BlockSpec((tile, size), lambda i: (i, 0))

    return pl.pallas_call(
        functools.partial(columns_kernel, nc=nc, seg=seg, groups=groups),
        out_shape=(
            jax.ShapeDtypeStruct((rows, width), F32),
            jax.ShapeDtypeStruct((rows, 1), F32),
        ),
        grid=(rows // tile,),
        in_specs=[spec(parts[0].shape[1])] * nc + [spec(width), spec(1)],
        out_specs=[spec(width), spec(1)],
        cost_estimate=pl.CostEstimate(flops=0, transcendentals=0, bytes_accessed=1024),
        name="finish_columns",
    )(*parts, weight, gain)


def rows_kernel(*refs, nc):
    out = refs[nc]
    size = refs[0].shape[0]
    for c in range(nc):
        out[c * size : (c + 1) * size, :] = of_context(refs[:nc], c, nc).astype(F32)


def finish_rows(parts):
    nc = len(parts)
    rows, width = parts[0].shape
    tile = next(t for t in (512, 256, 128) if width % t == 0)
    return pl.pallas_call(
        functools.partial(rows_kernel, nc=nc),
        out_shape=jax.ShapeDtypeStruct((nc * rows, width), F32),
        grid=(width // tile,),
        in_specs=[pl.BlockSpec((rows, tile), lambda i: (0, i))] * nc,
        out_specs=pl.BlockSpec((nc * rows, tile), lambda i: (0, i)),
        cost_estimate=pl.CostEstimate(flops=0, transcendentals=0, bytes_accessed=1024),
        name="finish_rows",
    )(*parts)


def mm(a, b):
    return jnp.dot(a, b, preferred_element_type=F32)


def mm_tn(a, b):
    return lax.dot_general(a, b, (((0,), (0,)), ((), ())), preferred_element_type=F32)


def mm_nt(a, b):
    return lax.dot_general(a, b, (((1,), (1,)), ((), ())), preferred_element_type=F32)


def inverse_rms(values):
    return lax.rsqrt(jnp.mean(values * values, axis=-1, keepdims=True) + EPS)


def local(
    tokens,
    segment_ids,
    norm1_gain,
    w_query,
    w_key,
    w_value,
    w_out,
    norm2_gain,
    w_gate,
    w_up,
    w_down,
    cotangent,
):
    nc, nf = lax.axis_size(C), lax.axis_size(F)
    c = lax.axis_index(C)
    rows, width = tokens.shape[1], tokens.shape[2]
    heads = HEADS // nc
    qk = heads * QK
    hidden_all = w_gate.shape[1]
    seg_len = hidden_all // (nc * nf)
    hidden = seg_len * nf
    shard = w_gate.shape[0]

    own = tokens[0]
    grad_top = cotangent[0]
    gain_one = norm1_gain.astype(F32)[:, None]
    gain_two = norm2_gain.astype(F32)[:, None]

    def columns(weight, size):
        return lax.dynamic_slice_in_dim(weight, c * size, size, axis=1)

    part_qkv = (
        jnp.concatenate(
            [columns(w_query, qk), columns(w_key, qk), columns(w_value, heads * VH)], axis=1
        ).astype(F32)
        * gain_one
    ).astype(BF)

    def hidden_columns(weight):
        picked = lax.dynamic_index_in_dim(
            weight.reshape(shard, nf, nc, seg_len), c, axis=2, keepdims=False
        )
        return (picked.reshape(shard, hidden).astype(F32) * gain_two).astype(BF)

    part_out = group_pieces(w_out)
    part_gate = hidden_columns(w_gate)
    part_up = hidden_columns(w_up)
    part_down = lax.dynamic_slice_in_dim(w_down, c * seg_len, seg_len, axis=0)

    seg_all = jnp.concatenate(spread_direct(segment_ids[0]), axis=0)
    nb = nc
    seg_row = seg_all.reshape(nb, 1, rows)
    seg_col = seg_all.reshape(nb * rows, 1)
    meta = jnp.concatenate(
        [jnp.stack(spread_index()), seg_row[:, 0, 0], seg_row[:, 0, rows - 1]]
    ).astype(jnp.int32)

    line_qkv = gather_lines(part_qkv)
    x_parts = spread(own, [line_qkv])
    line_out = gather_lines(after(part_out, x_parts[-2]))
    line_gate = gather_lines(part_gate)
    line_up = gather_lines(part_up)
    line_down = gather_lines(part_down)
    other_qkv = side_swap(line_qkv)
    x_all = after(jnp.concatenate(x_parts, axis=0), other_qkv)
    scale_one = inverse_rms(x_all.astype(F32))
    full_qkv = assemble(line_qkv, other_qkv)
    qkv = (mm(x_all, full_qkv) * scale_one).astype(BF)
    g_parts = spread(after(grad_top, seg_all, x_all), [qkv])
    mixed, den = attention_forward(meta, qkv, seg_col, seg_row, heads, rows)

    def blocks(value):
        return [value[i * rows : (i + 1) * rows] for i in range(nb)]

    full_out = assemble(line_out, side_swap(after(line_out, qkv)))
    projected = mm(after(mixed, *g_parts), full_out).astype(BF)
    sums = add_cores(blocks(projected))
    low, high = jnp.split(after(line_gate, *sums), 2)
    other_gate = [side_swap(low), side_swap(high)]
    residual = after(own.astype(F32) + add_chips(sums), other_gate[0])

    scale_two = inverse_rms(residual)
    unit_two = residual * scale_two
    full_gate = assemble(line_gate, *other_gate)
    n_all = jnp.concatenate(spread(unit_two.astype(BF), other_gate), axis=0)
    g_all = jnp.concatenate(g_parts, axis=0)
    low, high = jnp.split(after(line_up, unit_two), 2)
    other_up = [side_swap(low), side_swap(high)]
    gate = mm(after(n_all, other_up[0]), full_gate)
    full_up = assemble(line_up, other_up[0], after(other_up[1], gate))
    full_down = assemble(line_down, side_swap(after(line_down, n_all)))
    up = mm(after(n_all, gate), full_up)
    grad_hidden = mm_nt(after(g_all, up), full_down)
    sigmoid = jax.nn.sigmoid(gate)
    silu = gate * sigmoid
    act = (silu * up).astype(BF)
    grad_gate = (grad_hidden * up * sigmoid * (1.0 + gate * (1.0 - sigmoid))).astype(BF)
    grad_up = (grad_hidden * silu).astype(BF)
    back_two = (mm_nt(grad_gate, full_gate) + mm_nt(grad_up, full_up)).astype(BF)
    back_sums = add_cores(blocks(back_two))

    total_gate = mm_tn(n_all, after(grad_gate, *back_sums)).astype(BF)
    mine_gate, sent_gate = scatter_sides(total_gate)
    total_up = mm_tn(n_all, after(grad_up, total_gate)).astype(BF)
    mine_up, sent_up = scatter_sides(total_up)
    grad_unit_two = add_chips([after(back_sums[0], total_up)] + back_sums[1:])

    grad_residual = grad_top.astype(F32) + scale_two * (
        grad_unit_two - unit_two * jnp.mean(grad_unit_two * unit_two, axis=-1, keepdims=True)
    )
    branch = grad_residual.astype(BF)
    total_down = mm_tn(after(act, branch), g_all).astype(BF)
    mine_down, sent_down = scatter_sides(total_down, 2)
    projected_two = mm(after(act, total_down), full_down).astype(BF)
    both_gate = add_sides(mine_gate, sent_gate, total_down)
    sum_gate = scatter_lines(both_gate)
    b_all = jnp.concatenate(spread(branch, [projected_two, both_gate]), axis=0)
    out_sums = add_cores(blocks(after(projected_two, b_all)))

    grad_mixed = mm_nt(b_all, full_out)
    total_out = mm_tn(mixed, after(b_all, grad_mixed)).astype(BF)
    mine_out, sent_out = scatter_sides(total_out)
    grad_qkv = attention_backward(
        meta, qkv, seg_col, seg_row, after(grad_mixed, total_out, *out_sums), mixed, den, scale_one, heads, rows
    )
    block_out = residual + after(add_chips([jnp.zeros_like(out_sums[0])] + out_sums[1:]), grad_qkv) + out_sums[0]
    both_up = add_sides(mine_up, sent_up, grad_qkv)
    sum_up = scatter_lines(both_up)
    back_one = mm_nt(after(grad_qkv, block_out, both_up, sent_down[0]), full_qkv).astype(BF)
    one_sums = add_cores(blocks(back_one))
    total_qkv = mm_tn(x_all, after(grad_qkv, sum_gate, *one_sums)).astype(BF)
    mine_qkv, sent_qkv = scatter_sides(total_qkv)
    grad_unit_one = add_chips(one_sums)
    both_down = add_sides(mine_down, sent_down, total_qkv)
    sum_down = scatter_lines(both_down)
    both_out = add_sides(mine_out, sent_out, both_down, sum_up)
    sum_out = scatter_lines(both_out)
    both_qkv = add_sides(mine_qkv, sent_qkv, both_out, grad_unit_one, sum_down)
    sum_qkv = scatter_lines(both_qkv)
    sum_gate = after(sum_gate, both_out)
    sum_up = after(sum_up, both_out)
    sum_out = after(sum_out, both_qkv)

    unit_one = own.astype(F32) * inverse_rms(own.astype(F32))
    input_grad = grad_residual + grad_unit_one - unit_one * jnp.mean(
        grad_unit_one * unit_one, axis=-1, keepdims=True
    )

    def over_context(value):
        return spread(value.astype(BF))

    def from_hidden(value, weight):
        stacked = in_order(over_context(value)).reshape(nc, shard, nf, seg_len)
        grad = stacked.transpose(1, 2, 0, 3).reshape(shard, hidden_all).astype(F32)
        return grad * gain_two, jnp.sum(weight.astype(F32) * grad, axis=1, keepdims=True)

    grad_w_gate, along_gate = from_hidden(sum_gate, w_gate)
    grad_w_up, along_up = from_hidden(sum_up, w_up)
    qkv_parts = over_context(sum_qkv)

    def columns_of(first, size):
        return [part[:, first : first + size] for part in qkv_parts]

    grad_w_query, along_query = finish_columns(columns_of(0, qk), w_query, gain_one, qk, 1)
    grad_w_key, along_key = finish_columns(columns_of(qk, qk), w_key, gain_one, qk, 1)
    grad_w_value, along_value = finish_columns(
        columns_of(2 * qk, heads * VH), w_value, gain_one, heads * VH, 1
    )
    grad_w_down = finish_rows(over_context(sum_down))
    grad_w_out = ungroup_pieces(sum_out.astype(BF)).astype(F32)
    return (
        block_out.astype(BF)[None],
        input_grad[None],
        (along_query + along_key + along_value)[:, 0],
        grad_w_query,
        grad_w_key,
        grad_w_value,
        grad_w_out,
        (along_gate + along_up)[:, 0],
        grad_w_gate,
        grad_w_up,
        grad_w_down,
    )


def solution(mesh):
    rows = P(F, None)
    acts = P(F, C, None)
    return jax.shard_map(
        local,
        mesh=mesh,
        in_specs=(acts, P(F, C), P(F), rows, rows, rows, rows, P(F), rows, rows, rows, acts),
        out_specs=(acts, acts, P(F), rows, rows, rows, rows, P(F), rows, rows, rows),
        check_vma=False,
    )
```

```python
import functools

import jax
import jax.numpy as jnp
from jax import lax
from jax.experimental import pallas as pl
from jax.experimental.pallas import tpu as pltpu
from jax.sharding import PartitionSpec as P

HEADS = 16
QK = 16
VH = 128
EPS = 1e-05

C = "context"
F = "fsdp"
BF = jnp.bfloat16
F32 = jnp.float32


def after(value, *earlier):
    return lax.optimization_barrier((value,) + earlier)[0]


def lines():
    return lax.axis_size(F) // 2


def line_groups():
    m = lines()
    return [[2 * line + side for line in range(m)] for side in range(2)]


def side_swap(value):
    return lax.ppermute(value, F, [(j, j ^ 1) for j in range(lax.axis_size(F))])


def line_and_side():
    me = lax.axis_index(F)
    return me // 2, lax.rem(me, 2)


def scatter_sides(total):
    m = lines()
    _, side = line_and_side()
    parts = total.reshape(m, 2, total.shape[0] // (2 * m), total.shape[1])
    mine = lax.dynamic_index_in_dim(parts, side, 1, keepdims=False)
    return mine, side_swap(lax.dynamic_index_in_dim(parts, 1 - side, 1, keepdims=False))


def add_sides(mine, sent):
    both = (mine.astype(F32) + sent.astype(F32)).astype(BF)
    return both.reshape(-1, both.shape[-1])


def scatter_lines(total):
    return lax.psum_scatter(total, F, scatter_dimension=0, axis_index_groups=line_groups(), tiled=True)


def gather_lines(block):
    return lax.all_gather(block, F, axis=0, axis_index_groups=line_groups())


def assemble_kernel(own, *refs, m, pieces):
    side = lax.rem(lax.axis_index(F), 2)
    out, sems = refs[pieces], refs[pieces + 1]
    size = m // pieces
    copies = []
    for k in range(m):
        other = refs[k // size].at[k % size]
        copies.append(pltpu.make_async_copy(own.at[k], out.at[2 * k + side], sems.at[k]))
        copies.append(pltpu.make_async_copy(other, out.at[2 * k + 1 - side], sems.at[m + k]))
    for copy in copies:
        copy.start()
    for copy in copies:
        copy.wait()


def assemble(own, *other):
    m, rows, width = own.shape
    out = pl.pallas_call(
        functools.partial(assemble_kernel, m=m, pieces=len(other)),
        out_shape=jax.ShapeDtypeStruct((2 * m, rows, width), own.dtype),
        in_specs=[pl.BlockSpec(memory_space=pl.ANY)] * (1 + len(other)),
        out_specs=pl.BlockSpec(memory_space=pltpu.VMEM),
        scratch_shapes=[pltpu.SemaphoreType.DMA((2 * m,))],
        cost_estimate=pl.CostEstimate(flops=0, transcendentals=0, bytes_accessed=1024),
        name="assemble",
    )(own, *other)
    return out.reshape(2 * m * rows, width)


def chips():
    return lax.axis_size(C) // 2


def core_swap(value):
    n = lax.axis_size(C)
    return lax.ppermute(value, C, [(i, i ^ 1) for i in range(n)])


def chip_shift(value, k):
    n = lax.axis_size(C)
    return lax.ppermute(value, C, [(i, (i + 2 * k) % n) for i in range(n)])


def spread(block, marks=()):
    out = []
    for k in range(chips()):
        near = after(chip_shift(block, k), *marks) if k else block
        out += [near, core_swap(near)]
    return out


def spread_direct(block):
    n = lax.axis_size(C)
    return [
        lax.ppermute(block, C, [(i, (i + 2 * k) % n ^ h) for i in range(n)]) if k or h else block
        for k in range(chips())
        for h in range(2)
    ]


def spread_index():
    n, me = lax.axis_size(C), lax.axis_index(C)
    out = []
    for k in range(chips()):
        near = lax.rem(me - 2 * k + n, n)
        out += [near, near ^ 1]
    return out


def add_cores(parts):
    sums = []
    for k in range(chips()):
        both = parts[2 * k].astype(F32) + core_swap(parts[2 * k + 1]).astype(F32)
        sums.append(both.astype(BF) if k else both)
    return sums


def add_chips(sums):
    total = sums[0]
    for k in range(1, chips()):
        total = total + chip_shift(sums[k], -k).astype(F32)
    return total


def gather_back(parts):
    return add_chips(add_cores(parts))


def in_order(parts):
    out = jnp.zeros((len(parts),) + parts[0].shape, parts[0].dtype)
    for index, part in zip(spread_index(), parts):
        out = lax.dynamic_update_index_in_dim(out, part, index, 0)
    return out


def group_pairs(back):
    nc, nf = lax.axis_size(C), lax.axis_size(F)
    m = nf // nc
    out = []
    for q in range(nc):
        pairs = [
            (c * nf + m * c + s, c * nf + s * nc + q) for c in range(nc) for s in range(m)
        ]
        out.append([(b, a) for a, b in pairs] if back else pairs)
    return out


def group_pieces(shard):
    nc = lax.axis_size(C)
    rows = shard.shape[0] // nc
    out = None
    for q, pairs in enumerate(group_pairs(False)):
        got = lax.ppermute(shard[q * rows : (q + 1) * rows], (C, F), pairs)
        out = got if out is None else out + got
    return out


def ungroup_pieces(piece):
    nc, nf = lax.axis_size(C), lax.axis_size(F)
    m = nf // nc
    shard = jnp.concatenate(
        [lax.ppermute(piece, (C, F), pairs) for pairs in group_pairs(True)], axis=0
    )
    out = shard
    for k in range(1, nc // 2):
        out = out + lax.ppermute(
            shard, (C, F), [((j // m) * nf + j, ((j // m + 2 * k) % nc) * nf + j) for j in range(nf)]
        )
    holders = [((j // m) % 2, j) for j in range(nf)]
    swap = [
        ((2 * x + h) * nf + j, (2 * x + 1 - h) * nf + j) for h, j in holders for x in range(nc // 2)
    ]
    return out + lax.ppermute(out, (C, F), swap)


def dot_nt(a, b):
    return lax.dot_general(a, b, (((1,), (1,)), ((), ())), preferred_element_type=F32)


def dot_nn(a, b):
    return lax.dot_general(a, b, (((1,), (0,)), ((), ())), preferred_element_type=F32)


def with_one(values, width):
    rows = values.shape[0]
    padded = jnp.concatenate([values, jnp.zeros((rows, 128 - width), values.dtype)], axis=1)
    lane = lax.broadcasted_iota(jnp.int32, (rows, 128), 1)
    return jnp.where(lane == width, jnp.ones_like(padded), padded)


def one_head(values, head, width):
    lane = lax.broadcasted_iota(jnp.int32, values.shape, 1)
    keep = jnp.logical_or(lane // QK == head, lane == width)
    return jnp.where(keep, values, jnp.zeros_like(values))


def needed(meta, a, b, nb):
    before = meta[b] < meta[a]
    return jnp.logical_and(before, meta[nb + a] <= meta[2 * nb + b])


def forward_kernel(meta, qkv, seg_col, seg_row, mixed, den, num_sum, den_sum, *, heads, rows, nb):
    width = heads * QK
    a = pl.program_id(0)
    here = pl.ds(pl.multiple_of(a * rows, rows), rows)
    queries = with_one(qkv[here, :width] * 0.25, width)
    seg_q = seg_col[here, :]
    num_sum[...] = jnp.zeros_like(num_sum)
    den_sum[...] = jnp.zeros_like(den_sum)

    def pair(b, diagonal):
        there = pl.ds(pl.multiple_of(b * rows, rows), rows)
        keys = with_one(qkv[there, width : 2 * width], width)
        allowed = seg_q == seg_row[b]
        if diagonal:
            t = lax.broadcasted_iota(jnp.int32, (rows, rows), 0)
            u = lax.broadcasted_iota(jnp.int32, (rows, rows), 1)
            allowed = jnp.logical_and(allowed, u <= t)
        for h in range(heads):
            shifted = dot_nt(one_head(queries, h, width), keys)
            weight = jnp.where(allowed, shifted * shifted + 1.0, 0.0)
            lanes = slice(h * VH, (h + 1) * VH)
            values = qkv[there, 2 * width + h * VH : 2 * width + (h + 1) * VH]
            num_sum[:, lanes] += dot_nn(weight.astype(BF), values)
            den_sum[:, lanes] += jnp.broadcast_to(
                jnp.sum(weight, axis=1, keepdims=True), (rows, VH)
            )

    pair(a, True)

    @pl.loop(0, nb)
    def _(b):
        @pl.when(needed(meta, a, b, nb))
        def _():
            pair(b, False)

    mixed[...] = (num_sum[...] / den_sum[...]).astype(BF)
    for h in range(heads):
        den[:, h : h + 1] = den_sum[:, h * VH : h * VH + 1]


def backward_kernel(
    meta, qkv, seg_col, seg_row, gm, mixed, den, scale, out, key_sum, value_sum, query_sum, *, heads, rows, nb
):
    width = heads * QK
    a = pl.program_id(0)
    here = pl.ds(pl.multiple_of(a * rows, rows), rows)
    queries = with_one(qkv[here, :width] * 0.25, width)
    seg_q = seg_row[a]

    @pl.when(a == 0)
    def _():
        key_sum[...] = jnp.zeros_like(key_sum)
        value_sum[...] = jnp.zeros_like(value_sum)
        query_sum[...] = jnp.zeros_like(query_sum)

    grads, offsets, head_queries = [], [], []
    for h in range(heads):
        g = gm[:, h * VH : (h + 1) * VH].astype(F32)
        d = den[:, h : h + 1]
        grads.append((g / d).astype(BF))
        inner = -jnp.sum(g * mixed[:, h * VH : (h + 1) * VH].astype(F32), axis=1, keepdims=True) / d
        offsets.append(jnp.transpose(jnp.broadcast_to(inner, (rows, 128)))[0:1, :])
        head_queries.append(one_head(queries, h, width))

    def pair(b, diagonal):
        there = pl.ds(pl.multiple_of(b * rows, rows), rows)
        raw = qkv[there, width : 2 * width]
        keys = with_one(raw, width)
        turned = jnp.transpose(keys)
        allowed = seg_col[there, :] == seg_q
        if diagonal:
            u = lax.broadcasted_iota(jnp.int32, (rows, rows), 0)
            t = lax.broadcasted_iota(jnp.int32, (rows, rows), 1)
            allowed = jnp.logical_and(allowed, u <= t)
        for h in range(heads):
            lanes = slice(h * VH, (h + 1) * VH)
            shifted = dot_nt(keys, head_queries[h])
            weight = jnp.where(allowed, shifted * shifted + 1.0, 0.0).astype(BF)
            value_sum[there, lanes] += dot_nn(weight, grads[h])
            values = qkv[there, 2 * width + h * VH : 2 * width + (h + 1) * VH]
            grad = dot_nt(values, grads[h]) + offsets[h]
            score = jnp.where(allowed, grad * shifted, 0.0).astype(BF)
            key_sum[there, :] += dot_nn(score, head_queries[h])
            query_sum[a, h * QK : (h + 1) * QK, :] += dot_nn(turned[h * QK : (h + 1) * QK, :], score)

    pair(a, True)

    @pl.loop(0, nb)
    def _(b):
        @pl.when(needed(meta, a, b, nb))
        def _():
            pair(b, False)

    @pl.when(a == nb - 1)
    def _():
        for b in range(nb):
            span = slice(b * rows, (b + 1) * rows)
            s = scale[span, :]
            grad_q = jnp.transpose(query_sum[b]) * (0.5 * s)
            out[span, :width] = grad_q.astype(BF)
            out[span, width : 2 * width] = (key_sum[span, :width] * (2.0 * s)).astype(BF)
            out[span, 2 * width :] = (value_sum[span, :] * s).astype(BF)


def block_spec(shape, index):
    return pl.BlockSpec(shape, index)


def whole(shape):
    return pl.BlockSpec(shape, lambda a, *_: (0,) * len(shape))


def attention_forward(meta, qkv, seg_col, seg_row, heads, rows):
    tokens = qkv.shape[0]
    nb = tokens // rows
    values = heads * VH
    return pl.pallas_call(
        functools.partial(forward_kernel, heads=heads, rows=rows, nb=nb),
        out_shape=(
            jax.ShapeDtypeStruct((tokens, values), BF),
            jax.ShapeDtypeStruct((tokens, heads), F32),
        ),
        grid_spec=pltpu.PrefetchScalarGridSpec(
            num_scalar_prefetch=1,
            grid=(nb,),
            in_specs=[whole(qkv.shape), whole(seg_col.shape), whole(seg_row.shape)],
            out_specs=[
                pl.BlockSpec((rows, values), lambda a, *_: (a, 0)),
                pl.BlockSpec((rows, heads), lambda a, *_: (a, 0)),
            ],
            scratch_shapes=[pltpu.VMEM((rows, values), F32), pltpu.VMEM((rows, values), F32)],
        ),
        cost_estimate=pl.CostEstimate(
            flops=4 * tokens * values, transcendentals=0, bytes_accessed=8 * tokens
        ),
        name="attention_forward",
    )(meta, qkv, seg_col, seg_row)


def attention_backward(meta, qkv, seg_col, seg_row, gm, mixed, den, scale, heads, rows):
    tokens = qkv.shape[0]
    nb = tokens // rows
    values = heads * VH
    width = heads * QK
    return pl.pallas_call(
        functools.partial(backward_kernel, heads=heads, rows=rows, nb=nb),
        out_shape=jax.ShapeDtypeStruct((tokens, 2 * width + values), BF),
        grid_spec=pltpu.PrefetchScalarGridSpec(
            num_scalar_prefetch=1,
            grid=(nb,),
            in_specs=[
                whole(qkv.shape),
                whole(seg_col.shape),
                whole(seg_row.shape),
                pl.BlockSpec((rows, values), lambda a, *_: (a, 0)),
                pl.BlockSpec((rows, values), lambda a, *_: (a, 0)),
                pl.BlockSpec((rows, heads), lambda a, *_: (a, 0)),
                whole(scale.shape),
            ],
            out_specs=whole((tokens, 2 * width + values)),
            scratch_shapes=[
                pltpu.VMEM((tokens, 128), F32),
                pltpu.VMEM((tokens, values), F32),
                pltpu.VMEM((nb, width, rows), F32),
            ],
        ),
        cost_estimate=pl.CostEstimate(
            flops=10 * tokens * values, transcendentals=0, bytes_accessed=16 * tokens
        ),
        name="attention_backward",
    )(meta, qkv, seg_col, seg_row, gm, mixed, den, scale)


def of_context(parts, c, nc):
    me = lax.axis_index(C)
    out = parts[0][...]
    for i in range(1, nc):
        near = lax.rem(me - 2 * (i // 2) + nc, nc)
        index = near if i % 2 == 0 else near + 1 - 2 * lax.rem(near, 2)
        out = jnp.where(index == c, parts[i][...], out)
    return out


def columns_kernel(*refs, nc, seg, groups):
    parts, weight, gain, out, along = refs[:nc], refs[nc], refs[nc + 1], refs[nc + 2], refs[nc + 3]
    total = jnp.zeros(along.shape, F32)
    for c in range(nc):
        part = of_context(parts, c, nc)
        for j in range(groups):
            place = slice((j * nc + c) * seg, (j * nc + c + 1) * seg)
            value = part[:, j * seg : (j + 1) * seg].astype(F32)
            total += jnp.sum(value * weight[:, place].astype(F32), axis=1, keepdims=True)
            out[:, place] = value * gain[...]
    along[...] = total


def finish_columns(parts, weight, gain, seg, groups):
    nc = len(parts)
    rows, width = weight.shape
    tile = next(t for t in (64, 32, 16, 8) if rows % t == 0)

    def spec(size):
        return pl.BlockSpec((tile, size), lambda i: (i, 0))

    return pl.pallas_call(
        functools.partial(columns_kernel, nc=nc, seg=seg, groups=groups),
        out_shape=(
            jax.ShapeDtypeStruct((rows, width), F32),
            jax.ShapeDtypeStruct((rows, 1), F32),
        ),
        grid=(rows // tile,),
        in_specs=[spec(parts[0].shape[1])] * nc + [spec(width), spec(1)],
        out_specs=[spec(width), spec(1)],
        cost_estimate=pl.CostEstimate(flops=0, transcendentals=0, bytes_accessed=1024),
        name="finish_columns",
    )(*parts, weight, gain)


def rows_kernel(*refs, nc):
    out = refs[nc]
    size = refs[0].shape[0]
    for c in range(nc):
        out[c * size : (c + 1) * size, :] = of_context(refs[:nc], c, nc).astype(F32)


def finish_rows(parts):
    nc = len(parts)
    rows, width = parts[0].shape
    tile = next(t for t in (512, 256, 128) if width % t == 0)
    return pl.pallas_call(
        functools.partial(rows_kernel, nc=nc),
        out_shape=jax.ShapeDtypeStruct((nc * rows, width), F32),
        grid=(width // tile,),
        in_specs=[pl.BlockSpec((rows, tile), lambda i: (0, i))] * nc,
        out_specs=pl.BlockSpec((nc * rows, tile), lambda i: (0, i)),
        cost_estimate=pl.CostEstimate(flops=0, transcendentals=0, bytes_accessed=1024),
        name="finish_rows",
    )(*parts)


def mm(a, b):
    return jnp.dot(a, b, preferred_element_type=F32)


def mm_tn(a, b):
    return lax.dot_general(a, b, (((0,), (0,)), ((), ())), preferred_element_type=F32)


def mm_nt(a, b):
    return lax.dot_general(a, b, (((1,), (1,)), ((), ())), preferred_element_type=F32)


def inverse_rms(values):
    return lax.rsqrt(jnp.mean(values * values, axis=-1, keepdims=True) + EPS)


def local(
    tokens,
    segment_ids,
    norm1_gain,
    w_query,
    w_key,
    w_value,
    w_out,
    norm2_gain,
    w_gate,
    w_up,
    w_down,
    cotangent,
):
    nc, nf = lax.axis_size(C), lax.axis_size(F)
    c = lax.axis_index(C)
    rows, width = tokens.shape[1], tokens.shape[2]
    heads = HEADS // nc
    qk = heads * QK
    hidden_all = w_gate.shape[1]
    seg_len = hidden_all // (nc * nf)
    hidden = seg_len * nf
    shard = w_gate.shape[0]

    own = tokens[0]
    grad_top = cotangent[0]
    gain_one = norm1_gain.astype(F32)[:, None]
    gain_two = norm2_gain.astype(F32)[:, None]

    def columns(weight, size):
        return lax.dynamic_slice_in_dim(weight, c * size, size, axis=1)

    part_qkv = (
        jnp.concatenate(
            [columns(w_query, qk), columns(w_key, qk), columns(w_value, heads * VH)], axis=1
        ).astype(F32)
        * gain_one
    ).astype(BF)

    def hidden_columns(weight):
        picked = lax.dynamic_index_in_dim(
            weight.reshape(shard, nf, nc, seg_len), c, axis=2, keepdims=False
        )
        return (picked.reshape(shard, hidden).astype(F32) * gain_two).astype(BF)

    part_out = group_pieces(w_out)
    part_gate = hidden_columns(w_gate)
    part_up = hidden_columns(w_up)
    part_down = lax.dynamic_slice_in_dim(w_down, c * seg_len, seg_len, axis=0)

    seg_all = jnp.concatenate(spread_direct(segment_ids[0]), axis=0)
    nb = nc
    seg_row = seg_all.reshape(nb, 1, rows)
    seg_col = seg_all.reshape(nb * rows, 1)
    meta = jnp.concatenate(
        [jnp.stack(spread_index()), seg_row[:, 0, 0], seg_row[:, 0, rows - 1]]
    ).astype(jnp.int32)

    line_qkv = gather_lines(part_qkv)
    x_parts = spread(own, [line_qkv])
    line_out = gather_lines(after(part_out, x_parts[-2]))
    line_gate = gather_lines(part_gate)
    line_up = gather_lines(part_up)
    line_down = gather_lines(part_down)
    x_all = jnp.concatenate(x_parts, axis=0)
    scale_one = inverse_rms(x_all.astype(F32))
    full_qkv = assemble(line_qkv, side_swap(line_qkv))
    g_parts = spread(after(grad_top, seg_all, x_all))
    qkv = (mm(x_all, full_qkv) * scale_one).astype(BF)
    mixed, den = attention_forward(meta, qkv, seg_col, seg_row, heads, rows)

    def blocks(value):
        return [value[i * rows : (i + 1) * rows] for i in range(nb)]

    full_out = assemble(line_out, side_swap(line_out))
    projected = mm(after(mixed, *g_parts), full_out).astype(BF)
    sums = add_cores(blocks(projected))
    residual = own.astype(F32) + add_chips(sums)

    scale_two = inverse_rms(residual)
    unit_two = residual * scale_two
    full_gate = assemble(line_gate, side_swap(after(line_gate, *sums)))
    n_all = jnp.concatenate(spread(unit_two.astype(BF)), axis=0)
    g_all = jnp.concatenate(g_parts, axis=0)
    full_up = assemble(line_up, side_swap(after(line_up, unit_two)))
    gate = mm(after(n_all, full_up), full_gate)
    low, high = jnp.split(after(line_down, n_all), 2)
    other_down = [side_swap(low), side_swap(high)]
    up = mm(after(n_all, gate, other_down[0]), full_up)
    full_down = assemble(line_down, *other_down)
    grad_hidden = mm_nt(after(g_all, up), full_down)
    sigmoid = jax.nn.sigmoid(gate)
    silu = gate * sigmoid
    act = (silu * up).astype(BF)
    grad_gate = (grad_hidden * up * sigmoid * (1.0 + gate * (1.0 - sigmoid))).astype(BF)
    grad_up = (grad_hidden * silu).astype(BF)
    back_two = (mm_nt(grad_gate, full_gate) + mm_nt(grad_up, full_up)).astype(BF)
    back_sums = add_cores(blocks(back_two))

    total_gate = mm_tn(n_all, after(grad_gate, *back_sums)).astype(BF)
    mine_gate, sent_gate = scatter_sides(total_gate)
    total_up = mm_tn(n_all, after(grad_up, total_gate)).astype(BF)
    mine_up, sent_up = scatter_sides(total_up)
    grad_unit_two = add_chips([after(back_sums[0], total_up)] + back_sums[1:])

    grad_residual = grad_top.astype(F32) + scale_two * (
        grad_unit_two - unit_two * jnp.mean(grad_unit_two * unit_two, axis=-1, keepdims=True)
    )
    branch = grad_residual.astype(BF)
    total_down = mm_tn(after(act, branch), g_all).astype(BF)
    mine_down, sent_down = scatter_sides(total_down)
    projected_two = mm(after(act, total_down), full_down).astype(BF)
    both_gate = add_sides(mine_gate, after(sent_gate, total_down))
    sum_gate = scatter_lines(both_gate)
    b_all = jnp.concatenate(spread(branch, [projected_two, both_gate]), axis=0)
    out_sums = add_cores(blocks(after(projected_two, b_all)))

    grad_mixed = mm_nt(b_all, full_out)
    total_out = mm_tn(mixed, after(b_all, grad_mixed)).astype(BF)
    mine_out, sent_out = scatter_sides(total_out)
    both_up = add_sides(mine_up, after(sent_up, total_out))
    sum_up = scatter_lines(both_up)
    grad_qkv = attention_backward(
        meta, qkv, seg_col, seg_row, after(grad_mixed, both_up, sum_gate, *out_sums), mixed, den, scale_one, heads, rows
    )
    block_out = residual + after(add_chips([jnp.zeros_like(out_sums[0])] + out_sums[1:]), grad_qkv) + out_sums[0]
    back_one = mm_nt(after(grad_qkv, block_out), full_qkv).astype(BF)
    one_sums = add_cores(blocks(back_one))
    both_down = add_sides(mine_down, after(sent_down, *one_sums))
    total_qkv = mm_tn(x_all, after(grad_qkv, both_down)).astype(BF)
    mine_qkv, sent_qkv = scatter_sides(total_qkv)
    grad_unit_one = add_chips(one_sums)
    sum_down = scatter_lines(both_down)
    both_out = add_sides(mine_out, after(sent_out, both_down, sum_up))
    sum_out = scatter_lines(both_out)
    both_qkv = add_sides(mine_qkv, after(sent_qkv, both_out, grad_unit_one, sum_down))
    sum_qkv = scatter_lines(both_qkv)
    sum_gate = after(sum_gate, both_qkv)
    sum_up = after(sum_up, both_qkv, grad_unit_one)
    sum_out = after(sum_out, both_qkv)

    unit_one = own.astype(F32) * inverse_rms(own.astype(F32))
    input_grad = grad_residual + grad_unit_one - unit_one * jnp.mean(
        grad_unit_one * unit_one, axis=-1, keepdims=True
    )

    def over_context(value):
        return spread(value.astype(BF))

    def from_hidden(value, weight):
        stacked = in_order(over_context(value)).reshape(nc, shard, nf, seg_len)
        grad = stacked.transpose(1, 2, 0, 3).reshape(shard, hidden_all).astype(F32)
        return grad * gain_two, jnp.sum(weight.astype(F32) * grad, axis=1, keepdims=True)

    grad_w_gate, along_gate = from_hidden(sum_gate, w_gate)
    grad_w_up, along_up = from_hidden(sum_up, w_up)
    qkv_parts = over_context(sum_qkv)

    def columns_of(first, size):
        return [part[:, first : first + size] for part in qkv_parts]

    grad_w_query, along_query = finish_columns(columns_of(0, qk), w_query, gain_one, qk, 1)
    grad_w_key, along_key = finish_columns(columns_of(qk, qk), w_key, gain_one, qk, 1)
    grad_w_value, along_value = finish_columns(
        columns_of(2 * qk, heads * VH), w_value, gain_one, heads * VH, 1
    )
    grad_w_down = finish_rows(over_context(sum_down))
    grad_w_out = ungroup_pieces(sum_out.astype(BF)).astype(F32)
    return (
        block_out.astype(BF)[None],
        input_grad[None],
        (along_query + along_key + along_value)[:, 0],
        grad_w_query,
        grad_w_key,
        grad_w_value,
        grad_w_out,
        (along_gate + along_up)[:, 0],
        grad_w_gate,
        grad_w_up,
        grad_w_down,
    )


def solution(mesh):
    rows = P(F, None)
    acts = P(F, C, None)
    return jax.shard_map(
        local,
        mesh=mesh,
        in_specs=(acts, P(F, C), P(F), rows, rows, rows, rows, P(F), rows, rows, rows, acts),
        out_specs=(acts, acts, P(F), rows, rows, rows, rows, P(F), rows, rows, rows),
        check_vma=False,
    )
```
